512 devices in a mesh: row: 32 (over z, x), col: 16 (over y, core).
Axes of the slice: x: 4, y: 8, z: 8, core: 2. Of those that a mesh axis runs over, the one named last changes fastest.
Arguments:
- matrix: float32 [16384, 16384], P('row', 'col'), may hold values from -300 to 300, as said below
Outputs:
- trailing: float32 [16384, 16384], P('row', 'col')
- reflectors: float32 [16384, 8], P('row')
The draws below stay inside these ranges and needn't reach their ends.
Inputs may be any that keep to these rules, and one draw needn't show every extreme that they name: matrix is exactly symmetric.
All inputs are finite; a program needn't handle non-finite values.
Results may differ from the reference program's by a relative error of at most 0.00021.
Values sent between devices are 32-bit elements; how exact they have to be, the bound alone decides.
No kernel may reach another device: no remote copies, remote signals or barrier semaphores. Data moves between devices by JAX's collectives and lax.ppermute only.
A program may use at most 64 MiB of HBM per device.

```python
import math
import jax
import jax.numpy as jnp
from jax import lax

N = 16384
COLS = 8


def draw_matrix(key, part):
    first_key, second_key = jax.random.split(jax.random.fold_in(key, 11))
    positions = jnp.arange(N, dtype=jnp.float32)
    rising = jnp.exp(0.5 * math.log(3.0) * positions / N)
    entries = jnp.clip(jax.random.normal(first_key, (N, N), jnp.float32), -6.0, 6.0)
    spread = jnp.exp(0.5 * jax.random.uniform(second_key, (N,), jnp.float32, 0.0, math.log(10.0)))
    symmetric = (entries + entries.T) * (1.0 / math.sqrt(2.0))
    scales = rising * spread
    outer = scales[:, None] * scales[None, :]
    return (symmetric * outer).astype(jnp.float32)


def setup_inputs(seed: int = 0) -> dict:
    streams_of = jax.random.split(jax.random.key(seed), 2)
    return {
        "matrix": draw_matrix(jax.random.fold_in(streams_of[1], 71), 0),
    }


def precise_dot(operand, factor):
    return jnp.dot(operand, factor, precision=lax.Precision.HIGHEST, preferred_element_type=jnp.float32)

def reference(matrix):
    reflect = jnp.zeros((N, COLS), jnp.float32)
    companion = jnp.zeros((N, COLS), jnp.float32)
    positions = jnp.arange(N, dtype=jnp.int32)
    for column in range(COLS):
        current = matrix[:, column] - precise_dot(reflect, companion[column]) - precise_dot(companion, reflect[column])
        below_part = jnp.where(positions > column, current, 0.0)
        squared = jnp.sum(below_part * below_part)
        leading = jnp.sum(jnp.where(positions == column + 1, current, 0.0))
        length = jnp.sqrt(squared)
        vector = below_part + jnp.where(positions == column + 1, length, 0.0)
        scaling = 1.0 / (length * (length + leading))
        column_image = precise_dot(matrix, vector)
        weight_comp = precise_dot(companion.T, vector)
        weight_refl = precise_dot(reflect.T, vector)
        pushed = scaling * (column_image - precise_dot(reflect, weight_comp) - precise_dot(companion, weight_refl))
        inner_product = jnp.sum(pushed * vector)
        update = pushed - 0.5 * scaling * inner_product * vector
        reflect = reflect.at[:, column].set(vector)
        companion = companion.at[:, column].set(update)
    trailing = matrix - precise_dot(reflect, companion.T) - precise_dot(companion, reflect.T)
    return (trailing, reflect)
```

```python
import functools

import jax
import jax.numpy as jnp
from jax import lax
from jax.experimental import pallas as pl
from jax.experimental.pallas import tpu as pltpu
from jax.sharding import PartitionSpec as P


N = 16384
COLS = 8
LANES = 128
F32 = jnp.float32
VMEM = pltpu.VMEM
LIMIT = 16 << 20


def total(x):
    return jnp.sum(jnp.sum(x, axis=0, keepdims=True), axis=1, keepdims=True)


def iota(shape, dim):
    return lax.broadcasted_iota(jnp.int32, shape, dim)


def without_first(x, owner):
    hit = (iota(x.shape, 0) == 0) & (iota(x.shape, 1) == 0)
    if owner is not None:
        hit = hit & (owner == 0)
    return jnp.where(hit, 0.0, x)


def times_rows(a_ref, x):
    upright = jnp.concatenate([x, jnp.zeros_like(x)], axis=0).T
    out = []
    for t in range(8):
        acc = jnp.zeros((8, LANES), F32)
        for q in range(4):
            block = a_ref[q * LANES : (q + 1) * LANES, t * LANES : (t + 1) * LANES]
            acc = acc + jnp.sum((block * upright[:, q : q + 1]).reshape(16, 8, LANES), axis=0)
        out.append(jnp.sum(acc, axis=0, keepdims=True))
    return jnp.concatenate(out, axis=0)


def times_cols(a_ref, x):
    out = []
    for q in range(4):
        acc = jnp.zeros((LANES, LANES), F32)
        for t in range(8):
            block = a_ref[q * LANES : (q + 1) * LANES, t * LANES : (t + 1) * LANES]
            acc = acc + block * x[t : t + 1, :]
        out.append(jnp.sum(acc.T, axis=0, keepdims=True))
    return jnp.concatenate(out, axis=0)


def send_all(send_ref, first, parts):
    for member in range(send_ref.shape[0]):
        for k, part in enumerate(parts):
            send_ref[member, first + k] = part


def halves(x):
    return [x[:4], x[4:]]


def along_cols(recv_ref):
    s = jnp.sum(recv_ref[:, 0:2], axis=0)
    return jnp.concatenate([s[0], s[1]], axis=0)


def along_rows(recv_ref):
    return jnp.sum(recv_ref[:, 0], axis=0)


def whole_from_rows(recv_ref, group):
    return jnp.concatenate([recv_ref[r, group] for r in range(recv_ref.shape[0])], axis=0)


def whole_from_cols(recv_ref, group):
    return jnp.concatenate(
        [recv_ref[c, group + k] for c in range(recv_ref.shape[0]) for k in range(2)], axis=0
    )


def start_kernel(a_ref, held_ref, send_ref):
    held_ref[...] = a_ref[...]
    left = [a_ref[q * LANES : (q + 1) * LANES, 0:LANES].T for q in range(4)]
    column = jnp.concatenate([x[0:1] for x in left], axis=0)
    corner = a_ref[0:16, 0:LANES]
    packed = jnp.zeros((1, LANES), F32)
    for j in range(COLS):
        lanes = iota((1, LANES), 1)
        entry = jnp.where(lanes < 16, corner[j + 1 : j + 2], 0.0)
        packed = packed + (pltpu.roll(entry, 16 * j, 1) if j else entry)
    blank = jnp.zeros((1, LANES), F32)
    for member in range(16):
        j, half = member // 2, member % 2
        rows = [left[2 * half + k][j + 1 : j + 2] for k in range(2)]
        send_ref[member, 0] = column
        send_ref[member, 1] = jnp.concatenate([*rows, packed, blank], axis=0)


def first_kernel(ids_ref, a_ref, recv_ref, send_ref, piece_ref):
    column = recv_ref[0, 0]
    piece_ref[...] = recv_ref[0, 1]
    packed = recv_ref[0, 1][2:3]
    send_all(send_ref, 0, halves(times_rows(a_ref, without_first(column, ids_ref[0]))))
    send_all(send_ref, 2, [column])
    blank = jnp.zeros((1, LANES), F32)
    for member in range(32):
        j, quarter = member // 4, member % 4
        rows = [
            a_ref[j + 1 : j + 2, (2 * quarter + k) * LANES : (2 * quarter + k + 1) * LANES]
            for k in range(2)
        ]
        send_ref[member, 3] = jnp.concatenate([*rows, packed, blank], axis=0)


def coefficient(scal, k):
    return scal[k : k + 1, 0:1]


def settle(step, y_whole, scal, qs, aqs):
    if step == 2:
        aq = None
        u = without_first(y_whole, None)
    else:
        aq = y_whole
        for i in range(1, step - 2):
            aq = aq - coefficient(scal, i) * aqs[i]
        aq = aq * coefficient(scal, 8)
        u = aq
        if step > 3:
            u = u - coefficient(scal, 0) * qs[step - 3]
        u = without_first(u, None)
    known = range(1, step - 1)
    rows = [jnp.sum(u * qs[i], axis=0, keepdims=True) for i in known]
    w = u
    cs = {}
    if rows:
        rows = rows + [jnp.zeros((1, LANES), F32)] * (8 - len(rows))
        sums = jnp.sum(jnp.concatenate(rows, axis=0), axis=1, keepdims=True)
        for i in known:
            cs[i] = sums[i - 1 : i, 0:1]
            w = w - cs[i] * qs[i]
    length = jnp.sqrt(total(w * w))
    inverse = 1.0 / length
    zero = jnp.zeros((1, LANES), F32)
    out = [zero + length] + [zero + cs[i] if i in cs else zero for i in range(1, 8)]
    out = out + [zero + inverse] + [zero] * 7
    return aq, w * inverse, length, inverse, cs, jnp.concatenate(out, axis=0)


def step_kernel(step, *refs):
    refs = list(refs)
    ids_ref, a_ref, recv_ref = refs[:3]
    del refs[:3]
    piece_ref = refs.pop(0) if step in (2, 3) else None
    scal = refs.pop(0)[...] if step > 2 else None
    q_refs = {i: refs.pop(0) for i in range(1, step - 1)}
    aq_refs = {i: refs.pop(0) for i in range(1, step - 2)}
    send_ref = refs.pop(0)
    q_ref = refs.pop(0)
    aq_ref = refs.pop(0) if step > 2 else None
    scal_ref = refs.pop(0)
    edge_ref = refs.pop(0) if step in (3, 4) else None
    new_piece_ref = refs.pop(0) if step == 2 else None

    even = step % 2 == 0
    if even:
        y_here = along_cols(recv_ref)
        y_whole = whole_from_rows(recv_ref, 2)
        chunk, rows = ids_ref[1], 8
    else:
        y_here = along_rows(recv_ref)
        y_whole = whole_from_cols(recv_ref, 1)
        chunk, rows = ids_ref[0], 4
    aq, q, length, inverse, cs, scal_out = settle(
        step,
        y_whole,
        scal,
        {i: r[...] for i, r in q_refs.items()},
        {i: r[...] for i, r in aq_refs.items()},
    )
    q_ref[...] = q
    scal_ref[...] = scal_out
    if aq_ref is not None:
        aq_ref[...] = aq
    at = pl.ds(chunk * rows, rows)
    here = y_here
    for i in cs:
        source = aq_ref if i == step - 2 else aq_refs[i]
        here = here - cs[i] * source[at, :]
    here = here * inverse
    if step > 2:
        here = here - length * q_refs[step - 2][at, :]
    here = without_first(here, chunk)
    if even:
        send_all(send_ref, 0, [times_cols(a_ref, here)])
        send_all(send_ref, 1, halves(y_here))
    else:
        send_all(send_ref, 0, halves(times_rows(a_ref, here)))
        send_all(send_ref, 2, [y_here])
    if step in (2, 3):
        send_all(send_ref, 3, [piece_ref[...]])
    if step == 2:
        new_piece_ref[...] = recv_ref[0, 3]
    if step == 3:
        edge_ref[...] = jnp.concatenate([recv_ref[c, 3][0:2] for c in range(16)], axis=0)
    if step == 4:
        edge_ref[...] = jnp.concatenate([recv_ref[r, 3][0:2] for r in range(32)], axis=0)


def last_send_kernel(recv_ref, send_ref):
    send_all(send_ref, 0, [along_rows(recv_ref)])


def sign(k):
    return -1.0 if k % 2 else 1.0


def product(x, y):
    return lax.dot_general(
        x,
        y,
        (((0,), (0,)), ((), ())),
        precision=lax.Precision.HIGHEST,
        preferred_element_type=F32,
    )


def rows_at(refs, row):
    return jnp.concatenate([sign(k) * refs[k][pl.ds(row, 1), :] for k in range(1, 9)], axis=0)


def d_tile(q_refs, row):
    lanes, ks = iota((8, LANES), 1), iota((8, LANES), 0)
    unit = jnp.where((lanes == ks + 1) & (row == 0), 1.0, 0.0)
    return unit - rows_at(q_refs, row)


def panel_kernel(*refs):
    refs = list(refs)
    ids_ref, recv_ref = refs[:2]
    scal_refs = {i: refs[1 + i] for i in range(1, 8)}
    q_refs = {i: refs[8 + i] for i in range(1, 8)}
    aq_refs = {i: refs[15 + i] for i in range(1, 7)}
    q_out, aq_out, scal_out, factor_ref, reflect_ref = refs[22:27]
    y_whole = whole_from_cols(recv_ref, 1)
    aq, q, _, _, _, scal = settle(
        9,
        y_whole,
        scal_refs[7][...],
        {i: r[...] for i, r in q_refs.items()},
        {i: r[...] for i, r in aq_refs.items()},
    )
    q_out[...] = q
    aq_out[...] = aq
    scal_out[...] = scal
    q_refs[8] = q_out
    lanes, ks = iota((8, LANES), 1), iota((8, LANES), 0)
    top = d_tile(q_refs, 0)
    work = jnp.where(lanes < 8, pltpu.roll(top, LANES - 1, 1), 0.0)
    work = work + jnp.where(lanes == ks + 8, 1.0, 0.0)
    to_reflect = jnp.zeros((8, LANES), F32)
    for k in range(8):
        row = work[k : k + 1]
        beta = (scal if k == 7 else scal_refs[k + 1])[0:1, :]
        to_reflect = jnp.where(ks == k, row * beta, to_reflect)
        row = row / row[:, k : k + 1]
        column = jnp.where(ks == k, 0.0, work)[:, k : k + 1]
        work = jnp.where(ks == k, row, work - column * row)
    factor_ref[...] = jnp.where(lanes < 8, pltpu.roll(work, LANES - 8, 1), 0.0)
    to_reflect = jnp.where(lanes < 8, pltpu.roll(to_reflect, LANES - 8, 1), 0.0)
    for t in range(4):
        row = 4 * ids_ref[0] + t
        d = d_tile(q_refs, row)
        out = jnp.zeros((8, LANES), F32)
        for k in range(8):
            out = out + to_reflect[:, k : k + 1] * d[k : k + 1, :]
        out = jnp.where((row == 0) & (lanes <= ks), 0.0, out)
        reflect_ref[:, t * LANES : (t + 1) * LANES] = out


def trailing_kernel(*refs):
    refs = list(refs)
    ids_ref, a_ref, recv_ref, packed_ref, edge_r_ref, edge_c_ref, factor_ref = refs[:7]
    scal_refs = {i: refs[6 + i] for i in range(1, 9)}
    q_refs = {i: refs[14 + i] for i in range(1, 9)}
    aq_refs = {i: refs[22 + i] for i in range(1, 8)}
    out_ref, last_ref, left_ref, right_ref = refs[30:34]
    scal = scal_refs[8][...]
    aq = whole_from_rows(recv_ref, 0)
    for i in range(1, 8):
        aq = aq - coefficient(scal, i) * aq_refs[i][...]
    aq = aq * coefficient(scal, 8)
    last_ref[...] = aq
    aq_refs[8] = last_ref
    lanes, ks = iota((8, LANES), 1), iota((8, LANES), 0)
    factor = factor_ref[...]
    inner = jnp.zeros((8, LANES), F32)
    packed = packed_ref[2:3]
    for j in range(8):
        entry = pltpu.roll(packed, LANES - 16 * j, 1) if j else packed
        inner = jnp.where(ks == j, entry, inner)
    inner = jnp.where((lanes >= 1) & (lanes <= 8), inner, 0.0)
    cross = rows_at(aq_refs, 0)
    cross = jnp.where((lanes >= 1) & (lanes <= 8), cross, 0.0)
    inner = pltpu.roll(inner - cross, LANES - 1, 1)
    cross = pltpu.roll(cross, LANES - 1, 1)
    square = jnp.concatenate([cross, jnp.zeros((LANES - 8, LANES), F32)], axis=0)
    inner = inner - square.T[0:8]
    for k in range(1, 9):
        if k < 8:
            alpha = scal_refs[k + 1][k : k + 1, :]
            beta = scal_refs[k + 1][0:1, :]
            near = ((ks == k - 1) & (lanes == k)) | ((ks == k) & (lanes == k - 1))
            inner = inner - jnp.where(near, beta, 0.0)
        else:
            alpha = total(q_refs[8][...] * aq)
        inner = inner + jnp.where((ks == k - 1) & (lanes == k - 1), alpha, 0.0)
    factor = factor[:, 0:8]
    inner = inner[:, 0:8]
    core = product(factor, product(inner, factor))

    def tiles(base, count, edge_ref):
        ds, ys = [], []
        for t in range(count):
            row = base + t
            d = d_tile(q_refs, row)
            edge = jnp.concatenate(
                [edge_ref[count * j + t : count * j + t + 1, :] for j in range(8)], axis=0
            )
            ad = edge - rows_at(aq_refs, row)
            ds.append(d)
            ys.append(product(factor, ad) - 0.5 * product(core, d))
        return ds, ys

    ds, ys = tiles(4 * ids_ref[0], 4, edge_r_ref)
    for t in range(4):
        left_ref[0:8, t * LANES : (t + 1) * LANES] = ds[t]
        left_ref[8:16, t * LANES : (t + 1) * LANES] = ys[t]
    ds, ys = tiles(8 * ids_ref[1], 8, edge_c_ref)
    for t in range(8):
        right_ref[0:8, t * LANES : (t + 1) * LANES] = ys[t]
        right_ref[8:16, t * LANES : (t + 1) * LANES] = ds[t]
    for q in range(4):
        at = slice(q * LANES, (q + 1) * LANES)
        out_ref[at, :] = a_ref[at, :] - product(left_ref[:, at], right_ref[...])


def call(kernel, outs, *args, scratch=(), pinned=True, flops=1000):
    def spec(x):
        return pl.BlockSpec(memory_space=pltpu.SMEM if x.dtype == jnp.int32 else VMEM)

    return pl.pallas_call(
        kernel,
        out_shape=[VMEM(s, F32) if pinned else jax.ShapeDtypeStruct(s, F32) for s in outs],
        in_specs=[spec(x) for x in args],
        out_specs=[pl.BlockSpec(memory_space=VMEM)] * len(outs),
        scratch_shapes=[VMEM(s, F32) for s in scratch],
        compiler_params=pltpu.CompilerParams(vmem_limit_bytes=LIMIT),
        cost_estimate=pl.CostEstimate(flops=flops, bytes_accessed=1000, transcendentals=0),
    )(*args)


def exchange(x, axis):
    return lax.all_to_all(x, axis, 0, 0, tiled=True)


def local(matrix):
    ids = jnp.stack([lax.axis_index("row"), lax.axis_index("col")]).astype(jnp.int32)
    whole = (N // LANES, LANES)
    held, send = call(start_kernel, [matrix.shape, (16, 2, 4, LANES)], matrix)
    recv = exchange(send, "col")
    send, piece = call(first_kernel, [(32, 4, 4, LANES), (4, LANES)], ids, held, recv)
    recv = exchange(send, "row")
    qs, aqs, scals = {}, {}, {}
    for step in range(2, 9):
        args = [ids, held, recv]
        if step in (2, 3):
            args.append(piece)
        if step > 2:
            args.append(scals[step - 2])
        args += [qs[i] for i in range(1, step - 1)] + [aqs[i] for i in range(1, step - 2)]
        groups = 4 if step in (2, 3) else 3
        outs = [(16 if step % 2 == 0 else 32, groups, 4, LANES), whole]
        if step > 2:
            outs.append(whole)
        outs.append((16, LANES))
        if step in (3, 4):
            outs.append((32 if step == 3 else 64, LANES))
        if step == 2:
            outs.append((4, LANES))
        result = list(call(functools.partial(step_kernel, step), outs, *args))
        send = result.pop(0)
        qs[step - 1] = result.pop(0)
        if step > 2:
            aqs[step - 2] = result.pop(0)
        scals[step - 1] = result.pop(0)
        if step == 3:
            edge_r = result.pop(0)
        if step == 4:
            edge_c = result.pop(0)
        if step == 2:
            piece = packed = result.pop(0)
        recv = exchange(send, "col" if step % 2 == 0 else "row")
    (send,) = call(last_send_kernel, [(32, 1, 4, LANES)], recv)
    last = exchange(send, "row")
    qs[8], aqs[7], scals[8], factor, reflect = call(
        panel_kernel,
        [whole, whole, (16, LANES), (8, LANES), (8, matrix.shape[0])],
        ids,
        recv,
        *[scals[i] for i in range(1, 8)],
        *[qs[i] for i in range(1, 8)],
        *[aqs[i] for i in range(1, 7)],
        flops=40000000,
    )
    (trailing,) = call(
        trailing_kernel,
        [matrix.shape],
        ids,
        held,
        last,
        packed,
        edge_r,
        edge_c,
        factor,
        *[scals[i] for i in range(1, 9)],
        *[qs[i] for i in range(1, 9)],
        *[aqs[i] for i in range(1, 8)],
        scratch=[whole, (16, 512), (16, 1024)],
        pinned=False,
    )
    return trailing, reflect.T


def solution(mesh):
    placed = (P("row", "col"),)
    return jax.shard_map(
        local,
        mesh=mesh,
        in_specs=placed,
        out_specs=(P("row", "col"), P("row", None)),
        check_vma=False,
    )
```

```python
import functools

import jax
import jax.numpy as jnp
from jax import lax
from jax.experimental import pallas as pl
from jax.experimental.pallas import tpu as pltpu
from jax.sharding import PartitionSpec as P


N = 16384
COLS = 8
LANES = 128
F32 = jnp.float32
VMEM = pltpu.VMEM
LIMIT = 16 << 20


def places():
    return lax.axis_index("row"), lax.axis_index("col")


def total(x):
    return jnp.sum(jnp.sum(x, axis=0, keepdims=True), axis=1, keepdims=True)


def iota(shape, dim):
    return lax.broadcasted_iota(jnp.int32, shape, dim)


def without_first(x, owner):
    hit = (iota(x.shape, 0) == 0) & (iota(x.shape, 1) == 0)
    if owner is not None:
        hit = hit & (owner == 0)
    return jnp.where(hit, 0.0, x)


def times_rows(a_ref, x):
    upright = jnp.concatenate([x, jnp.zeros_like(x)], axis=0).T
    out = []
    for t in range(8):
        acc = jnp.zeros((8, LANES), F32)
        for q in range(4):
            block = a_ref[q * LANES : (q + 1) * LANES, t * LANES : (t + 1) * LANES]
            acc = acc + jnp.sum((block * upright[:, q : q + 1]).reshape(16, 8, LANES), axis=0)
        out.append(jnp.sum(acc, axis=0, keepdims=True))
    return jnp.concatenate(out, axis=0)


def times_cols(a_ref, x):
    out = []
    for q in range(4):
        acc = jnp.zeros((LANES, LANES), F32)
        for t in range(8):
            block = a_ref[q * LANES : (q + 1) * LANES, t * LANES : (t + 1) * LANES]
            acc = acc + block * x[t : t + 1, :]
        out.append(jnp.sum(acc.T, axis=0, keepdims=True))
    return jnp.concatenate(out, axis=0)


def send_all(send_ref, first, parts):
    for member in range(send_ref.shape[0]):
        for k, part in enumerate(parts):
            send_ref[member, first + k] = part


def halves(x):
    return [x[:4], x[4:]]


def along_cols(recv_ref):
    s = jnp.sum(recv_ref[:, 0:2], axis=0)
    return jnp.concatenate([s[0], s[1]], axis=0)


def along_rows(recv_ref):
    return jnp.sum(recv_ref[:, 0], axis=0)


def whole_from_rows(recv_ref, group):
    return jnp.concatenate([recv_ref[r, group] for r in range(recv_ref.shape[0])], axis=0)


def whole_from_cols(recv_ref, group):
    return jnp.concatenate(
        [recv_ref[c, group + k] for c in range(recv_ref.shape[0]) for k in range(2)], axis=0
    )


def start_kernel(a_ref, send_ref, slab_ref, sem):
    copy = pltpu.make_async_copy(a_ref.at[:, pl.ds(0, LANES)], slab_ref, sem)
    copy.start()
    copy.wait()
    left = [slab_ref[q * LANES : (q + 1) * LANES, :].T for q in range(4)]
    column = jnp.concatenate([x[0:1] for x in left], axis=0)
    corner = slab_ref[0:16, :]
    packed = jnp.zeros((1, LANES), F32)
    for j in range(COLS):
        lanes = iota((1, LANES), 1)
        entry = jnp.where(lanes < 16, corner[j + 1 : j + 2], 0.0)
        packed = packed + (pltpu.roll(entry, 16 * j, 1) if j else entry)
    blank = jnp.zeros((1, LANES), F32)
    for member in range(16):
        j, half = member // 2, member % 2
        rows = [left[2 * half + k][j + 1 : j + 2] for k in range(2)]
        send_ref[member, 0] = column
        send_ref[member, 1] = jnp.concatenate([*rows, packed, blank], axis=0)


def first_kernel(a_ref, recv_ref, send_ref, piece_ref):
    ids_ref = places()
    column = recv_ref[0, 0]
    piece_ref[...] = recv_ref[0, 1]
    packed = recv_ref[0, 1][2:3]
    send_all(send_ref, 0, halves(times_rows(a_ref, without_first(column, ids_ref[0]))))
    send_all(send_ref, 2, [column])
    blank = jnp.zeros((1, LANES), F32)
    for member in range(32):
        j, quarter = member // 4, member % 4
        rows = [
            a_ref[j + 1 : j + 2, (2 * quarter + k) * LANES : (2 * quarter + k + 1) * LANES]
            for k in range(2)
        ]
        send_ref[member, 3] = jnp.concatenate([*rows, packed, blank], axis=0)


def coefficient(scal, k):
    return scal[k : k + 1, 0:1]


def settle(step, y_whole, scal, qs, aqs):
    if step == 2:
        aq = None
        u = without_first(y_whole, None)
    else:
        aq = y_whole
        for i in range(1, step - 2):
            aq = aq - coefficient(scal, i) * aqs[i]
        aq = aq * coefficient(scal, 8)
        u = aq
        if step > 3:
            u = u - coefficient(scal, 0) * qs[step - 3]
        u = without_first(u, None)
    known = range(1, step - 1)
    rows = [jnp.sum(u * qs[i], axis=0, keepdims=True) for i in known]
    w = u
    cs = {}
    if rows:
        rows = rows + [jnp.zeros((1, LANES), F32)] * (8 - len(rows))
        sums = jnp.sum(jnp.concatenate(rows, axis=0), axis=1, keepdims=True)
        for i in known:
            cs[i] = sums[i - 1 : i, 0:1]
            w = w - cs[i] * qs[i]
    length = jnp.sqrt(total(w * w))
    inverse = 1.0 / length
    zero = jnp.zeros((1, LANES), F32)
    out = [zero + length] + [zero + cs[i] if i in cs else zero for i in range(1, 8)]
    out = out + [zero + inverse] + [zero] * 7
    return aq, w * inverse, length, inverse, cs, jnp.concatenate(out, axis=0)


def step_kernel(step, *refs):
    refs = list(refs)
    a_ref, recv_ref = refs[:2]
    del refs[:2]
    ids_ref = places()
    piece_ref = refs.pop(0) if step in (2, 3) else None
    scal = refs.pop(0)[...] if step > 2 else None
    q_refs = {i: refs.pop(0) for i in range(1, step - 1)}
    aq_refs = {i: refs.pop(0) for i in range(1, step - 2)}
    send_ref = refs.pop(0)
    q_ref = refs.pop(0)
    aq_ref = refs.pop(0) if step > 2 else None
    scal_ref = refs.pop(0)
    edge_ref = refs.pop(0) if step in (3, 4) else None
    new_piece_ref = refs.pop(0) if step == 2 else None

    even = step % 2 == 0
    if even:
        y_here = along_cols(recv_ref)
        y_whole = whole_from_rows(recv_ref, 2)
        chunk, rows = ids_ref[1], 8
    else:
        y_here = along_rows(recv_ref)
        y_whole = whole_from_cols(recv_ref, 1)
        chunk, rows = ids_ref[0], 4
    aq, q, length, inverse, cs, scal_out = settle(
        step,
        y_whole,
        scal,
        {i: r[...] for i, r in q_refs.items()},
        {i: r[...] for i, r in aq_refs.items()},
    )
    q_ref[...] = q
    scal_ref[...] = scal_out
    if aq_ref is not None:
        aq_ref[...] = aq
    at = pl.ds(chunk * rows, rows)
    here = y_here
    for i in cs:
        source = aq_ref if i == step - 2 else aq_refs[i]
        here = here - cs[i] * source[at, :]
    here = here * inverse
    if step > 2:
        here = here - length * q_refs[step - 2][at, :]
    here = without_first(here, chunk)
    if even:
        send_all(send_ref, 0, [times_cols(a_ref, here)])
        send_all(send_ref, 1, halves(y_here))
    else:
        send_all(send_ref, 0, halves(times_rows(a_ref, here)))
        send_all(send_ref, 2, [y_here])
    if step in (2, 3):
        send_all(send_ref, 3, [piece_ref[...]])
    if step == 2:
        new_piece_ref[...] = recv_ref[0, 3]
    if step == 3:
        edge_ref[...] = jnp.concatenate([recv_ref[c, 3][0:2] for c in range(16)], axis=0)
    if step == 4:
        edge_ref[...] = jnp.concatenate([recv_ref[r, 3][0:2] for r in range(32)], axis=0)


def last_send_kernel(recv_ref, send_ref):
    send_all(send_ref, 0, [along_rows(recv_ref)])


def sign(k):
    return -1.0 if k % 2 else 1.0


def product(x, y):
    return lax.dot_general(
        x,
        y,
        (((0,), (0,)), ((), ())),
        precision=lax.Precision.HIGHEST,
        preferred_element_type=F32,
    )


def rows_at(refs, row):
    return jnp.concatenate([sign(k) * refs[k][pl.ds(row, 1), :] for k in range(1, 9)], axis=0)


def d_tile(q_refs, row):
    lanes, ks = iota((8, LANES), 1), iota((8, LANES), 0)
    unit = jnp.where((lanes == ks + 1) & (row == 0), 1.0, 0.0)
    return unit - rows_at(q_refs, row)


def panel_kernel(*refs):
    refs = list(refs)
    ids_ref = places()
    refs.insert(0, None)
    recv_ref = refs[1]
    scal_refs = {i: refs[1 + i] for i in range(1, 8)}
    q_refs = {i: refs[8 + i] for i in range(1, 8)}
    aq_refs = {i: refs[15 + i] for i in range(1, 7)}
    q_out, aq_out, scal_out, factor_ref, reflect_ref = refs[22:27]
    y_whole = whole_from_cols(recv_ref, 1)
    aq, q, _, _, _, scal = settle(
        9,
        y_whole,
        scal_refs[7][...],
        {i: r[...] for i, r in q_refs.items()},
        {i: r[...] for i, r in aq_refs.items()},
    )
    q_out[...] = q
    aq_out[...] = aq
    scal_out[...] = scal
    q_refs[8] = q_out
    lanes, ks = iota((8, LANES), 1), iota((8, LANES), 0)
    top = d_tile(q_refs, 0)
    work = jnp.where(lanes < 8, pltpu.roll(top, LANES - 1, 1), 0.0)
    work = work + jnp.where(lanes == ks + 8, 1.0, 0.0)
    to_reflect = jnp.zeros((8, LANES), F32)
    for k in range(8):
        row = work[k : k + 1]
        beta = (scal if k == 7 else scal_refs[k + 1])[0:1, :]
        to_reflect = jnp.where(ks == k, row * beta, to_reflect)
        row = row / row[:, k : k + 1]
        column = jnp.where(ks == k, 0.0, work)[:, k : k + 1]
        work = jnp.where(ks == k, row, work - column * row)
    factor_ref[...] = jnp.where(lanes < 8, pltpu.roll(work, LANES - 8, 1), 0.0)
    to_reflect = jnp.where(lanes < 8, pltpu.roll(to_reflect, LANES - 8, 1), 0.0)
    for t in range(4):
        row = 4 * ids_ref[0] + t
        d = d_tile(q_refs, row)
        out = jnp.zeros((8, LANES), F32)
        for k in range(8):
            out = out + to_reflect[:, k : k + 1] * d[k : k + 1, :]
        out = jnp.where((row == 0) & (lanes <= ks), 0.0, out)
        reflect_ref[:, t * LANES : (t + 1) * LANES] = out


def trailing_kernel(*refs):
    refs = list(refs)
    ids_ref = places()
    refs.insert(0, None)
    a_ref, recv_ref, packed_ref, edge_r_ref, edge_c_ref, factor_ref = refs[1:7]
    scal_refs = {i: refs[6 + i] for i in range(1, 9)}
    q_refs = {i: refs[14 + i] for i in range(1, 9)}
    aq_refs = {i: refs[22 + i] for i in range(1, 8)}
    out_ref, last_ref, left_ref, right_ref = refs[30:34]
    scal = scal_refs[8][...]
    aq = whole_from_rows(recv_ref, 0)
    for i in range(1, 8):
        aq = aq - coefficient(scal, i) * aq_refs[i][...]
    aq = aq * coefficient(scal, 8)
    last_ref[...] = aq
    aq_refs[8] = last_ref
    lanes, ks = iota((8, LANES), 1), iota((8, LANES), 0)
    factor = factor_ref[...]
    inner = jnp.zeros((8, LANES), F32)
    packed = packed_ref[2:3]
    for j in range(8):
        entry = pltpu.roll(packed, LANES - 16 * j, 1) if j else packed
        inner = jnp.where(ks == j, entry, inner)
    inner = jnp.where((lanes >= 1) & (lanes <= 8), inner, 0.0)
    cross = rows_at(aq_refs, 0)
    cross = jnp.where((lanes >= 1) & (lanes <= 8), cross, 0.0)
    inner = pltpu.roll(inner - cross, LANES - 1, 1)
    cross = pltpu.roll(cross, LANES - 1, 1)
    square = jnp.concatenate([cross, jnp.zeros((LANES - 8, LANES), F32)], axis=0)
    inner = inner - square.T[0:8]
    for k in range(1, 9):
        if k < 8:
            alpha = scal_refs[k + 1][k : k + 1, :]
            beta = scal_refs[k + 1][0:1, :]
            near = ((ks == k - 1) & (lanes == k)) | ((ks == k) & (lanes == k - 1))
            inner = inner - jnp.where(near, beta, 0.0)
        else:
            alpha = total(q_refs[8][...] * aq)
        inner = inner + jnp.where((ks == k - 1) & (lanes == k - 1), alpha, 0.0)
    factor = factor[:, 0:8]
    inner = inner[:, 0:8]
    core = product(factor, product(inner, factor))

    def tiles(base, count, edge_ref):
        ds, ys = [], []
        for t in range(count):
            row = base + t
            d = d_tile(q_refs, row)
            edge = jnp.concatenate(
                [edge_ref[count * j + t : count * j + t + 1, :] for j in range(8)], axis=0
            )
            ad = edge - rows_at(aq_refs, row)
            ds.append(d)
            ys.append(product(factor, ad) - 0.5 * product(core, d))
        return ds, ys

    ds, ys = tiles(4 * ids_ref[0], 4, edge_r_ref)
    for t in range(4):
        left_ref[0:8, t * LANES : (t + 1) * LANES] = ds[t]
        left_ref[8:16, t * LANES : (t + 1) * LANES] = ys[t]
    ds, ys = tiles(8 * ids_ref[1], 8, edge_c_ref)
    for t in range(8):
        right_ref[0:8, t * LANES : (t + 1) * LANES] = ys[t]
        right_ref[8:16, t * LANES : (t + 1) * LANES] = ds[t]
    for q in range(4):
        at = slice(q * LANES, (q + 1) * LANES)
        out_ref[at, :] = a_ref[at, :] - product(left_ref[:, at], right_ref[...])


def call(kernel, outs, *args, scratch=(), pinned=True, flops=1000):
    return pl.pallas_call(
        kernel,
        out_shape=[VMEM(s, F32) if pinned else jax.ShapeDtypeStruct(s, F32) for s in outs],
        in_specs=[pl.BlockSpec(memory_space=VMEM)] * len(args),
        out_specs=[pl.BlockSpec(memory_space=VMEM)] * len(outs),
        scratch_shapes=[VMEM(s, F32) for s in scratch],
        compiler_params=pltpu.CompilerParams(vmem_limit_bytes=LIMIT),
        cost_estimate=pl.CostEstimate(flops=flops, bytes_accessed=1000, transcendentals=0),
    )(*args)


def exchange(x, axis):
    return lax.all_to_all(x, axis, 0, 0, tiled=True)


def local(matrix):
    whole = (N // LANES, LANES)
    send = pl.pallas_call(
        start_kernel,
        out_shape=VMEM((16, 2, 4, LANES), F32),
        in_specs=[pl.BlockSpec(memory_space=pltpu.HBM)],
        out_specs=pl.BlockSpec(memory_space=VMEM),
        scratch_shapes=[VMEM((matrix.shape[0], LANES), F32), pltpu.SemaphoreType.DMA],
        compiler_params=pltpu.CompilerParams(vmem_limit_bytes=LIMIT),
    )(pltpu.with_memory_space_constraint(matrix, pltpu.HBM))
    held = matrix
    recv = exchange(send, "col")
    send, piece = call(first_kernel, [(32, 4, 4, LANES), (4, LANES)], held, recv)
    recv = exchange(send, "row")
    qs, aqs, scals = {}, {}, {}
    for step in range(2, 9):
        args = [held, recv]
        if step in (2, 3):
            args.append(piece)
        if step > 2:
            args.append(scals[step - 2])
        args += [qs[i] for i in range(1, step - 1)] + [aqs[i] for i in range(1, step - 2)]
        groups = 4 if step in (2, 3) else 3
        outs = [(16 if step % 2 == 0 else 32, groups, 4, LANES), whole]
        if step > 2:
            outs.append(whole)
        outs.append((16, LANES))
        if step in (3, 4):
            outs.append((32 if step == 3 else 64, LANES))
        if step == 2:
            outs.append((4, LANES))
        result = list(call(functools.partial(step_kernel, step), outs, *args))
        send = result.pop(0)
        qs[step - 1] = result.pop(0)
        if step > 2:
            aqs[step - 2] = result.pop(0)
        scals[step - 1] = result.pop(0)
        if step == 3:
            edge_r = result.pop(0)
        if step == 4:
            edge_c = result.pop(0)
        if step == 2:
            piece = packed = result.pop(0)
        recv = exchange(send, "col" if step % 2 == 0 else "row")
    (send,) = call(last_send_kernel, [(32, 1, 4, LANES)], recv)
    last = exchange(send, "row")
    qs[8], aqs[7], scals[8], factor, reflect = call(
        panel_kernel,
        [whole, whole, (16, LANES), (8, LANES), (8, matrix.shape[0])],
        recv,
        *[scals[i] for i in range(1, 8)],
        *[qs[i] for i in range(1, 8)],
        *[aqs[i] for i in range(1, 7)],
        flops=40000000,
    )
    (trailing,) = call(
        trailing_kernel,
        [matrix.shape],
        held,
        last,
        packed,
        edge_r,
        edge_c,
        factor,
        *[scals[i] for i in range(1, 9)],
        *[qs[i] for i in range(1, 9)],
        *[aqs[i] for i in range(1, 8)],
        scratch=[whole, (16, 512), (16, 1024)],
        pinned=False,
    )
    return trailing, reflect.T


def solution(mesh):
    placed = (P("row", "col"),)
    return jax.shard_map(
        local,
        mesh=mesh,
        in_specs=placed,
        out_specs=(P("row", "col"), P("row", None)),
        check_vma=False,
    )
```

```python
import functools

import jax
import jax.numpy as jnp
from jax import lax
from jax.experimental import pallas as pl
from jax.experimental.pallas import tpu as pltpu
from jax.sharding import PartitionSpec as P


N = 16384
COLS = 8
LANES = 128
F32 = jnp.float32
VMEM = pltpu.VMEM
LIMIT = 16 << 20


def places():
    return lax.axis_index("row"), lax.axis_index("col")


def total(x):
    return jnp.sum(jnp.sum(x, axis=0, keepdims=True), axis=1, keepdims=True)


def iota(shape, dim):
    return lax.broadcasted_iota(jnp.int32, shape, dim)


def without_first(x, owner):
    hit = (iota(x.shape, 0) == 0) & (iota(x.shape, 1) == 0)
    if owner is not None:
        hit = hit & (owner == 0)
    return jnp.where(hit, 0.0, x)


def times_rows(a_ref, x):
    upright = jnp.concatenate([x, jnp.zeros_like(x)], axis=0).T
    out = []
    for t in range(8):
        acc = jnp.zeros((8, LANES), F32)
        for q in range(4):
            block = a_ref[q * LANES : (q + 1) * LANES, t * LANES : (t + 1) * LANES]
            acc = acc + jnp.sum((block * upright[:, q : q + 1]).reshape(16, 8, LANES), axis=0)
        out.append(jnp.sum(acc, axis=0, keepdims=True))
    return jnp.concatenate(out, axis=0)


def times_cols(a_ref, x):
    out = []
    for q in range(4):
        acc = jnp.zeros((LANES, LANES), F32)
        for t in range(8):
            block = a_ref[q * LANES : (q + 1) * LANES, t * LANES : (t + 1) * LANES]
            acc = acc + block * x[t : t + 1, :]
        out.append(jnp.sum(acc.T, axis=0, keepdims=True))
    return jnp.concatenate(out, axis=0)


def send_all(send_ref, first, parts):
    for member in range(send_ref.shape[0]):
        for k, part in enumerate(parts):
            send_ref[member, first + k] = part


def halves(x):
    return [x[:4], x[4:]]


def along_cols(recv_ref):
    s = jnp.sum(recv_ref[:, 0:2], axis=0)
    return jnp.concatenate([s[0], s[1]], axis=0)


def along_rows(recv_ref):
    return jnp.sum(recv_ref[:, 0], axis=0)


def whole_from_rows(recv_ref, group):
    return jnp.concatenate([recv_ref[r, group] for r in range(recv_ref.shape[0])], axis=0)


def whole_from_cols(recv_ref, group):
    return jnp.concatenate(
        [recv_ref[c, group + k] for c in range(recv_ref.shape[0]) for k in range(2)], axis=0
    )


def start_kernel(a_ref, send_ref, slab_ref, sem):
    copy = pltpu.make_async_copy(a_ref.at[:, pl.ds(0, LANES)], slab_ref, sem)
    copy.start()
    copy.wait()
    left = [slab_ref[q * LANES : (q + 1) * LANES, :].T for q in range(4)]
    column = jnp.concatenate([x[0:1] for x in left], axis=0)
    corner = slab_ref[0:16, :]
    packed = jnp.zeros((1, LANES), F32)
    for j in range(COLS):
        lanes = iota((1, LANES), 1)
        entry = jnp.where(lanes < 16, corner[j + 1 : j + 2], 0.0)
        packed = packed + (pltpu.roll(entry, 16 * j, 1) if j else entry)
    blank = jnp.zeros((1, LANES), F32)
    for member in range(16):
        j, half = member // 2, member % 2
        rows = [left[2 * half + k][j + 1 : j + 2] for k in range(2)]
        send_ref[member, 0] = column
        send_ref[member, 1] = jnp.concatenate([*rows, packed, blank], axis=0)


def first_kernel(a_ref, recv_ref, send_ref, piece_ref):
    ids_ref = places()
    column = recv_ref[0, 0]
    piece_ref[...] = recv_ref[0, 1]
    packed = recv_ref[0, 1][2:3]
    send_all(send_ref, 0, halves(times_rows(a_ref, without_first(column, ids_ref[0]))))
    send_all(send_ref, 2, [column])
    blank = jnp.zeros((1, LANES), F32)
    for member in range(32):
        j, quarter = member // 4, member % 4
        rows = [
            a_ref[j + 1 : j + 2, (2 * quarter + k) * LANES : (2 * quarter + k + 1) * LANES]
            for k in range(2)
        ]
        send_ref[member, 3] = jnp.concatenate([*rows, packed, blank], axis=0)


def coefficient(scal, k):
    return scal[k : k + 1, 0:1]


def settle(step, y_whole, scal, qs, previous):
    if step == 2:
        aq = None
        u = without_first(y_whole, None)
    else:
        aq = y_whole
        if step > 3:
            aq = aq - coefficient(scal, step - 3) * previous
        aq = aq * coefficient(scal, 8)
        u = aq
        if step > 3:
            u = u - coefficient(scal, 0) * qs[step - 3]
        u = without_first(u, None)
    known = range(1, step - 1)
    rows = [jnp.sum(u * qs[i], axis=0, keepdims=True) for i in known]
    w = u
    cs = {}
    if rows:
        rows = rows + [jnp.zeros((1, LANES), F32)] * (8 - len(rows))
        sums = jnp.sum(jnp.concatenate(rows, axis=0), axis=1, keepdims=True)
        for i in known:
            cs[i] = sums[i - 1 : i, 0:1]
            w = w - cs[i] * qs[i]
    length = jnp.sqrt(total(w * w))
    inverse = 1.0 / length
    zero = jnp.zeros((1, LANES), F32)
    out = [zero + length] + [zero + cs[i] if i in cs else zero for i in range(1, 8)]
    out = out + [zero + inverse] + [zero] * 7
    return aq, w * inverse, length, inverse, cs, jnp.concatenate(out, axis=0)


def keep_rows(out_ref, ref):
    row_index, col_index = places()
    out_ref[0:4, :] = ref[pl.ds(4 * row_index, 4), :]
    out_ref[4:12, :] = ref[pl.ds(8 * col_index, 8), :]
    out_ref[12:13, :] = ref[0:1, :]


def step_kernel(step, *refs):
    refs = list(refs)
    a_ref, recv_ref = refs[:2]
    del refs[:2]
    ids_ref = places()
    piece_ref = refs.pop(0) if step in (2, 3) else None
    scal = refs.pop(0)[...] if step > 2 else None
    q_refs = {i: refs.pop(0) for i in range(1, step - 1)}
    previous_ref = refs.pop(0) if step > 3 else None
    send_ref = refs.pop(0)
    q_ref = refs.pop(0)
    aq_ref = refs.pop(0) if step > 2 else None
    aq_rows_ref = refs.pop(0) if step > 2 else None
    scal_ref = refs.pop(0)
    edge_ref = refs.pop(0) if step in (3, 4) else None
    new_piece_ref = refs.pop(0) if step == 2 else None

    even = step % 2 == 0
    if even:
        y_here = along_cols(recv_ref)
        y_whole = whole_from_rows(recv_ref, 2)
        chunk, rows = ids_ref[1], 8
    else:
        y_here = along_rows(recv_ref)
        y_whole = whole_from_cols(recv_ref, 1)
        chunk, rows = ids_ref[0], 4
    aq, q, length, inverse, cs, scal_out = settle(
        step,
        y_whole,
        scal,
        {i: r[...] for i, r in q_refs.items()},
        previous_ref[...] if step > 3 else None,
    )
    q_ref[...] = q
    scal_ref[...] = scal_out
    if aq_ref is not None:
        aq_ref[...] = aq
        keep_rows(aq_rows_ref, aq_ref)
    at = pl.ds(chunk * rows, rows)
    here = y_here
    if step > 2:
        here = here - cs[step - 2] * aq_ref[at, :]
    here = here * inverse
    if step > 2:
        here = here - length * q_refs[step - 2][at, :]
    here = without_first(here, chunk)
    if even:
        send_all(send_ref, 0, [times_cols(a_ref, here)])
        send_all(send_ref, 1, halves(y_here))
    else:
        send_all(send_ref, 0, halves(times_rows(a_ref, here)))
        send_all(send_ref, 2, [y_here])
    if step in (2, 3):
        send_all(send_ref, 3, [piece_ref[...]])
    if step == 2:
        new_piece_ref[...] = recv_ref[0, 3]
    if step == 3:
        edge_ref[...] = jnp.concatenate([recv_ref[c, 3][0:2] for c in range(16)], axis=0)
    if step == 4:
        edge_ref[...] = jnp.concatenate([recv_ref[r, 3][0:2] for r in range(32)], axis=0)


def last_send_kernel(recv_ref, send_ref):
    send_all(send_ref, 0, [along_rows(recv_ref)])


def sign(k):
    return -1.0 if k % 2 else 1.0


def product(x, y):
    return lax.dot_general(
        x,
        y,
        (((0,), (0,)), ((), ())),
        precision=lax.Precision.HIGHEST,
        preferred_element_type=F32,
    )


def rows_at(refs, row):
    blank = jnp.zeros((1, LANES), F32)
    return jnp.concatenate(
        [sign(k) * refs[k][pl.ds(row, 1), :] if k in refs else blank for k in range(1, 9)], axis=0
    )


def d_tile(q_refs, row):
    lanes, ks = iota((8, LANES), 1), iota((8, LANES), 0)
    unit = jnp.where((lanes == ks + 1) & (row == 0), 1.0, 0.0)
    return unit - rows_at(q_refs, row)


def three(x):
    high = x.astype(jnp.bfloat16).astype(F32)
    middle = (x - high).astype(jnp.bfloat16).astype(F32)
    low = (x - high - middle).astype(jnp.bfloat16).astype(F32)
    return high, middle, low


def panel_kernel(*refs):
    row_index, col_index = places()
    refs = list(refs)
    refs.insert(0, None)
    recv_ref, packed_ref, edge_r_ref, edge_c_ref = refs[1:5]
    scal_refs = {i: refs[4 + i] for i in range(1, 8)}
    q_refs = {i: refs[11 + i] for i in range(1, 8)}
    aq_rows = {i: refs[18 + i] for i in range(1, 7)}
    previous_ref = refs[25]
    q_out, rest_out, reflect_ref, side_ref, left_ref, right_ref, aq_out, rows_out = refs[26:34]
    y_whole = whole_from_cols(recv_ref, 1)
    aq, q, _, _, cs, scal = settle(
        9,
        y_whole,
        scal_refs[7][...],
        {i: r[...] for i, r in q_refs.items()},
        previous_ref[...],
    )
    q_out[...] = q
    aq_out[...] = aq
    side_ref[96:104, :] = scal[8:16]
    q_refs[8] = q_out
    keep_rows(rows_out, aq_out)
    aq_rows[7] = rows_out
    rest_out[...] = cs[7] * aq
    lanes, ks = iota((8, LANES), 1), iota((8, LANES), 0)
    top = d_tile(q_refs, 0)
    work = jnp.where(lanes < 8, pltpu.roll(top, LANES - 1, 1), 0.0)
    work = work + jnp.where(lanes == ks + 8, 1.0, 0.0)
    to_reflect = jnp.zeros((8, LANES), F32)
    for k in range(8):
        row = work[k : k + 1]
        beta = (scal if k == 7 else scal_refs[k + 1])[0:1, :]
        to_reflect = jnp.where(ks == k, row * beta, to_reflect)
        row = row / row[:, k : k + 1]
        column = jnp.where(ks == k, 0.0, work)[:, k : k + 1]
        work = jnp.where(ks == k, row, work - column * row)
    factor = pltpu.roll(work, LANES - 8, 1)[:, 0:8]
    flipped = jnp.concatenate(
        [jnp.where(lanes < 8, pltpu.roll(work, LANES - 8, 1), 0.0), jnp.zeros((LANES - 8, LANES), F32)],
        axis=0,
    ).T[0:8, 0:8]
    to_reflect = jnp.where(lanes < 8, pltpu.roll(to_reflect, LANES - 8, 1), 0.0)
    inner = jnp.zeros((8, LANES), F32)
    packed = packed_ref[2:3]
    for k in range(8):
        entry = pltpu.roll(packed, LANES - 16 * k, 1) if k else packed
        inner = jnp.where(ks == k, entry, inner)
    used = (lanes >= 1) & (lanes <= 8)
    inner = jnp.where(used, inner, 0.0)
    cross = jnp.where(used, rows_at(aq_rows, 12), 0.0)
    inner = pltpu.roll(inner - cross, LANES - 1, 1)
    cross = pltpu.roll(cross, LANES - 1, 1)
    square = jnp.concatenate([cross, jnp.zeros((LANES - 8, LANES), F32)], axis=0)
    inner = inner - square.T[0:8]
    for k in range(1, 8):
        source = scal if k == 7 else scal_refs[k + 1]
        near = ((ks == k - 1) & (lanes == k)) | ((ks == k) & (lanes == k - 1))
        inner = inner - jnp.where(near, source[0:1, :], 0.0)
        inner = inner + jnp.where((ks == k - 1) & (lanes == k - 1), source[k : k + 1, :], 0.0)
    inner = inner[:, 0:8]
    core = product(factor, product(inner, factor))

    def tiles(base, count, edge_ref, first, kept):
        ds, ys = [], []
        for t in range(count):
            row = base + t
            d = d_tile(q_refs, row)
            edge = jnp.concatenate(
                [edge_ref[count * k + t : count * k + t + 1, :] for k in range(8)], axis=0
            )
            ad = edge - rows_at(aq_rows, kept + t)
            ds.append(d)
            ys.append(product(factor, ad) - 0.5 * product(core, d))
            side_ref[first + 8 * t : first + 8 * t + 8, :] = product(flipped, d)
        return ds, ys

    ds, ys = tiles(4 * row_index, 4, edge_r_ref, 0, 0)
    for t in range(4):
        high, middle, low = three(jnp.concatenate([ds[t], ys[t]], axis=0))
        stack = [high, high, middle, middle, high, low, jnp.zeros((32, LANES), F32)]
        at = slice(t * LANES, (t + 1) * LANES)
        left_ref[at, :] = jnp.concatenate(stack, axis=0).T.astype(jnp.bfloat16)
        out = jnp.zeros((8, LANES), F32)
        for k in range(8):
            out = out + to_reflect[:, k : k + 1] * ds[t][k : k + 1, :]
        out = jnp.where((4 * row_index + t == 0) & (lanes <= ks), 0.0, out)
        reflect_ref[:, t * LANES : (t + 1) * LANES] = out
    ds, ys = tiles(8 * col_index, 8, edge_c_ref, 32, 4)
    for t in range(8):
        high, middle, low = three(jnp.concatenate([ys[t], ds[t]], axis=0))
        stack = [high, middle, high, middle, low, high]
        at = slice(t * LANES, (t + 1) * LANES)
        right_ref[:, at] = jnp.concatenate(stack, axis=0).astype(jnp.bfloat16)


def trailing_kernel(
    a_ref, recv_ref, q_ref, rest_ref, side_ref, left_ref, right_ref, out_ref, last_ref, block_ref, sems,
):
    row_index, col_index = places()
    aq = (whole_from_rows(recv_ref, 0) - rest_ref[...]) * coefficient(side_ref, 96)
    last_ref[...] = aq
    alpha = total(q_ref[...] * aq)
    lanes = iota((1, LANES), 1)
    shifted = pltpu.roll(aq[0:1, :], LANES - 1, 1)
    added = jnp.where(lanes == 7, 0.5 * alpha, 0.0) - jnp.where(lanes < 8, shifted, 0.0)
    added = jnp.concatenate([added, jnp.zeros((7, LANES), F32)], axis=0).T[0:8, 0:1]

    def last(base, count, first):
        return [
            -last_ref[pl.ds(base + t, 1), :]
            - jnp.sum(added * side_ref[first + 8 * t : first + 8 * t + 8, :], axis=0, keepdims=True)
            for t in range(count)
        ]

    ws_r = last(4 * row_index, 4, 0)
    ws_c = last(8 * col_index, 8, 32)
    blank = jnp.zeros((6, LANES), F32)
    copies = []
    for q in range(4):
        at = slice(q * LANES, (q + 1) * LANES)
        upright = jnp.concatenate([side_ref[8 * q + 7 : 8 * q + 8, :], ws_r[q], blank], axis=0).T
        change = jnp.dot(left_ref[at, 0:96], right_ref[...], preferred_element_type=F32)
        for t in range(8):
            to = slice(t * LANES, (t + 1) * LANES)
            block_ref[at, to] = (
                a_ref[at, to]
                - change[:, to]
                - upright[:, 0:1] * ws_c[t]
                - upright[:, 1:2] * side_ref[39 + 8 * t : 40 + 8 * t, :]
            )
        copy = pltpu.make_async_copy(block_ref.at[at, :], out_ref.at[at, :], sems.at[q])
        copy.start()
        copies.append(copy)
    for copy in copies:
        copy.wait()


def call(kernel, outs, *args, scratch=(), pinned=True, flops=1000):
    def shape(x):
        if not isinstance(x, tuple):
            return x
        return VMEM(x, F32) if pinned else jax.ShapeDtypeStruct(x, F32)

    return pl.pallas_call(
        kernel,
        out_shape=[shape(x) for x in outs],
        in_specs=[pl.BlockSpec(memory_space=VMEM)] * len(args),
        out_specs=[pl.BlockSpec(memory_space=VMEM)] * len(outs),
        scratch_shapes=[VMEM(s, F32) for s in scratch],
        compiler_params=pltpu.CompilerParams(vmem_limit_bytes=LIMIT),
        cost_estimate=pl.CostEstimate(flops=flops, bytes_accessed=1000, transcendentals=0),
    )(*args)


def exchange(x, axis):
    return lax.all_to_all(x, axis, 0, 0, tiled=True)


def local(matrix):
    whole = (N // LANES, LANES)
    send = pl.pallas_call(
        start_kernel,
        out_shape=VMEM((16, 2, 4, LANES), F32),
        in_specs=[pl.BlockSpec(memory_space=pltpu.HBM)],
        out_specs=pl.BlockSpec(memory_space=VMEM),
        scratch_shapes=[VMEM((matrix.shape[0], LANES), F32), pltpu.SemaphoreType.DMA],
        compiler_params=pltpu.CompilerParams(vmem_limit_bytes=LIMIT),
    )(pltpu.with_memory_space_constraint(matrix, pltpu.HBM))
    held = matrix
    recv = exchange(send, "col")
    send, piece = call(first_kernel, [(32, 4, 4, LANES), (4, LANES)], held, recv)
    recv = exchange(send, "row")
    qs, aq_rows, scals, previous = {}, {}, {}, None
    for step in range(2, 9):
        args = [held, recv]
        if step in (2, 3):
            args.append(piece)
        if step > 2:
            args.append(scals[step - 2])
        args += [qs[i] for i in range(1, step - 1)]
        if step > 3:
            args.append(previous)
        groups = 4 if step in (2, 3) else 3
        outs = [(16 if step % 2 == 0 else 32, groups, 4, LANES), whole]
        if step > 2:
            outs += [whole, (16, LANES)]
        outs.append((16, LANES))
        if step in (3, 4):
            outs.append((32 if step == 3 else 64, LANES))
        if step == 2:
            outs.append((4, LANES))
        result = list(call(functools.partial(step_kernel, step), outs, *args))
        send = result.pop(0)
        qs[step - 1] = result.pop(0)
        if step > 2:
            previous = result.pop(0)
            aq_rows[step - 2] = result.pop(0)
        scals[step - 1] = result.pop(0)
        if step == 3:
            edge_r = result.pop(0)
        if step == 4:
            edge_c = result.pop(0)
        if step == 2:
            piece = packed = result.pop(0)
        recv = exchange(send, "col" if step % 2 == 0 else "row")
    (send,) = call(last_send_kernel, [(32, 1, 4, LANES)], recv)
    last = exchange(send, "row")
    rows, cols = matrix.shape
    q, rest, reflect, side, left, right = call(
        panel_kernel,
        [whole, whole, (8, rows), (104, LANES)]
        + [VMEM((rows, LANES), jnp.bfloat16), VMEM((96, cols), jnp.bfloat16)],
        recv,
        packed,
        edge_r,
        edge_c,
        *[scals[i] for i in range(1, 8)],
        *[qs[i] for i in range(1, 8)],
        *[aq_rows[i] for i in range(1, 7)],
        previous,
        scratch=[whole, (16, LANES)],
        flops=40000000,
    )
    trailing = pl.pallas_call(
        trailing_kernel,
        out_shape=jax.ShapeDtypeStruct(matrix.shape, F32),
        in_specs=[pl.BlockSpec(memory_space=VMEM)] * 7,
        out_specs=pl.BlockSpec(memory_space=pltpu.HBM),
        scratch_shapes=[VMEM(whole, F32), VMEM(matrix.shape, F32), pltpu.SemaphoreType.DMA((4,))],
        compiler_params=pltpu.CompilerParams(vmem_limit_bytes=LIMIT),
    )(held, last, q, rest, side, left, right)
    return trailing, reflect.T


def solution(mesh):
    placed = (P("row", "col"),)
    return jax.shard_map(
        local,
        mesh=mesh,
        in_specs=placed,
        out_specs=(P("row", "col"), P("row", None)),
        check_vma=False,
    )
```

```python
import functools

import jax
import jax.numpy as jnp
from jax import lax
from jax.experimental import pallas as pl
from jax.experimental.pallas import tpu as pltpu
from jax.sharding import PartitionSpec as P


N = 16384
COLS = 8
LANES = 128
F32 = jnp.float32
VMEM = pltpu.VMEM
LIMIT = 16 << 20
GUARD = False
GROWTH = 16.0
PIVOT = 0.05


def places():
    return lax.axis_index("row"), lax.axis_index("col")


def total(x):
    return jnp.sum(jnp.sum(x, axis=0, keepdims=True), axis=1, keepdims=True)


def iota(shape, dim):
    return lax.broadcasted_iota(jnp.int32, shape, dim)


def without_first(x, owner):
    hit = (iota(x.shape, 0) == 0) & (iota(x.shape, 1) == 0)
    if owner is not None:
        hit = hit & (owner == 0)
    return jnp.where(hit, 0.0, x)


def times_rows(a_ref, x):
    upright = jnp.concatenate([x, jnp.zeros_like(x)], axis=0).T
    out = []
    for t in range(8):
        acc = jnp.zeros((8, LANES), F32)
        for q in range(4):
            block = a_ref[q * LANES : (q + 1) * LANES, t * LANES : (t + 1) * LANES]
            acc = acc + jnp.sum((block * upright[:, q : q + 1]).reshape(16, 8, LANES), axis=0)
        out.append(jnp.sum(acc, axis=0, keepdims=True))
    return jnp.concatenate(out, axis=0)


def times_cols(a_ref, x):
    out = []
    for q in range(4):
        acc = jnp.zeros((LANES, LANES), F32)
        for t in range(8):
            block = a_ref[q * LANES : (q + 1) * LANES, t * LANES : (t + 1) * LANES]
            acc = acc + block * x[t : t + 1, :]
        out.append(jnp.sum(acc.T, axis=0, keepdims=True))
    return jnp.concatenate(out, axis=0)


def send_all(send_ref, first, parts):
    for member in range(send_ref.shape[0]):
        for k, part in enumerate(parts):
            send_ref[member, first + k] = part


def halves(x):
    return [x[:4], x[4:]]


def along_cols(recv_ref):
    s = jnp.sum(recv_ref[:, 0:2], axis=0)
    return jnp.concatenate([s[0], s[1]], axis=0)


def along_rows(recv_ref):
    return jnp.sum(recv_ref[:, 0], axis=0)


def whole_from_rows(recv_ref, group):
    return jnp.concatenate([recv_ref[r, group] for r in range(recv_ref.shape[0])], axis=0)


def whole_from_cols(recv_ref, group):
    return jnp.concatenate(
        [recv_ref[c, group + k] for c in range(recv_ref.shape[0]) for k in range(2)], axis=0
    )


def start_kernel(a_ref, send_ref, slab_ref, sem):
    copy = pltpu.make_async_copy(a_ref.at[:, pl.ds(0, LANES)], slab_ref, sem)
    copy.start()
    copy.wait()
    left = [slab_ref[q * LANES : (q + 1) * LANES, :].T for q in range(4)]
    column = jnp.concatenate([x[0:1] for x in left], axis=0)
    corner = slab_ref[0:16, :]
    packed = jnp.zeros((1, LANES), F32)
    for j in range(COLS):
        lanes = iota((1, LANES), 1)
        entry = jnp.where(lanes < 16, corner[j + 1 : j + 2], 0.0)
        packed = packed + (pltpu.roll(entry, 16 * j, 1) if j else entry)
    blank = jnp.zeros((1, LANES), F32)
    for member in range(16):
        j, half = member // 2, member % 2
        rows = [left[2 * half + k][j + 1 : j + 2] for k in range(2)]
        send_ref[member, 0] = column
        send_ref[member, 1] = jnp.concatenate([*rows, packed, blank], axis=0)


def first_kernel(a_ref, recv_ref, send_ref, piece_ref):
    ids_ref = places()
    column = recv_ref[0, 0]
    piece_ref[...] = recv_ref[0, 1]
    packed = recv_ref[0, 1][2:3]
    send_all(send_ref, 0, halves(times_rows(a_ref, without_first(column, ids_ref[0]))))
    send_all(send_ref, 2, [column])
    blank = jnp.zeros((1, LANES), F32)
    for member in range(32):
        j, quarter = member // 4, member % 4
        rows = [
            a_ref[j + 1 : j + 2, (2 * quarter + k) * LANES : (2 * quarter + k + 1) * LANES]
            for k in range(2)
        ]
        send_ref[member, 3] = jnp.concatenate([*rows, packed, blank], axis=0)


def coefficient(scal, k):
    return scal[k : k + 1, 0:1]


def settle(step, given, scal, qs):
    u = without_first(given, None) if step == 2 else given
    zero = jnp.zeros((1, LANES), F32)
    w, cs, growth = u, {}, zero + 1.0
    if step == 2:
        alpha = shift = given[0:1, 0:1]
    else:
        known = range(1, step - 1)
        rows = [jnp.sum(u * qs[i], axis=0, keepdims=True) for i in known]
        rows = rows + [zero] * (8 - len(rows))
        sums = jnp.sum(jnp.concatenate(rows, axis=0), axis=1, keepdims=True)
        for i in known:
            cs[i] = sums[i - 1 : i, 0:1]
            w = w - cs[i] * qs[i]
        growth = jnp.sum(sums * sums, axis=0, keepdims=True)
        alpha, before = cs[step - 2] + coefficient(scal, 9), coefficient(scal, 10)
        smaller = jnp.where(jnp.abs(alpha) < jnp.abs(before), alpha, before)
        shift = jnp.where(alpha * before > 0.0, smaller, 0.0)
    length = jnp.sqrt(total(w * w))
    inverse = 1.0 / length
    if step > 2:
        growth = coefficient(scal, 11) * (1.0 + growth * inverse * inverse)
    out = [zero + length] + [zero + cs[i] if i in cs else zero for i in range(1, 8)]
    out = out + [zero + x for x in (inverse, shift, alpha, growth)] + [zero] * 4
    return w * inverse, length, inverse, shift, cs, jnp.concatenate(out, axis=0)


def given_rows(recv_ref, by_rows):
    row_index, col_index = places()
    if by_rows:
        group = recv_ref.shape[1] - 1 if recv_ref.shape[1] < 3 else 2
        here = recv_ref[row_index, group]
        there = [recv_ref[2 * col_index + k, group] for k in range(2)]
        first = recv_ref[0, group][0:1]
    else:
        here = recv_ref[row_index // 2, 1 + row_index % 2]
        there = [recv_ref[col_index, 1 + k] for k in range(2)]
        first = recv_ref[0, 1][0:1]
    return jnp.concatenate([here, *there, first, jnp.zeros((3, LANES), F32)], axis=0)


def kept_rows(ref):
    row_index, col_index = places()
    here, there = ref[pl.ds(4 * row_index, 4), :], ref[pl.ds(8 * col_index, 8), :]
    return jnp.concatenate([here, there, ref[0:1, :], jnp.zeros((3, LANES), F32)], axis=0)


def product_rows(step, recv_ref, scal, q_refs):
    out = given_rows(recv_ref, step % 2 == 0)
    out = out + coefficient(scal, 9) * kept_rows(q_refs[step - 2])
    if step > 3:
        return out + coefficient(scal, 0) * kept_rows(q_refs[step - 3])
    row_index, col_index = places()
    rows, lanes = iota(out.shape, 0), iota(out.shape, 1)
    start = ((rows == 0) & (row_index == 0)) | ((rows == 4) & (col_index == 0)) | (rows == 12)
    return out + jnp.where(start & (lanes == 0), coefficient(scal, 0), 0.0)


def step_kernel(step, *refs):
    refs = list(refs)
    a_ref, recv_ref = refs[:2]
    del refs[:2]
    row_index, col_index = places()
    piece_ref = refs.pop(0) if step in (2, 3) else None
    scal = refs.pop(0)[...] if step > 2 else None
    q_refs = {i: refs.pop(0) for i in range(1, step - 1)}
    rows_refs = {i: refs.pop(0) for i in range(1, step - 2)}
    send_ref = refs.pop(0)
    q_ref = refs.pop(0)
    if step > 2:
        rows_refs[step - 2] = refs.pop(0)
    scal_ref = refs.pop(0)
    edge_ref = refs.pop(0) if step in (3, 4) else None
    new_piece_ref = refs.pop(0) if step == 2 else None

    even = step % 2 == 0
    if even:
        y_here, given = along_cols(recv_ref), whole_from_rows(recv_ref, 2)
        chunk, count, part = col_index, 8, slice(4, 12)
    else:
        y_here, given = along_rows(recv_ref), whole_from_cols(recv_ref, 1)
        chunk, count, part = row_index, 4, slice(0, 4)
    if step > 2:
        rows_refs[step - 2][...] = product_rows(step, recv_ref, scal, q_refs)
    q, length, inverse, shift, cs, scal_out = settle(
        step, given, scal, {i: r[...] for i, r in q_refs.items()}
    )
    q_ref[...] = q
    scal_ref[...] = scal_out
    at = pl.ds(chunk * count, count)
    here = y_here
    for i in cs:
        here = here - cs[i] * rows_refs[i][part, :]
    here = here * inverse - shift * q_ref[at, :]
    if step > 2:
        here = here - length * q_refs[step - 2][at, :]
    here = without_first(here, chunk)
    if even:
        send_all(send_ref, 0, [times_cols(a_ref, here)])
        send_all(send_ref, 1, halves(here))
    else:
        send_all(send_ref, 0, halves(times_rows(a_ref, here)))
        send_all(send_ref, 2, [here])
    if step in (2, 3):
        send_all(send_ref, 3, [piece_ref[...]])
    if step == 2:
        new_piece_ref[...] = recv_ref[0, 3]
    if step == 3:
        edge_ref[...] = jnp.concatenate([recv_ref[c, 3][0:2] for c in range(16)], axis=0)
    if step == 4:
        edge_ref[...] = jnp.concatenate([recv_ref[r, 3][0:2] for r in range(32)], axis=0)


def last_send_kernel(recv_ref, send_ref):
    send_all(send_ref, 0, [along_rows(recv_ref)])


def sign(k):
    return -1.0 if k % 2 else 1.0


def product(x, y):
    return lax.dot_general(
        x,
        y,
        (((0,), (0,)), ((), ())),
        precision=lax.Precision.HIGHEST,
        preferred_element_type=F32,
    )


def rows_at(refs, row):
    blank = jnp.zeros((1, LANES), F32)
    return jnp.concatenate(
        [sign(k) * refs[k][pl.ds(row, 1), :] if k in refs else blank for k in range(1, 9)], axis=0
    )


def d_tile(q_refs, row):
    lanes, ks = iota((8, LANES), 1), iota((8, LANES), 0)
    unit = jnp.where((lanes == ks + 1) & (row == 0), 1.0, 0.0)
    return unit - rows_at(q_refs, row)


def three(x):
    high = x.astype(jnp.bfloat16).astype(F32)
    middle = (x - high).astype(jnp.bfloat16).astype(F32)
    low = (x - high - middle).astype(jnp.bfloat16).astype(F32)
    return high, middle, low


def panel_kernel(*refs):
    row_index, col_index = places()
    refs = list(refs)
    refs.insert(0, None)
    recv_ref, packed_ref, edge_r_ref, edge_c_ref = refs[1:5]
    scal_refs = {i: refs[4 + i] for i in range(1, 8)}
    q_refs = {i: refs[11 + i] for i in range(1, 8)}
    aq_rows = {i: refs[18 + i] for i in range(1, 7)}
    q_out, flag_ref, reflect_ref, side_ref, left_ref, right_ref, rows_out = refs[25:32]
    q, length, _, _, cs, scal = settle(
        9, whole_from_cols(recv_ref, 1), scal_refs[7][...], {i: r[...] for i, r in q_refs.items()}
    )
    q_out[...] = q
    rows_out[...] = product_rows(9, recv_ref, scal_refs[7][...], q_refs)
    aq_rows[7] = rows_out
    rest = jnp.zeros((16, LANES), F32)
    for i in range(1, 8):
        rest = rest + cs[i] * aq_rows[i][...]
    side_ref[96:104, :] = scal[8:16]
    side_ref[104:120, :] = rest
    side_ref[120:128, :] = jnp.zeros((8, LANES), F32) + cs[7] * length
    q_refs[8] = q_out
    lanes, ks = iota((8, LANES), 1), iota((8, LANES), 0)
    top = d_tile(q_refs, 0)
    work = jnp.where(lanes < 8, pltpu.roll(top, LANES - 1, 1), 0.0)
    work = work + jnp.where(lanes == ks + 8, 1.0, 0.0)
    to_reflect = jnp.zeros((8, LANES), F32)
    pivot = jnp.ones((1, 1), F32)
    for k in range(8):
        row = work[k : k + 1]
        pivot = jnp.minimum(pivot, row[:, k : k + 1])
        beta = (scal if k == 7 else scal_refs[k + 1])[0:1, :]
        to_reflect = jnp.where(ks == k, row * beta, to_reflect)
        row = row / row[:, k : k + 1]
        column = jnp.where(ks == k, 0.0, work)[:, k : k + 1]
        work = jnp.where(ks == k, row, work - column * row)
    sound = (scal[11:12, 0:1] <= GROWTH) & (pivot >= PIVOT)
    flag_ref[...] = jnp.zeros((8, LANES), F32) + jnp.where(sound, 1.0, 0.0)
    factor = pltpu.roll(work, LANES - 8, 1)[:, 0:8]
    flipped = jnp.concatenate(
        [jnp.where(lanes < 8, pltpu.roll(work, LANES - 8, 1), 0.0), jnp.zeros((LANES - 8, LANES), F32)],
        axis=0,
    ).T[0:8, 0:8]
    to_reflect = jnp.where(lanes < 8, pltpu.roll(to_reflect, LANES - 8, 1), 0.0)
    inner = jnp.zeros((8, LANES), F32)
    packed = packed_ref[2:3]
    for k in range(8):
        entry = pltpu.roll(packed, LANES - 16 * k, 1) if k else packed
        inner = jnp.where(ks == k, entry, inner)
    used = (lanes >= 1) & (lanes <= 8)
    inner = jnp.where(used, inner, 0.0)
    cross = jnp.where(used, rows_at(aq_rows, 12), 0.0)
    inner = pltpu.roll(inner - cross, LANES - 1, 1)
    cross = pltpu.roll(cross, LANES - 1, 1)
    square = jnp.concatenate([cross, jnp.zeros((LANES - 8, LANES), F32)], axis=0)
    inner = inner - square.T[0:8]
    for k in range(1, 8):
        source = scal if k == 7 else scal_refs[k + 1]
        near = ((ks == k - 1) & (lanes == k)) | ((ks == k) & (lanes == k - 1))
        inner = inner - jnp.where(near, source[0:1, :], 0.0)
        alpha = source[10:11, :]
        inner = inner + jnp.where((ks == k - 1) & (lanes == k - 1), alpha, 0.0)
    inner = inner[:, 0:8]
    core = product(factor, product(inner, factor))

    def tiles(base, count, edge_ref, first, kept):
        ds, ys = [], []
        for t in range(count):
            row = base + t
            d = d_tile(q_refs, row)
            edge = jnp.concatenate(
                [edge_ref[count * k + t : count * k + t + 1, :] for k in range(8)], axis=0
            )
            ad = edge - rows_at(aq_rows, kept + t)
            ds.append(d)
            ys.append(product(factor, ad) - 0.5 * product(core, d))
            side_ref[first + 8 * t : first + 8 * t + 8, :] = product(flipped, d)
        return ds, ys

    ds, ys = tiles(4 * row_index, 4, edge_r_ref, 0, 0)
    for t in range(4):
        high, middle, low = three(jnp.concatenate([ds[t], ys[t]], axis=0))
        stack = [high, high, middle, middle, high, low, jnp.zeros((32, LANES), F32)]
        at = slice(t * LANES, (t + 1) * LANES)
        left_ref[at, :] = jnp.concatenate(stack, axis=0).T.astype(jnp.bfloat16)
        out = jnp.zeros((8, LANES), F32)
        for k in range(8):
            out = out + to_reflect[:, k : k + 1] * ds[t][k : k + 1, :]
        out = jnp.where((4 * row_index + t == 0) & (lanes <= ks), 0.0, out)
        reflect_ref[:, t * LANES : (t + 1) * LANES] = out
    ds, ys = tiles(8 * col_index, 8, edge_c_ref, 32, 4)
    for t in range(8):
        high, middle, low = three(jnp.concatenate([ys[t], ds[t]], axis=0))
        stack = [high, middle, high, middle, low, high]
        at = slice(t * LANES, (t + 1) * LANES)
        right_ref[:, at] = jnp.concatenate(stack, axis=0).astype(jnp.bfloat16)


def trailing_kernel(
    a_ref, recv_ref, q_ref, side_ref, left_ref, right_ref, out_ref, block_ref, sems
):
    inverse = coefficient(side_ref, 96)
    aq = (given_rows(recv_ref, True) - side_ref[104:120, :]) * inverse
    alpha = total(q_ref[...] * whole_from_rows(recv_ref, 0)) - coefficient(side_ref, 120)
    alpha = alpha * inverse
    lanes = iota((1, LANES), 1)
    shifted = pltpu.roll(aq[12:13, :], LANES - 1, 1)
    added = jnp.where(lanes == 7, 0.5 * alpha, 0.0) - jnp.where(lanes < 8, shifted, 0.0)
    added = jnp.concatenate([added, jnp.zeros((7, LANES), F32)], axis=0).T[0:8, 0:1]

    def last(count, first, kept):
        return [
            -aq[kept + t : kept + t + 1, :]
            - jnp.sum(added * side_ref[first + 8 * t : first + 8 * t + 8, :], axis=0, keepdims=True)
            for t in range(count)
        ]

    ws_r = last(4, 0, 0)
    ws_c = last(8, 32, 4)
    blank = jnp.zeros((6, LANES), F32)
    copies = []
    for q in range(4):
        at = slice(q * LANES, (q + 1) * LANES)
        upright = jnp.concatenate([side_ref[8 * q + 7 : 8 * q + 8, :], ws_r[q], blank], axis=0).T
        change = jnp.dot(left_ref[at, 0:96], right_ref[...], preferred_element_type=F32)
        for t in range(8):
            to = slice(t * LANES, (t + 1) * LANES)
            block_ref[at, to] = (
                a_ref[at, to]
                - change[:, to]
                - upright[:, 0:1] * ws_c[t]
                - upright[:, 1:2] * side_ref[39 + 8 * t : 40 + 8 * t, :]
            )
        copy = pltpu.make_async_copy(block_ref.at[at, :], out_ref.at[at, :], sems.at[q])
        copy.start()
        copies.append(copy)
    for copy in copies:
        copy.wait()


def call(kernel, outs, *args, scratch=(), pinned=True, flops=1000):
    def shape(x):
        if not isinstance(x, tuple):
            return x
        return VMEM(x, F32) if pinned else jax.ShapeDtypeStruct(x, F32)

    return pl.pallas_call(
        kernel,
        out_shape=[shape(x) for x in outs],
        in_specs=[pl.BlockSpec(memory_space=VMEM)] * len(args),
        out_specs=[pl.BlockSpec(memory_space=VMEM)] * len(outs),
        scratch_shapes=[VMEM(s, F32) for s in scratch],
        compiler_params=pltpu.CompilerParams(vmem_limit_bytes=LIMIT),
        cost_estimate=pl.CostEstimate(flops=flops, bytes_accessed=1000, transcendentals=0),
    )(*args)


def exchange(x, axis):
    return lax.all_to_all(x, axis, 0, 0, tiled=True)


def local(matrix):
    whole = (N // LANES, LANES)
    send = pl.pallas_call(
        start_kernel,
        out_shape=VMEM((16, 2, 4, LANES), F32),
        in_specs=[pl.BlockSpec(memory_space=pltpu.HBM)],
        out_specs=pl.BlockSpec(memory_space=VMEM),
        scratch_shapes=[VMEM((matrix.shape[0], LANES), F32), pltpu.SemaphoreType.DMA],
        compiler_params=pltpu.CompilerParams(vmem_limit_bytes=LIMIT),
    )(pltpu.with_memory_space_constraint(matrix, pltpu.HBM))
    held = matrix
    recv = exchange(send, "col")
    send, piece = call(first_kernel, [(32, 4, 4, LANES), (4, LANES)], held, recv)
    recv = exchange(send, "row")
    qs, aq_rows, scals = {}, {}, {}
    for step in range(2, 9):
        args = [held, recv]
        if step in (2, 3):
            args.append(piece)
        if step > 2:
            args.append(scals[step - 2])
        args += [qs[i] for i in range(1, step - 1)] + [aq_rows[i] for i in range(1, step - 2)]
        groups = 4 if step in (2, 3) else 3
        outs = [(16 if step % 2 == 0 else 32, groups, 4, LANES), whole]
        if step > 2:
            outs.append((16, LANES))
        outs.append((16, LANES))
        if step in (3, 4):
            outs.append((32 if step == 3 else 64, LANES))
        if step == 2:
            outs.append((4, LANES))
        result = list(call(functools.partial(step_kernel, step), outs, *args))
        send = result.pop(0)
        qs[step - 1] = result.pop(0)
        if step > 2:
            aq_rows[step - 2] = result.pop(0)
        scals[step - 1] = result.pop(0)
        if step == 3:
            edge_r = result.pop(0)
        if step == 4:
            edge_c = result.pop(0)
        if step == 2:
            piece = packed = result.pop(0)
        recv = exchange(send, "col" if step % 2 == 0 else "row")
    (send,) = call(last_send_kernel, [(32, 1, 4, LANES)], recv)
    last = exchange(send, "row")
    rows, cols = matrix.shape
    q, flag, reflect, side, left, right = call(
        panel_kernel,
        [whole, jax.ShapeDtypeStruct((8, LANES), F32), (8, rows), (128, LANES)]
        + [VMEM((rows, LANES), jnp.bfloat16), VMEM((96, cols), jnp.bfloat16)],
        recv,
        packed,
        edge_r,
        edge_c,
        *[scals[i] for i in range(1, 8)],
        *[qs[i] for i in range(1, 8)],
        *[aq_rows[i] for i in range(1, 7)],
        scratch=[(16, LANES)],
        flops=40000000,
    )
    trailing = pl.pallas_call(
        trailing_kernel,
        out_shape=jax.ShapeDtypeStruct(matrix.shape, F32),
        in_specs=[pl.BlockSpec(memory_space=VMEM)] * 6,
        out_specs=pl.BlockSpec(memory_space=pltpu.HBM),
        scratch_shapes=[VMEM(matrix.shape, F32), pltpu.SemaphoreType.DMA((4,))],
        compiler_params=pltpu.CompilerParams(vmem_limit_bytes=LIMIT),
    )(held, last, q, side, left, right)
    if not GUARD:
        return trailing, reflect.T
    kept = matrix
    _, trailing, reflect = lax.while_loop(
        lambda state: state[0] < 0.5,
        lambda state: (jnp.float32(1.0), *column_by_column(kept)),
        (flag[0, 0], trailing, reflect),
    )
    return trailing, reflect.T


def of_everyone(shard, axis):
    size = lax.axis_size(axis)
    return exchange(jnp.broadcast_to(shard[None], (size, *shard.shape)), axis)


def column_by_column(matrix):
    rows, cols = matrix.shape
    row_at, col_at = lax.axis_index("row") * rows, lax.axis_index("col") * cols
    panel = of_everyone(matrix[:, :COLS].T, "col")[0]
    panel = of_everyone(panel, "row").transpose(1, 0, 2).reshape(COLS, N)
    positions = jnp.arange(N, dtype=jnp.int32)

    def one(column, state):
        reflect, companion = state

        def row(x):
            return lax.dynamic_index_in_dim(x, column, 0, keepdims=False)

        def entries(x):
            return lax.dynamic_index_in_dim(x, column, 1, keepdims=True)

        current = row(panel) - jnp.sum(
            reflect * entries(companion) + companion * entries(reflect), axis=0
        )
        below = jnp.where(positions > column, current, 0.0)
        leading = jnp.sum(jnp.where(positions == column + 1, current, 0.0))
        length = jnp.sqrt(jnp.sum(below * below))
        vector = below + jnp.where(positions == column + 1, length, 0.0)
        scaling = 1.0 / (length * (length + leading))
        along_rows_here = lax.dynamic_slice_in_dim(vector, row_at, rows, 0)
        image = jnp.sum(matrix * along_rows_here[:, None], axis=0)
        image = of_everyone(image, "row").sum(axis=0)
        image = of_everyone(image, "col").reshape(N)
        to_reflect = jnp.sum(companion * vector, axis=1, keepdims=True)
        to_companion = jnp.sum(reflect * vector, axis=1, keepdims=True)
        pushed = scaling * (
            image - jnp.sum(reflect * to_reflect + companion * to_companion, axis=0)
        )
        update = pushed - 0.5 * scaling * jnp.sum(pushed * vector) * vector
        reflect = lax.dynamic_update_index_in_dim(reflect, vector, column, 0)
        return reflect, lax.dynamic_update_index_in_dim(companion, update, column, 0)

    zero = jnp.zeros((COLS, N), F32)
    reflect, companion = lax.fori_loop(0, COLS, one, (zero, zero))
    reflect_rows = lax.dynamic_slice_in_dim(reflect, row_at, rows, 1)
    companion_rows = lax.dynamic_slice_in_dim(companion, row_at, rows, 1)
    reflect_cols = lax.dynamic_slice_in_dim(reflect, col_at, cols, 1)
    companion_cols = lax.dynamic_slice_in_dim(companion, col_at, cols, 1)

    def subtract(k, trailing):
        def row(x):
            return lax.dynamic_index_in_dim(x, k, 0, keepdims=False)

        return (
            trailing
            - row(reflect_rows)[:, None] * row(companion_cols)[None, :]
            - row(companion_rows)[:, None] * row(reflect_cols)[None, :]
        )

    return lax.fori_loop(0, COLS, subtract, matrix), reflect_rows


def solution(mesh):
    placed = (P("row", "col"),)
    return jax.shard_map(
        local,
        mesh=mesh,
        in_specs=placed,
        out_specs=(P("row", "col"), P("row", None)),
        check_vma=False,
    )
```

```python
import functools

import jax
import jax.numpy as jnp
from jax import lax
from jax.experimental import pallas as pl
from jax.experimental.pallas import tpu as pltpu
from jax.sharding import PartitionSpec as P


N = 16384
COLS = 8
LANES = 128
F32 = jnp.float32
VMEM = pltpu.VMEM
LIMIT = 16 << 20
GUARD = True
GROWTH = 16.0
PIVOT = 0.05


def places():
    return lax.axis_index("row"), lax.axis_index("col")


def total(x):
    return jnp.sum(jnp.sum(x, axis=0, keepdims=True), axis=1, keepdims=True)


def iota(shape, dim):
    return lax.broadcasted_iota(jnp.int32, shape, dim)


def without_first(x, owner):
    hit = (iota(x.shape, 0) == 0) & (iota(x.shape, 1) == 0)
    if owner is not None:
        hit = hit & (owner == 0)
    return jnp.where(hit, 0.0, x)


def times_rows(a_ref, x):
    upright = jnp.concatenate([x, jnp.zeros_like(x)], axis=0).T
    out = []
    for t in range(8):
        acc = jnp.zeros((8, LANES), F32)
        for q in range(4):
            block = a_ref[q * LANES : (q + 1) * LANES, t * LANES : (t + 1) * LANES]
            acc = acc + jnp.sum((block * upright[:, q : q + 1]).reshape(16, 8, LANES), axis=0)
        out.append(jnp.sum(acc, axis=0, keepdims=True))
    return jnp.concatenate(out, axis=0)


def times_cols(a_ref, x):
    out = []
    for q in range(4):
        acc = jnp.zeros((LANES, LANES), F32)
        for t in range(8):
            block = a_ref[q * LANES : (q + 1) * LANES, t * LANES : (t + 1) * LANES]
            acc = acc + block * x[t : t + 1, :]
        out.append(jnp.sum(acc.T, axis=0, keepdims=True))
    return jnp.concatenate(out, axis=0)


def send_all(send_ref, first, parts):
    for member in range(send_ref.shape[0]):
        for k, part in enumerate(parts):
            send_ref[member, first + k] = part


def halves(x):
    return [x[:4], x[4:]]


def along_cols(recv_ref):
    s = jnp.sum(recv_ref[:, 0:2], axis=0)
    return jnp.concatenate([s[0], s[1]], axis=0)


def along_rows(recv_ref):
    return jnp.sum(recv_ref[:, 0], axis=0)


def whole_from_rows(recv_ref, group):
    return jnp.concatenate([recv_ref[r, group] for r in range(recv_ref.shape[0])], axis=0)


def whole_from_cols(recv_ref, group):
    return jnp.concatenate(
        [recv_ref[c, group + k] for c in range(recv_ref.shape[0]) for k in range(2)], axis=0
    )


def start_kernel(a_ref, send_ref, held_ref, slab_ref, sems):
    copy = pltpu.make_async_copy(a_ref.at[:, pl.ds(0, LANES)], slab_ref, sems.at[0])
    copy.start()
    hold = pltpu.make_async_copy(a_ref, held_ref, sems.at[1])
    hold.start()
    copy.wait()
    left = [slab_ref[q * LANES : (q + 1) * LANES, :].T for q in range(4)]
    column = jnp.concatenate([x[0:1] for x in left], axis=0)
    corner = slab_ref[0:16, :]
    packed = jnp.zeros((1, LANES), F32)
    for j in range(COLS):
        lanes = iota((1, LANES), 1)
        entry = jnp.where(lanes < 16, corner[j + 1 : j + 2], 0.0)
        packed = packed + (pltpu.roll(entry, 16 * j, 1) if j else entry)
    blank = jnp.zeros((1, LANES), F32)
    for member in range(16):
        j, half = member // 2, member % 2
        rows = [left[2 * half + k][j + 1 : j + 2] for k in range(2)]
        send_ref[member, 0] = column
        send_ref[member, 1] = jnp.concatenate([*rows, packed, blank], axis=0)
    hold.wait()


def first_kernel(a_ref, recv_ref, send_ref, piece_ref):
    ids_ref = places()
    column = recv_ref[0, 0]
    piece_ref[...] = recv_ref[0, 1]
    packed = recv_ref[0, 1][2:3]
    send_all(send_ref, 0, halves(times_rows(a_ref, without_first(column, ids_ref[0]))))
    send_all(send_ref, 2, [column])
    blank = jnp.zeros((1, LANES), F32)
    for member in range(32):
        j, quarter = member // 4, member % 4
        rows = [
            a_ref[j + 1 : j + 2, (2 * quarter + k) * LANES : (2 * quarter + k + 1) * LANES]
            for k in range(2)
        ]
        send_ref[member, 3] = jnp.concatenate([*rows, packed, blank], axis=0)


def coefficient(scal, k):
    return scal[k : k + 1, 0:1]


def settle(step, given, scal, qs):
    u = without_first(given, None) if step == 2 else given
    zero = jnp.zeros((1, LANES), F32)
    w, cs, growth = u, {}, zero + 1.0
    if step == 2:
        alpha = shift = given[0:1, 0:1]
    else:
        known = range(1, step - 1)
        rows = [jnp.sum(u * qs[i], axis=0, keepdims=True) for i in known]
        rows = rows + [zero] * (8 - len(rows))
        sums = jnp.sum(jnp.concatenate(rows, axis=0), axis=1, keepdims=True)
        for i in known:
            cs[i] = sums[i - 1 : i, 0:1]
            w = w - cs[i] * qs[i]
        growth = jnp.sum(sums * sums, axis=0, keepdims=True)
        alpha, before = cs[step - 2] + coefficient(scal, 9), coefficient(scal, 10)
        smaller = jnp.where(jnp.abs(alpha) < jnp.abs(before), alpha, before)
        shift = jnp.where(alpha * before > 0.0, smaller, 0.0)
    length = jnp.sqrt(total(w * w))
    inverse = 1.0 / length
    if step > 2:
        growth = coefficient(scal, 11) * (1.0 + growth * inverse * inverse)
    out = [zero + length] + [zero + cs[i] if i in cs else zero for i in range(1, 8)]
    out = out + [zero + x for x in (inverse, shift, alpha, growth)] + [zero] * 4
    return w * inverse, length, inverse, shift, cs, jnp.concatenate(out, axis=0)


def given_rows(recv_ref, by_rows):
    row_index, col_index = places()
    if by_rows:
        group = recv_ref.shape[1] - 1 if recv_ref.shape[1] < 3 else 2
        here = recv_ref[row_index, group]
        there = [recv_ref[2 * col_index + k, group] for k in range(2)]
        first = recv_ref[0, group][0:1]
    else:
        here = recv_ref[row_index // 2, 1 + row_index % 2]
        there = [recv_ref[col_index, 1 + k] for k in range(2)]
        first = recv_ref[0, 1][0:1]
    return jnp.concatenate([here, *there, first, jnp.zeros((3, LANES), F32)], axis=0)


def kept_rows(ref):
    row_index, col_index = places()
    here, there = ref[pl.ds(4 * row_index, 4), :], ref[pl.ds(8 * col_index, 8), :]
    return jnp.concatenate([here, there, ref[0:1, :], jnp.zeros((3, LANES), F32)], axis=0)


def product_rows(step, recv_ref, scal, q_refs):
    out = given_rows(recv_ref, step % 2 == 0)
    out = out + coefficient(scal, 9) * kept_rows(q_refs[step - 2])
    if step > 3:
        return out + coefficient(scal, 0) * kept_rows(q_refs[step - 3])
    row_index, col_index = places()
    rows, lanes = iota(out.shape, 0), iota(out.shape, 1)
    start = ((rows == 0) & (row_index == 0)) | ((rows == 4) & (col_index == 0)) | (rows == 12)
    return out + jnp.where(start & (lanes == 0), coefficient(scal, 0), 0.0)


def step_kernel(step, *refs):
    refs = list(refs)
    a_ref, recv_ref = refs[:2]
    del refs[:2]
    row_index, col_index = places()
    piece_ref = refs.pop(0) if step in (2, 3) else None
    scal = refs.pop(0)[...] if step > 2 else None
    q_refs = {i: refs.pop(0) for i in range(1, step - 1)}
    rows_refs = {i: refs.pop(0) for i in range(1, step - 2)}
    send_ref = refs.pop(0)
    q_ref = refs.pop(0)
    if step > 2:
        rows_refs[step - 2] = refs.pop(0)
    scal_ref = refs.pop(0)
    edge_ref = refs.pop(0) if step in (3, 4) else None
    new_piece_ref = refs.pop(0) if step == 2 else None

    even = step % 2 == 0
    if even:
        y_here, given = along_cols(recv_ref), whole_from_rows(recv_ref, 2)
        chunk, count, part = col_index, 8, slice(4, 12)
    else:
        y_here, given = along_rows(recv_ref), whole_from_cols(recv_ref, 1)
        chunk, count, part = row_index, 4, slice(0, 4)
    if step > 2:
        rows_refs[step - 2][...] = product_rows(step, recv_ref, scal, q_refs)
    q, length, inverse, shift, cs, scal_out = settle(
        step, given, scal, {i: r[...] for i, r in q_refs.items()}
    )
    q_ref[...] = q
    scal_ref[...] = scal_out
    at = pl.ds(chunk * count, count)
    here = y_here
    for i in cs:
        here = here - cs[i] * rows_refs[i][part, :]
    here = here * inverse - shift * q_ref[at, :]
    if step > 2:
        here = here - length * q_refs[step - 2][at, :]
    here = without_first(here, chunk)
    if even:
        send_all(send_ref, 0, [times_cols(a_ref, here)])
        send_all(send_ref, 1, halves(here))
    else:
        send_all(send_ref, 0, halves(times_rows(a_ref, here)))
        send_all(send_ref, 2, [here])
    if step in (2, 3):
        send_all(send_ref, 3, [piece_ref[...]])
    if step == 2:
        new_piece_ref[...] = recv_ref[0, 3]
    if step == 3:
        edge_ref[...] = jnp.concatenate([recv_ref[c, 3][0:2] for c in range(16)], axis=0)
    if step == 4:
        edge_ref[...] = jnp.concatenate([recv_ref[r, 3][0:2] for r in range(32)], axis=0)


def last_send_kernel(recv_ref, send_ref):
    send_all(send_ref, 0, [along_rows(recv_ref)])


def sign(k):
    return -1.0 if k % 2 else 1.0


def product(x, y):
    return lax.dot_general(
        x,
        y,
        (((0,), (0,)), ((), ())),
        precision=lax.Precision.HIGHEST,
        preferred_element_type=F32,
    )


def rows_at(refs, row):
    blank = jnp.zeros((1, LANES), F32)
    return jnp.concatenate(
        [sign(k) * refs[k][pl.ds(row, 1), :] if k in refs else blank for k in range(1, 9)], axis=0
    )


def d_tile(q_refs, row):
    lanes, ks = iota((8, LANES), 1), iota((8, LANES), 0)
    unit = jnp.where((lanes == ks + 1) & (row == 0), 1.0, 0.0)
    return unit - rows_at(q_refs, row)


def three(x):
    high = x.astype(jnp.bfloat16).astype(F32)
    middle = (x - high).astype(jnp.bfloat16).astype(F32)
    low = (x - high - middle).astype(jnp.bfloat16).astype(F32)
    return high, middle, low


def panel_kernel(*refs):
    row_index, col_index = places()
    refs = list(refs)
    refs.insert(0, None)
    recv_ref, packed_ref, edge_r_ref, edge_c_ref = refs[1:5]
    scal_refs = {i: refs[4 + i] for i in range(1, 8)}
    q_refs = {i: refs[11 + i] for i in range(1, 8)}
    aq_rows = {i: refs[18 + i] for i in range(1, 7)}
    q_out, flag_ref, reflect_ref, side_ref, left_ref, right_ref, rows_out = refs[25:32]
    q, length, _, _, cs, scal = settle(
        9, whole_from_cols(recv_ref, 1), scal_refs[7][...], {i: r[...] for i, r in q_refs.items()}
    )
    q_out[...] = q
    rows_out[...] = product_rows(9, recv_ref, scal_refs[7][...], q_refs)
    aq_rows[7] = rows_out
    rest = jnp.zeros((16, LANES), F32)
    for i in range(1, 8):
        rest = rest + cs[i] * aq_rows[i][...]
    side_ref[96:104, :] = scal[8:16]
    side_ref[104:120, :] = rest
    side_ref[120:128, :] = jnp.zeros((8, LANES), F32) + cs[7] * length
    q_refs[8] = q_out
    lanes, ks = iota((8, LANES), 1), iota((8, LANES), 0)
    top = d_tile(q_refs, 0)
    work = jnp.where(lanes < 8, pltpu.roll(top, LANES - 1, 1), 0.0)
    work = work + jnp.where(lanes == ks + 8, 1.0, 0.0)
    to_reflect = jnp.zeros((8, LANES), F32)
    pivot = jnp.ones((1, 1), F32)
    for k in range(8):
        row = work[k : k + 1]
        pivot = jnp.minimum(pivot, row[:, k : k + 1])
        beta = (scal if k == 7 else scal_refs[k + 1])[0:1, :]
        to_reflect = jnp.where(ks == k, row * beta, to_reflect)
        row = row / row[:, k : k + 1]
        column = jnp.where(ks == k, 0.0, work)[:, k : k + 1]
        work = jnp.where(ks == k, row, work - column * row)
    sound = (scal[11:12, 0:1] <= GROWTH) & (pivot >= PIVOT)
    flag_ref[...] = jnp.zeros((8, LANES), F32) + jnp.where(sound, 1.0, 0.0)
    factor = pltpu.roll(work, LANES - 8, 1)[:, 0:8]
    flipped = jnp.concatenate(
        [jnp.where(lanes < 8, pltpu.roll(work, LANES - 8, 1), 0.0), jnp.zeros((LANES - 8, LANES), F32)],
        axis=0,
    ).T[0:8, 0:8]
    to_reflect = jnp.where(lanes < 8, pltpu.roll(to_reflect, LANES - 8, 1), 0.0)
    inner = jnp.zeros((8, LANES), F32)
    packed = packed_ref[2:3]
    for k in range(8):
        entry = pltpu.roll(packed, LANES - 16 * k, 1) if k else packed
        inner = jnp.where(ks == k, entry, inner)
    used = (lanes >= 1) & (lanes <= 8)
    inner = jnp.where(used, inner, 0.0)
    cross = jnp.where(used, rows_at(aq_rows, 12), 0.0)
    inner = pltpu.roll(inner - cross, LANES - 1, 1)
    cross = pltpu.roll(cross, LANES - 1, 1)
    square = jnp.concatenate([cross, jnp.zeros((LANES - 8, LANES), F32)], axis=0)
    inner = inner - square.T[0:8]
    for k in range(1, 8):
        source = scal if k == 7 else scal_refs[k + 1]
        near = ((ks == k - 1) & (lanes == k)) | ((ks == k) & (lanes == k - 1))
        inner = inner - jnp.where(near, source[0:1, :], 0.0)
        alpha = source[10:11, :]
        inner = inner + jnp.where((ks == k - 1) & (lanes == k - 1), alpha, 0.0)
    inner = inner[:, 0:8]
    core = product(factor, product(inner, factor))

    def tiles(base, count, edge_ref, first, kept):
        ds, ys = [], []
        for t in range(count):
            row = base + t
            d = d_tile(q_refs, row)
            edge = jnp.concatenate(
                [edge_ref[count * k + t : count * k + t + 1, :] for k in range(8)], axis=0
            )
            ad = edge - rows_at(aq_rows, kept + t)
            ds.append(d)
            ys.append(product(factor, ad) - 0.5 * product(core, d))
            side_ref[first + 8 * t : first + 8 * t + 8, :] = product(flipped, d)
        return ds, ys

    ds, ys = tiles(4 * row_index, 4, edge_r_ref, 0, 0)
    for t in range(4):
        high, middle, low = three(jnp.concatenate([ds[t], ys[t]], axis=0))
        stack = [high, high, middle, middle, high, low, jnp.zeros((32, LANES), F32)]
        at = slice(t * LANES, (t + 1) * LANES)
        left_ref[at, :] = jnp.concatenate(stack, axis=0).T.astype(jnp.bfloat16)
        out = jnp.zeros((8, LANES), F32)
        for k in range(8):
            out = out + to_reflect[:, k : k + 1] * ds[t][k : k + 1, :]
        out = jnp.where((4 * row_index + t == 0) & (lanes <= ks), 0.0, out)
        reflect_ref[:, t * LANES : (t + 1) * LANES] = out
    ds, ys = tiles(8 * col_index, 8, edge_c_ref, 32, 4)
    for t in range(8):
        high, middle, low = three(jnp.concatenate([ys[t], ds[t]], axis=0))
        stack = [high, middle, high, middle, low, high]
        at = slice(t * LANES, (t + 1) * LANES)
        right_ref[:, at] = jnp.concatenate(stack, axis=0).astype(jnp.bfloat16)


def trailing_kernel(
    a_ref, recv_ref, q_ref, side_ref, left_ref, right_ref, out_ref, block_ref, sems
):
    inverse = coefficient(side_ref, 96)
    aq = (given_rows(recv_ref, True) - side_ref[104:120, :]) * inverse
    alpha = total(q_ref[...] * whole_from_rows(recv_ref, 0)) - coefficient(side_ref, 120)
    alpha = alpha * inverse
    lanes = iota((1, LANES), 1)
    shifted = pltpu.roll(aq[12:13, :], LANES - 1, 1)
    added = jnp.where(lanes == 7, 0.5 * alpha, 0.0) - jnp.where(lanes < 8, shifted, 0.0)
    added = jnp.concatenate([added, jnp.zeros((7, LANES), F32)], axis=0).T[0:8, 0:1]

    def last(count, first, kept):
        return [
            -aq[kept + t : kept + t + 1, :]
            - jnp.sum(added * side_ref[first + 8 * t : first + 8 * t + 8, :], axis=0, keepdims=True)
            for t in range(count)
        ]

    ws_r = last(4, 0, 0)
    ws_c = last(8, 32, 4)
    blank = jnp.zeros((6, LANES), F32)
    copies = []
    for q in range(4):
        at = slice(q * LANES, (q + 1) * LANES)
        upright = jnp.concatenate([side_ref[8 * q + 7 : 8 * q + 8, :], ws_r[q], blank], axis=0).T
        change = jnp.dot(left_ref[at, 0:96], right_ref[...], preferred_element_type=F32)
        for t in range(8):
            to = slice(t * LANES, (t + 1) * LANES)
            block_ref[at, to] = (
                a_ref[at, to]
                - change[:, to]
                - upright[:, 0:1] * ws_c[t]
                - upright[:, 1:2] * side_ref[39 + 8 * t : 40 + 8 * t, :]
            )
        copy = pltpu.make_async_copy(block_ref.at[at, :], out_ref.at[at, :], sems.at[q])
        copy.start()
        copies.append(copy)
    for copy in copies:
        copy.wait()


def call(kernel, outs, *args, scratch=(), pinned=True, flops=1000):
    def shape(x):
        if not isinstance(x, tuple):
            return x
        return VMEM(x, F32) if pinned else jax.ShapeDtypeStruct(x, F32)

    return pl.pallas_call(
        kernel,
        out_shape=[shape(x) for x in outs],
        in_specs=[pl.BlockSpec(memory_space=VMEM)] * len(args),
        out_specs=[pl.BlockSpec(memory_space=VMEM)] * len(outs),
        scratch_shapes=[VMEM(s, F32) for s in scratch],
        compiler_params=pltpu.CompilerParams(vmem_limit_bytes=LIMIT),
        cost_estimate=pl.CostEstimate(flops=flops, bytes_accessed=1000, transcendentals=0),
    )(*args)


def exchange(x, axis):
    return lax.all_to_all(x, axis, 0, 0, tiled=True)


def local(matrix):
    whole = (N // LANES, LANES)
    send, held = pl.pallas_call(
        start_kernel,
        out_shape=[VMEM((16, 2, 4, LANES), F32), VMEM(matrix.shape, F32)],
        in_specs=[pl.BlockSpec(memory_space=pltpu.HBM)],
        out_specs=[pl.BlockSpec(memory_space=VMEM)] * 2,
        scratch_shapes=[VMEM((matrix.shape[0], LANES), F32), pltpu.SemaphoreType.DMA((2,))],
        compiler_params=pltpu.CompilerParams(vmem_limit_bytes=LIMIT),
    )(pltpu.with_memory_space_constraint(matrix, pltpu.HBM))
    recv = exchange(send, "col")
    send, piece = call(first_kernel, [(32, 4, 4, LANES), (4, LANES)], held, recv)
    recv = exchange(send, "row")
    qs, aq_rows, scals = {}, {}, {}
    for step in range(2, 9):
        args = [held, recv]
        if step in (2, 3):
            args.append(piece)
        if step > 2:
            args.append(scals[step - 2])
        args += [qs[i] for i in range(1, step - 1)] + [aq_rows[i] for i in range(1, step - 2)]
        groups = 4 if step in (2, 3) else 3
        outs = [(16 if step % 2 == 0 else 32, groups, 4, LANES), whole]
        if step > 2:
            outs.append((16, LANES))
        outs.append((16, LANES))
        if step in (3, 4):
            outs.append((32 if step == 3 else 64, LANES))
        if step == 2:
            outs.append((4, LANES))
        result = list(call(functools.partial(step_kernel, step), outs, *args))
        send = result.pop(0)
        qs[step - 1] = result.pop(0)
        if step > 2:
            aq_rows[step - 2] = result.pop(0)
        scals[step - 1] = result.pop(0)
        if step == 3:
            edge_r = result.pop(0)
        if step == 4:
            edge_c = result.pop(0)
        if step == 2:
            piece = packed = result.pop(0)
        recv = exchange(send, "col" if step % 2 == 0 else "row")
    (send,) = call(last_send_kernel, [(32, 1, 4, LANES)], recv)
    last = exchange(send, "row")
    rows, cols = matrix.shape
    q, flag, reflect, side, left, right = call(
        panel_kernel,
        [whole, jax.ShapeDtypeStruct((8, LANES), F32), pltpu.HBM((8, rows), F32), (128, LANES)]
        + [VMEM((rows, LANES), jnp.bfloat16), VMEM((96, cols), jnp.bfloat16)],
        recv,
        packed,
        edge_r,
        edge_c,
        *[scals[i] for i in range(1, 8)],
        *[qs[i] for i in range(1, 8)],
        *[aq_rows[i] for i in range(1, 7)],
        scratch=[(16, LANES)],
        flops=40000000,
    )
    trailing = pl.pallas_call(
        trailing_kernel,
        out_shape=jax.ShapeDtypeStruct(matrix.shape, F32),
        in_specs=[pl.BlockSpec(memory_space=VMEM)] * 6,
        out_specs=pl.BlockSpec(memory_space=pltpu.HBM),
        scratch_shapes=[VMEM(matrix.shape, F32), pltpu.SemaphoreType.DMA((4,))],
        compiler_params=pltpu.CompilerParams(vmem_limit_bytes=LIMIT),
    )(held, last, q, side, left, right)
    if not GUARD:
        return trailing, reflect.T
    kept = matrix
    _, trailing, reflect = lax.while_loop(
        lambda state: state[0] < 0.5,
        lambda state: (jnp.float32(1.0), *column_by_column(kept)),
        (flag[0, 0], trailing, reflect),
    )
    return trailing, reflect.T


def as_it_is(x_ref, out_ref):
    out_ref[...] = x_ref[...]


def of_everyone(shard, axis):
    size = lax.axis_size(axis)
    return exchange(jnp.broadcast_to(shard[None], (size, *shard.shape)), axis)


def column_by_column(matrix):
    rows, cols = matrix.shape
    row_at, col_at = lax.axis_index("row") * rows, lax.axis_index("col") * cols
    panel = of_everyone(matrix[:, :COLS].T, "col")[0]
    panel = of_everyone(panel, "row").transpose(1, 0, 2).reshape(COLS, N)
    positions = jnp.arange(N, dtype=jnp.int32)

    def one(column, state):
        reflect, companion = state

        def row(x):
            return lax.dynamic_index_in_dim(x, column, 0, keepdims=False)

        def entries(x):
            return lax.dynamic_index_in_dim(x, column, 1, keepdims=True)

        current = row(panel) - jnp.sum(
            reflect * entries(companion) + companion * entries(reflect), axis=0
        )
        below = jnp.where(positions > column, current, 0.0)
        leading = jnp.sum(jnp.where(positions == column + 1, current, 0.0))
        length = jnp.sqrt(jnp.sum(below * below))
        vector = below + jnp.where(positions == column + 1, length, 0.0)
        scaling = 1.0 / (length * (length + leading))
        along_rows_here = lax.dynamic_slice_in_dim(vector, row_at, rows, 0)
        image = jnp.sum(matrix * along_rows_here[:, None], axis=0)
        image = of_everyone(image, "row").sum(axis=0)
        image = of_everyone(image, "col").reshape(N)
        to_reflect = jnp.sum(companion * vector, axis=1, keepdims=True)
        to_companion = jnp.sum(reflect * vector, axis=1, keepdims=True)
        pushed = scaling * (
            image - jnp.sum(reflect * to_reflect + companion * to_companion, axis=0)
        )
        update = pushed - 0.5 * scaling * jnp.sum(pushed * vector) * vector
        reflect = lax.dynamic_update_index_in_dim(reflect, vector, column, 0)
        return reflect, lax.dynamic_update_index_in_dim(companion, update, column, 0)

    zero = jnp.zeros((COLS, N), F32)
    reflect, companion = lax.fori_loop(0, COLS, one, (zero, zero))
    reflect_rows = lax.dynamic_slice_in_dim(reflect, row_at, rows, 1)
    companion_rows = lax.dynamic_slice_in_dim(companion, row_at, rows, 1)
    reflect_cols = lax.dynamic_slice_in_dim(reflect, col_at, cols, 1)
    companion_cols = lax.dynamic_slice_in_dim(companion, col_at, cols, 1)

    def subtract(k, trailing):
        def row(x):
            return lax.dynamic_index_in_dim(x, k, 0, keepdims=False)

        return (
            trailing
            - row(reflect_rows)[:, None] * row(companion_cols)[None, :]
            - row(companion_rows)[:, None] * row(reflect_cols)[None, :]
        )

    (reflect_rows,) = call(as_it_is, [(COLS, rows)], reflect_rows, pinned=False)
    return lax.fori_loop(0, COLS, subtract, matrix), reflect_rows


def solution(mesh):
    placed = (P("row", "col"),)
    return jax.shard_map(
        local,
        mesh=mesh,
        in_specs=placed,
        out_specs=(P("row", "col"), P("row", None)),
        check_vma=False,
    )
```

```python
import functools

import jax
import jax.numpy as jnp
from jax import lax
from jax.experimental import pallas as pl
from jax.experimental.pallas import tpu as pltpu
from jax.sharding import PartitionSpec as P


N = 16384
COLS = 8
LANES = 128
F32 = jnp.float32
VMEM = pltpu.VMEM
LIMIT = 16 << 20
GUARD = True
GROWTH = 16.0
PIVOT = 0.05


def places():
    return lax.axis_index("row"), lax.axis_index("col")


def total(x):
    return jnp.sum(jnp.sum(x, axis=0, keepdims=True), axis=1, keepdims=True)


def iota(shape, dim):
    return lax.broadcasted_iota(jnp.int32, shape, dim)


def without_first(x, owner):
    hit = (iota(x.shape, 0) == 0) & (iota(x.shape, 1) == 0)
    if owner is not None:
        hit = hit & (owner == 0)
    return jnp.where(hit, 0.0, x)


def times_rows(a_ref, x):
    upright = jnp.concatenate([x, jnp.zeros_like(x)], axis=0).T
    out = []
    for t in range(8):
        acc = jnp.zeros((8, LANES), F32)
        for q in range(4):
            block = a_ref[q * LANES : (q + 1) * LANES, t * LANES : (t + 1) * LANES]
            acc = acc + jnp.sum((block * upright[:, q : q + 1]).reshape(16, 8, LANES), axis=0)
        out.append(jnp.sum(acc, axis=0, keepdims=True))
    return jnp.concatenate(out, axis=0)


def times_cols(a_ref, x):
    out = []
    for q in range(4):
        acc = jnp.zeros((LANES, LANES), F32)
        for t in range(8):
            block = a_ref[q * LANES : (q + 1) * LANES, t * LANES : (t + 1) * LANES]
            acc = acc + block * x[t : t + 1, :]
        out.append(jnp.sum(acc.T, axis=0, keepdims=True))
    return jnp.concatenate(out, axis=0)


def send_all(send_ref, first, parts):
    for member in range(send_ref.shape[0]):
        for k, part in enumerate(parts):
            send_ref[member, first + k] = part


def halves(x):
    return [x[:4], x[4:]]


def along_cols(recv_ref):
    s = jnp.sum(recv_ref[:, 0:2], axis=0)
    return jnp.concatenate([s[0], s[1]], axis=0)


def along_rows(recv_ref):
    return jnp.sum(recv_ref[:, 0], axis=0)


def whole_from_rows(recv_ref, group):
    return jnp.concatenate([recv_ref[r, group] for r in range(recv_ref.shape[0])], axis=0)


def whole_from_cols(recv_ref, group):
    return jnp.concatenate(
        [recv_ref[c, group + k] for c in range(recv_ref.shape[0]) for k in range(2)], axis=0
    )


def start_kernel(a_ref, send_ref, held_ref, slab_ref, sems):
    copy = pltpu.make_async_copy(a_ref.at[:, pl.ds(0, LANES)], slab_ref, sems.at[0])
    copy.start()
    hold = pltpu.make_async_copy(a_ref, held_ref, sems.at[1])
    hold.start()
    copy.wait()
    left = [slab_ref[q * LANES : (q + 1) * LANES, :].T for q in range(4)]
    column = jnp.concatenate([x[0:1] for x in left], axis=0)
    corner = slab_ref[0:16, :]
    packed = jnp.zeros((1, LANES), F32)
    for j in range(COLS):
        lanes = iota((1, LANES), 1)
        entry = jnp.where(lanes < 16, corner[j + 1 : j + 2], 0.0)
        packed = packed + (pltpu.roll(entry, 16 * j, 1) if j else entry)
    blank = jnp.zeros((1, LANES), F32)
    for member in range(16):
        j, half = member // 2, member % 2
        rows = [left[2 * half + k][j + 1 : j + 2] for k in range(2)]
        send_ref[member, 0] = column
        send_ref[member, 1] = jnp.concatenate([*rows, packed, blank], axis=0)
    hold.wait()


def first_kernel(a_ref, recv_ref, send_ref, piece_ref):
    ids_ref = places()
    column = recv_ref[0, 0]
    piece_ref[...] = recv_ref[0, 1]
    packed = recv_ref[0, 1][2:3]
    send_all(send_ref, 0, halves(times_rows(a_ref, without_first(column, ids_ref[0]))))
    send_all(send_ref, 2, [column])
    blank = jnp.zeros((1, LANES), F32)
    for member in range(32):
        j, quarter = member // 4, member % 4
        rows = [
            a_ref[j + 1 : j + 2, (2 * quarter + k) * LANES : (2 * quarter + k + 1) * LANES]
            for k in range(2)
        ]
        send_ref[member, 3] = jnp.concatenate([*rows, packed, blank], axis=0)


def coefficient(scal, k):
    return scal[k : k + 1, 0:1]


def settle(step, given, scal, qs):
    u = without_first(given, None) if step == 2 else given
    zero = jnp.zeros((1, LANES), F32)
    w, cs, growth = u, {}, zero + 1.0
    if step == 2:
        alpha = shift = given[0:1, 0:1]
    else:
        known = range(1, step - 1)
        rows = [jnp.sum(u * qs[i], axis=0, keepdims=True) for i in known]
        rows = rows + [zero] * (8 - len(rows))
        sums = jnp.sum(jnp.concatenate(rows, axis=0), axis=1, keepdims=True)
        for i in known:
            cs[i] = sums[i - 1 : i, 0:1]
            w = w - cs[i] * qs[i]
        growth = jnp.sum(sums * sums, axis=0, keepdims=True)
        alpha, before = cs[step - 2] + coefficient(scal, 9), coefficient(scal, 10)
        smaller = jnp.where(jnp.abs(alpha) < jnp.abs(before), alpha, before)
        shift = jnp.where(alpha * before > 0.0, smaller, 0.0)
    length = jnp.sqrt(total(w * w))
    inverse = 1.0 / length
    if step > 2:
        growth = coefficient(scal, 11) * (1.0 + growth * inverse * inverse)
    out = [zero + length] + [zero + cs[i] if i in cs else zero for i in range(1, 8)]
    out = out + [zero + x for x in (inverse, shift, alpha, growth)] + [zero] * 4
    return w * inverse, length, inverse, shift, cs, jnp.concatenate(out, axis=0)


def given_rows(recv_ref, by_rows):
    row_index, col_index = places()
    if by_rows:
        group = recv_ref.shape[1] - 1 if recv_ref.shape[1] < 3 else 2
        here = recv_ref[row_index, group]
        there = [recv_ref[2 * col_index + k, group] for k in range(2)]
        first = recv_ref[0, group][0:1]
    else:
        here = recv_ref[row_index // 2, 1 + row_index % 2]
        there = [recv_ref[col_index, 1 + k] for k in range(2)]
        first = recv_ref[0, 1][0:1]
    return jnp.concatenate([here, *there, first, jnp.zeros((3, LANES), F32)], axis=0)


def kept_rows(ref):
    row_index, col_index = places()
    here, there = ref[pl.ds(4 * row_index, 4), :], ref[pl.ds(8 * col_index, 8), :]
    return jnp.concatenate([here, there, ref[0:1, :], jnp.zeros((3, LANES), F32)], axis=0)


def product_rows(step, recv_ref, scal, q_refs):
    out = given_rows(recv_ref, step % 2 == 0)
    out = out + coefficient(scal, 9) * kept_rows(q_refs[step - 2])
    if step > 3:
        return out + coefficient(scal, 0) * kept_rows(q_refs[step - 3])
    row_index, col_index = places()
    rows, lanes = iota(out.shape, 0), iota(out.shape, 1)
    start = ((rows == 0) & (row_index == 0)) | ((rows == 4) & (col_index == 0)) | (rows == 12)
    return out + jnp.where(start & (lanes == 0), coefficient(scal, 0), 0.0)


def step_kernel(step, *refs):
    refs = list(refs)
    a_ref, recv_ref = refs[:2]
    del refs[:2]
    row_index, col_index = places()
    piece_ref = refs.pop(0) if step in (2, 3) else None
    scal = refs.pop(0)[...] if step > 2 else None
    q_refs = {i: refs.pop(0) for i in range(1, step - 1)}
    rows_refs = {i: refs.pop(0) for i in range(1, step - 2)}
    send_ref = refs.pop(0)
    q_ref = refs.pop(0)
    if step > 2:
        rows_refs[step - 2] = refs.pop(0)
    scal_ref = refs.pop(0)
    edge_ref = refs.pop(0) if step in (3, 4) else None
    new_piece_ref = refs.pop(0) if step == 2 else None

    even = step % 2 == 0
    if even:
        y_here, given = along_cols(recv_ref), whole_from_rows(recv_ref, 2)
        chunk, count, part = col_index, 8, slice(4, 12)
    else:
        y_here, given = along_rows(recv_ref), whole_from_cols(recv_ref, 1)
        chunk, count, part = row_index, 4, slice(0, 4)
    if step > 2:
        rows_refs[step - 2][...] = product_rows(step, recv_ref, scal, q_refs)
    q, length, inverse, shift, cs, scal_out = settle(
        step, given, scal, {i: r[...] for i, r in q_refs.items()}
    )
    q_ref[...] = q
    scal_ref[...] = scal_out
    at = pl.ds(chunk * count, count)
    here = y_here
    for i in cs:
        here = here - cs[i] * rows_refs[i][part, :]
    here = here * inverse - shift * q_ref[at, :]
    if step > 2:
        here = here - length * q_refs[step - 2][at, :]
    here = without_first(here, chunk)
    if even:
        send_all(send_ref, 0, [times_cols(a_ref, here)])
        send_all(send_ref, 1, halves(here))
    else:
        send_all(send_ref, 0, halves(times_rows(a_ref, here)))
        send_all(send_ref, 2, [here])
    if step in (2, 3):
        send_all(send_ref, 3, [piece_ref[...]])
    if step == 2:
        new_piece_ref[...] = recv_ref[0, 3]
    if step == 3:
        edge_ref[...] = jnp.concatenate([recv_ref[c, 3][0:2] for c in range(16)], axis=0)
    if step == 4:
        edge_ref[...] = jnp.concatenate([recv_ref[r, 3][0:2] for r in range(32)], axis=0)


def last_send_kernel(recv_ref, send_ref):
    send_all(send_ref, 0, [along_rows(recv_ref)])


def sign(k):
    return -1.0 if k % 2 else 1.0


def product(x, y):
    return lax.dot_general(
        x,
        y,
        (((0,), (0,)), ((), ())),
        precision=lax.Precision.HIGHEST,
        preferred_element_type=F32,
    )


def rows_at(refs, row):
    blank = jnp.zeros((1, LANES), F32)
    return jnp.concatenate(
        [sign(k) * refs[k][pl.ds(row, 1), :] if k in refs else blank for k in range(1, 9)], axis=0
    )


def d_tile(q_refs, row):
    lanes, ks = iota((8, LANES), 1), iota((8, LANES), 0)
    unit = jnp.where((lanes == ks + 1) & (row == 0), 1.0, 0.0)
    return unit - rows_at(q_refs, row)


def three(x):
    high = x.astype(jnp.bfloat16).astype(F32)
    middle = (x - high).astype(jnp.bfloat16).astype(F32)
    low = (x - high - middle).astype(jnp.bfloat16).astype(F32)
    return high, middle, low


def panel_kernel(*refs):
    row_index, col_index = places()
    refs = list(refs)
    refs.insert(0, None)
    recv_ref, packed_ref, edge_r_ref, edge_c_ref = refs[1:5]
    scal_refs = {i: refs[4 + i] for i in range(1, 8)}
    q_refs = {i: refs[11 + i] for i in range(1, 8)}
    aq_rows = {i: refs[18 + i] for i in range(1, 7)}
    q_out, flag_ref, reflect_ref, side_ref, left_ref, right_ref, rows_out = refs[25:32]
    q, length, _, _, cs, scal = settle(
        9, whole_from_cols(recv_ref, 1), scal_refs[7][...], {i: r[...] for i, r in q_refs.items()}
    )
    q_out[...] = q
    rows_out[...] = product_rows(9, recv_ref, scal_refs[7][...], q_refs)
    aq_rows[7] = rows_out
    rest = jnp.zeros((16, LANES), F32)
    for i in range(1, 8):
        rest = rest + cs[i] * aq_rows[i][...]
    side_ref[96:104, :] = scal[8:16]
    side_ref[104:120, :] = rest
    side_ref[120:128, :] = jnp.zeros((8, LANES), F32) + cs[7] * length
    q_refs[8] = q_out
    lanes, ks = iota((8, LANES), 1), iota((8, LANES), 0)
    top = d_tile(q_refs, 0)
    work = jnp.where(lanes < 8, pltpu.roll(top, LANES - 1, 1), 0.0)
    work = work + jnp.where(lanes == ks + 8, 1.0, 0.0)
    to_reflect = jnp.zeros((8, LANES), F32)
    pivot = jnp.ones((1, 1), F32)
    for k in range(8):
        row = work[k : k + 1]
        pivot = jnp.minimum(pivot, row[:, k : k + 1])
        beta = (scal if k == 7 else scal_refs[k + 1])[0:1, :]
        to_reflect = jnp.where(ks == k, row * beta, to_reflect)
        row = row / row[:, k : k + 1]
        column = jnp.where(ks == k, 0.0, work)[:, k : k + 1]
        work = jnp.where(ks == k, row, work - column * row)
    sound = (scal[11:12, 0:1] <= GROWTH) & (pivot >= PIVOT)
    flag_ref[...] = jnp.zeros((8, LANES), F32) + jnp.where(sound, 1.0, 0.0)
    factor = pltpu.roll(work, LANES - 8, 1)[:, 0:8]
    flipped = jnp.concatenate(
        [jnp.where(lanes < 8, pltpu.roll(work, LANES - 8, 1), 0.0), jnp.zeros((LANES - 8, LANES), F32)],
        axis=0,
    ).T[0:8, 0:8]
    to_reflect = jnp.where(lanes < 8, pltpu.roll(to_reflect, LANES - 8, 1), 0.0)
    inner = jnp.zeros((8, LANES), F32)
    packed = packed_ref[2:3]
    for k in range(8):
        entry = pltpu.roll(packed, LANES - 16 * k, 1) if k else packed
        inner = jnp.where(ks == k, entry, inner)
    used = (lanes >= 1) & (lanes <= 8)
    inner = jnp.where(used, inner, 0.0)
    cross = jnp.where(used, rows_at(aq_rows, 12), 0.0)
    inner = pltpu.roll(inner - cross, LANES - 1, 1)
    cross = pltpu.roll(cross, LANES - 1, 1)
    square = jnp.concatenate([cross, jnp.zeros((LANES - 8, LANES), F32)], axis=0)
    inner = inner - square.T[0:8]
    for k in range(1, 8):
        source = scal if k == 7 else scal_refs[k + 1]
        near = ((ks == k - 1) & (lanes == k)) | ((ks == k) & (lanes == k - 1))
        inner = inner - jnp.where(near, source[0:1, :], 0.0)
        alpha = source[10:11, :]
        inner = inner + jnp.where((ks == k - 1) & (lanes == k - 1), alpha, 0.0)
    inner = inner[:, 0:8]
    core = product(factor, product(inner, factor))

    def tiles(base, count, edge_ref, first, kept):
        ds, ys = [], []
        for t in range(count):
            row = base + t
            d = d_tile(q_refs, row)
            edge = jnp.concatenate(
                [edge_ref[count * k + t : count * k + t + 1, :] for k in range(8)], axis=0
            )
            ad = edge - rows_at(aq_rows, kept + t)
            ds.append(d)
            ys.append(product(factor, ad) - 0.5 * product(core, d))
            side_ref[first + 8 * t : first + 8 * t + 8, :] = product(flipped, d)
        return ds, ys

    ds, ys = tiles(4 * row_index, 4, edge_r_ref, 0, 0)
    for t in range(4):
        high, middle, low = three(jnp.concatenate([ds[t], ys[t]], axis=0))
        stack = [high, high, middle, middle, high, low, jnp.zeros((32, LANES), F32)]
        at = slice(t * LANES, (t + 1) * LANES)
        left_ref[at, :] = jnp.concatenate(stack, axis=0).T.astype(jnp.bfloat16)
        out = jnp.zeros((8, LANES), F32)
        for k in range(8):
            out = out + to_reflect[:, k : k + 1] * ds[t][k : k + 1, :]
        out = jnp.where((4 * row_index + t == 0) & (lanes <= ks), 0.0, out)
        reflect_ref[:, t * LANES : (t + 1) * LANES] = out
    ds, ys = tiles(8 * col_index, 8, edge_c_ref, 32, 4)
    for t in range(8):
        high, middle, low = three(jnp.concatenate([ys[t], ds[t]], axis=0))
        stack = [high, middle, high, middle, low, high]
        at = slice(t * LANES, (t + 1) * LANES)
        right_ref[:, at] = jnp.concatenate(stack, axis=0).astype(jnp.bfloat16)


def trailing_kernel(
    a_ref, recv_ref, q_ref, side_ref, left_ref, right_ref, out_ref, block_ref, sems
):
    inverse = coefficient(side_ref, 96)
    aq = (given_rows(recv_ref, True) - side_ref[104:120, :]) * inverse
    alpha = total(q_ref[...] * whole_from_rows(recv_ref, 0)) - coefficient(side_ref, 120)
    alpha = alpha * inverse
    lanes = iota((1, LANES), 1)
    shifted = pltpu.roll(aq[12:13, :], LANES - 1, 1)
    added = jnp.where(lanes == 7, 0.5 * alpha, 0.0) - jnp.where(lanes < 8, shifted, 0.0)
    added = jnp.concatenate([added, jnp.zeros((7, LANES), F32)], axis=0).T[0:8, 0:1]

    def last(count, first, kept):
        return [
            -aq[kept + t : kept + t + 1, :]
            - jnp.sum(added * side_ref[first + 8 * t : first + 8 * t + 8, :], axis=0, keepdims=True)
            for t in range(count)
        ]

    ws_r = last(4, 0, 0)
    ws_c = last(8, 32, 4)
    blank = jnp.zeros((6, LANES), F32)
    copies = []
    for q in range(4):
        upright = jnp.concatenate([side_ref[8 * q + 7 : 8 * q + 8, :], ws_r[q], blank], axis=0).T
        for half in range(2):
            at = slice(q * LANES + half * 64, q * LANES + half * 64 + 64)
            piece = upright[half * 64 : half * 64 + 64]
            change = jnp.dot(left_ref[at, 0:96], right_ref[...], preferred_element_type=F32)
            for t in range(8):
                to = slice(t * LANES, (t + 1) * LANES)
                block_ref[at, to] = (
                    a_ref[at, to]
                    - change[:, to]
                    - piece[:, 0:1] * ws_c[t]
                    - piece[:, 1:2] * side_ref[39 + 8 * t : 40 + 8 * t, :]
                )
            copy = pltpu.make_async_copy(
                block_ref.at[at, :], out_ref.at[at, :], sems.at[2 * q + half]
            )
            copy.start()
            copies.append(copy)
    for copy in copies:
        copy.wait()


def call(kernel, outs, *args, scratch=(), pinned=True, flops=1000):
    def shape(x):
        if not isinstance(x, tuple):
            return x
        return VMEM(x, F32) if pinned else jax.ShapeDtypeStruct(x, F32)

    return pl.pallas_call(
        kernel,
        out_shape=[shape(x) for x in outs],
        in_specs=[pl.BlockSpec(memory_space=VMEM)] * len(args),
        out_specs=[pl.BlockSpec(memory_space=VMEM)] * len(outs),
        scratch_shapes=[VMEM(s, F32) for s in scratch],
        compiler_params=pltpu.CompilerParams(vmem_limit_bytes=LIMIT),
        cost_estimate=pl.CostEstimate(flops=flops, bytes_accessed=1000, transcendentals=0),
    )(*args)


def exchange(x, axis):
    return lax.all_to_all(x, axis, 0, 0, tiled=True)


def local(matrix):
    whole = (N // LANES, LANES)
    send, held = pl.pallas_call(
        start_kernel,
        out_shape=[VMEM((16, 2, 4, LANES), F32), VMEM(matrix.shape, F32)],
        in_specs=[pl.BlockSpec(memory_space=pltpu.HBM)],
        out_specs=[pl.BlockSpec(memory_space=VMEM)] * 2,
        scratch_shapes=[VMEM((matrix.shape[0], LANES), F32), pltpu.SemaphoreType.DMA((2,))],
        compiler_params=pltpu.CompilerParams(vmem_limit_bytes=LIMIT),
    )(pltpu.with_memory_space_constraint(matrix, pltpu.HBM))
    recv = exchange(send, "col")
    send, piece = call(first_kernel, [(32, 4, 4, LANES), (4, LANES)], held, recv)
    recv = exchange(send, "row")
    qs, aq_rows, scals = {}, {}, {}
    for step in range(2, 9):
        args = [held, recv]
        if step in (2, 3):
            args.append(piece)
        if step > 2:
            args.append(scals[step - 2])
        args += [qs[i] for i in range(1, step - 1)] + [aq_rows[i] for i in range(1, step - 2)]
        groups = 4 if step in (2, 3) else 3
        outs = [(16 if step % 2 == 0 else 32, groups, 4, LANES), whole]
        if step > 2:
            outs.append((16, LANES))
        outs.append((16, LANES))
        if step in (3, 4):
            outs.append((32 if step == 3 else 64, LANES))
        if step == 2:
            outs.append((4, LANES))
        result = list(call(functools.partial(step_kernel, step), outs, *args))
        send = result.pop(0)
        qs[step - 1] = result.pop(0)
        if step > 2:
            aq_rows[step - 2] = result.pop(0)
        scals[step - 1] = result.pop(0)
        if step == 3:
            edge_r = result.pop(0)
        if step == 4:
            edge_c = result.pop(0)
        if step == 2:
            piece = packed = result.pop(0)
        recv = exchange(send, "col" if step % 2 == 0 else "row")
    (send,) = call(last_send_kernel, [(32, 1, 4, LANES)], recv)
    last = exchange(send, "row")
    rows, cols = matrix.shape
    q, flag, reflect, side, left, right = call(
        panel_kernel,
        [whole, jax.ShapeDtypeStruct((8, LANES), F32), pltpu.HBM((8, rows), F32), (128, LANES)]
        + [VMEM((rows, LANES), jnp.bfloat16), VMEM((96, cols), jnp.bfloat16)],
        recv,
        packed,
        edge_r,
        edge_c,
        *[scals[i] for i in range(1, 8)],
        *[qs[i] for i in range(1, 8)],
        *[aq_rows[i] for i in range(1, 7)],
        scratch=[(16, LANES)],
        flops=40000000,
    )
    trailing = pl.pallas_call(
        trailing_kernel,
        out_shape=jax.ShapeDtypeStruct(matrix.shape, F32),
        in_specs=[pl.BlockSpec(memory_space=VMEM)] * 6,
        out_specs=pl.BlockSpec(memory_space=pltpu.HBM),
        scratch_shapes=[VMEM(matrix.shape, F32), pltpu.SemaphoreType.DMA((8,))],
        compiler_params=pltpu.CompilerParams(vmem_limit_bytes=LIMIT),
    )(held, last, q, side, left, right)
    if not GUARD:
        return trailing, reflect.T
    _, trailing, reflect = lax.while_loop(
        lambda state: state[0],
        lambda state: (jnp.bool_(False), *column_by_column(matrix)),
        (flag[0, 0] < 0.5, trailing, reflect),
    )
    return trailing, reflect.T


def as_it_is(x_ref, out_ref):
    out_ref[...] = x_ref[...]


def of_everyone(shard, axis):
    size = lax.axis_size(axis)
    return exchange(jnp.broadcast_to(shard[None], (size, *shard.shape)), axis)


def column_by_column(matrix):
    rows, cols = matrix.shape
    row_at, col_at = lax.axis_index("row") * rows, lax.axis_index("col") * cols
    panel = of_everyone(matrix[:, :COLS].T, "col")[0]
    panel = of_everyone(panel, "row").transpose(1, 0, 2).reshape(COLS, N)
    positions = jnp.arange(N, dtype=jnp.int32)

    def one(column, state):
        reflect, companion = state

        def row(x):
            return lax.dynamic_index_in_dim(x, column, 0, keepdims=False)

        def entries(x):
            return lax.dynamic_index_in_dim(x, column, 1, keepdims=True)

        current = row(panel) - jnp.sum(
            reflect * entries(companion) + companion * entries(reflect), axis=0
        )
        below = jnp.where(positions > column, current, 0.0)
        leading = jnp.sum(jnp.where(positions == column + 1, current, 0.0))
        length = jnp.sqrt(jnp.sum(below * below))
        vector = below + jnp.where(positions == column + 1, length, 0.0)
        scaling = 1.0 / (length * (length + leading))
        along_rows_here = lax.dynamic_slice_in_dim(vector, row_at, rows, 0)
        image = jnp.sum(matrix * along_rows_here[:, None], axis=0)
        image = of_everyone(image, "row").sum(axis=0)
        image = of_everyone(image, "col").reshape(N)
        to_reflect = jnp.sum(companion * vector, axis=1, keepdims=True)
        to_companion = jnp.sum(reflect * vector, axis=1, keepdims=True)
        pushed = scaling * (
            image - jnp.sum(reflect * to_reflect + companion * to_companion, axis=0)
        )
        update = pushed - 0.5 * scaling * jnp.sum(pushed * vector) * vector
        reflect = lax.dynamic_update_index_in_dim(reflect, vector, column, 0)
        return reflect, lax.dynamic_update_index_in_dim(companion, update, column, 0)

    zero = jnp.zeros((COLS, N), F32)
    reflect, companion = lax.fori_loop(0, COLS, one, (zero, zero))
    reflect_rows = lax.dynamic_slice_in_dim(reflect, row_at, rows, 1)
    companion_rows = lax.dynamic_slice_in_dim(companion, row_at, rows, 1)
    reflect_cols = lax.dynamic_slice_in_dim(reflect, col_at, cols, 1)
    companion_cols = lax.dynamic_slice_in_dim(companion, col_at, cols, 1)

    def subtract(k, trailing):
        def row(x):
            return lax.dynamic_index_in_dim(x, k, 0, keepdims=False)

        return (
            trailing
            - row(reflect_rows)[:, None] * row(companion_cols)[None, :]
            - row(companion_rows)[:, None] * row(reflect_cols)[None, :]
        )

    (reflect_rows,) = call(as_it_is, [(COLS, rows)], reflect_rows, pinned=False)
    return lax.fori_loop(0, COLS, subtract, matrix), reflect_rows


def solution(mesh):
    placed = (P("row", "col"),)
    return jax.shard_map(
        local,
        mesh=mesh,
        in_specs=placed,
        out_specs=(P("row", "col"), P("row", None)),
        check_vma=False,
    )
```

```python
import functools

import jax
import jax.numpy as jnp
from jax import lax
from jax.experimental import pallas as pl
from jax.experimental.pallas import tpu as pltpu
from jax.sharding import PartitionSpec as P


N = 16384
COLS = 8
LANES = 128
F32 = jnp.float32
VMEM = pltpu.VMEM
LIMIT = 16 << 20
GUARD = True
GROWTH = 16.0
PIVOT = 0.05


def places():
    return lax.axis_index("row"), lax.axis_index("col")


def total(x):
    return jnp.sum(jnp.sum(x, axis=0, keepdims=True), axis=1, keepdims=True)


def iota(shape, dim):
    return lax.broadcasted_iota(jnp.int32, shape, dim)


def without_first(x, owner):
    hit = (iota(x.shape, 0) == 0) & (iota(x.shape, 1) == 0)
    if owner is not None:
        hit = hit & (owner == 0)
    return jnp.where(hit, 0.0, x)


def times_rows(a_ref, x):
    upright = jnp.concatenate([x, jnp.zeros_like(x)], axis=0).T
    out = []
    for t in range(8):
        acc = jnp.zeros((8, LANES), F32)
        for q in range(4):
            block = a_ref[q * LANES : (q + 1) * LANES, t * LANES : (t + 1) * LANES]
            acc = acc + jnp.sum((block * upright[:, q : q + 1]).reshape(16, 8, LANES), axis=0)
        out.append(jnp.sum(acc, axis=0, keepdims=True))
    return jnp.concatenate(out, axis=0)


def times_cols(a_ref, x):
    out = []
    for q in range(4):
        acc = jnp.zeros((LANES, LANES), F32)
        for t in range(8):
            block = a_ref[q * LANES : (q + 1) * LANES, t * LANES : (t + 1) * LANES]
            acc = acc + block * x[t : t + 1, :]
        out.append(jnp.sum(acc.T, axis=0, keepdims=True))
    return jnp.concatenate(out, axis=0)


def send_all(send_ref, first, parts):
    for member in range(send_ref.shape[0]):
        for k, part in enumerate(parts):
            send_ref[member, first + k] = part


def halves(x):
    return [x[:4], x[4:]]


def along_cols(recv_ref):
    s = jnp.sum(recv_ref[:, 0:2], axis=0)
    return jnp.concatenate([s[0], s[1]], axis=0)


def along_rows(recv_ref):
    return jnp.sum(recv_ref[:, 0], axis=0)


def whole_from_rows(recv_ref, group):
    return jnp.concatenate([recv_ref[r, group] for r in range(recv_ref.shape[0])], axis=0)


def whole_from_cols(recv_ref, group):
    return jnp.concatenate(
        [recv_ref[c, group + k] for c in range(recv_ref.shape[0]) for k in range(2)], axis=0
    )


def start_kernel(a_ref, send_ref, held_ref, slab_ref, sems):
    copy = pltpu.make_async_copy(a_ref.at[:, pl.ds(0, LANES)], slab_ref, sems.at[0])
    copy.start()
    hold = pltpu.make_async_copy(a_ref, held_ref, sems.at[1])
    hold.start()
    copy.wait()
    left = [slab_ref[q * LANES : (q + 1) * LANES, :].T for q in range(4)]
    column = jnp.concatenate([x[0:1] for x in left], axis=0)
    corner = slab_ref[0:16, :]
    packed = jnp.zeros((1, LANES), F32)
    for j in range(COLS):
        lanes = iota((1, LANES), 1)
        entry = jnp.where(lanes < 16, corner[j + 1 : j + 2], 0.0)
        packed = packed + (pltpu.roll(entry, 16 * j, 1) if j else entry)
    blank = jnp.zeros((1, LANES), F32)
    for member in range(16):
        j, half = member // 2, member % 2
        rows = [left[2 * half + k][j + 1 : j + 2] for k in range(2)]
        send_ref[member, 0] = column
        send_ref[member, 1] = jnp.concatenate([*rows, packed, blank], axis=0)
    hold.wait()


def first_kernel(a_ref, recv_ref, send_ref, piece_ref):
    ids_ref = places()
    column = recv_ref[0, 0]
    piece_ref[...] = recv_ref[0, 1]
    packed = recv_ref[0, 1][2:3]
    send_all(send_ref, 0, halves(times_rows(a_ref, without_first(column, ids_ref[0]))))
    send_all(send_ref, 2, [column])
    blank = jnp.zeros((1, LANES), F32)
    for member in range(32):
        j, quarter = member // 4, member % 4
        rows = [
            a_ref[j + 1 : j + 2, (2 * quarter + k) * LANES : (2 * quarter + k + 1) * LANES]
            for k in range(2)
        ]
        send_ref[member, 3] = jnp.concatenate([*rows, packed, blank], axis=0)


def coefficient(scal, k):
    return scal[k : k + 1, 0:1]


def settle(step, given, scal, qs):
    u = without_first(given, None) if step == 2 else given
    zero = jnp.zeros((1, LANES), F32)
    w, cs, growth = u, {}, 0.0
    known = range(1, step - 1)
    rows = [jnp.sum(u * qs[i], axis=0, keepdims=True) for i in known]
    rows = rows + [zero] * (7 - len(rows)) + [jnp.sum(u * u, axis=0, keepdims=True)]
    sums = jnp.sum(jnp.concatenate(rows, axis=0), axis=1, keepdims=True)
    squared = sums[7:8, 0:1]
    if step == 2:
        alpha = shift = given[0:1, 0:1]
    else:
        for i in known:
            cs[i] = sums[i - 1 : i, 0:1]
            w = w - cs[i] * qs[i]
        growth = jnp.sum(jnp.where(iota((8, 1), 0) < 7, sums * sums, 0.0), axis=0, keepdims=True)
        squared = squared - growth
        alpha, before = cs[step - 2] + coefficient(scal, 9), coefficient(scal, 10)
        smaller = jnp.where(jnp.abs(alpha) < jnp.abs(before), alpha, before)
        shift = jnp.where(alpha * before > 0.0, smaller, 0.0)
    length = jnp.sqrt(squared)
    inverse = 1.0 / length
    growth = 1.0 + growth * inverse * inverse
    if step > 2:
        growth = growth * coefficient(scal, 11)
    out = [zero + length] + [zero + cs[i] if i in cs else zero for i in range(1, 8)]
    out = out + [zero + x for x in (inverse, shift, alpha, growth)] + [zero] * 4
    return w * inverse, length, inverse, shift, cs, jnp.concatenate(out, axis=0)


def given_rows(recv_ref, by_rows):
    row_index, col_index = places()
    if by_rows:
        group = 2 if recv_ref.shape[1] > 2 else 0
        here = recv_ref[row_index, group]
        there = [recv_ref[2 * col_index + k, group] for k in range(2)]
        first = recv_ref[0, group][0:1]
    else:
        here = recv_ref[row_index // 2, 1 + row_index % 2]
        there = [recv_ref[col_index, 1 + k] for k in range(2)]
        first = recv_ref[0, 1][0:1]
    return jnp.concatenate([here, *there, first, jnp.zeros((3, LANES), F32)], axis=0)


def kept_rows(ref):
    row_index, col_index = places()
    here, there = ref[pl.ds(4 * row_index, 4), :], ref[pl.ds(8 * col_index, 8), :]
    return jnp.concatenate([here, there, ref[0:1, :], jnp.zeros((3, LANES), F32)], axis=0)


def product_rows(step, recv_ref, scal, q_refs):
    out = given_rows(recv_ref, step % 2 == 0)
    out = out + coefficient(scal, 9) * kept_rows(q_refs[step - 2])
    if step > 3:
        return out + coefficient(scal, 0) * kept_rows(q_refs[step - 3])
    row_index, col_index = places()
    rows, lanes = iota(out.shape, 0), iota(out.shape, 1)
    start = ((rows == 0) & (row_index == 0)) | ((rows == 4) & (col_index == 0)) | (rows == 12)
    return out + jnp.where(start & (lanes == 0), coefficient(scal, 0), 0.0)


def step_kernel(step, *refs):
    refs = list(refs)
    a_ref, recv_ref = refs[:2]
    del refs[:2]
    row_index, col_index = places()
    piece_ref = refs.pop(0) if step == 2 else None
    scal = refs.pop(0)[...] if step > 2 else None
    q_refs = {i: refs.pop(0) for i in range(1, step - 1)}
    rows_refs = {i: refs.pop(0) for i in range(1, step - 2)}
    send_ref = refs.pop(0)
    q_ref = refs.pop(0)
    if step > 2:
        rows_refs[step - 2] = refs.pop(0)
    scal_ref = refs.pop(0)
    edge_ref = refs.pop(0) if step == 3 else None
    new_piece_ref = refs.pop(0) if step == 2 else None

    even = step % 2 == 0
    if even:
        y_here, given = along_cols(recv_ref), whole_from_rows(recv_ref, 2)
        chunk, count, part = col_index, 8, slice(4, 12)
    else:
        y_here, given = along_rows(recv_ref), whole_from_cols(recv_ref, 1)
        chunk, count, part = row_index, 4, slice(0, 4)
    if step > 2:
        rows_refs[step - 2][...] = product_rows(step, recv_ref, scal, q_refs)
    q, length, inverse, shift, cs, scal_out = settle(
        step, given, scal, {i: r[...] for i, r in q_refs.items()}
    )
    q_ref[...] = q
    scal_ref[...] = scal_out
    at = pl.ds(chunk * count, count)
    here = y_here
    for i in cs:
        here = here - cs[i] * rows_refs[i][part, :]
    q_here = without_first(given_rows(recv_ref, even)[part], chunk)
    for i in cs:
        q_here = q_here - cs[i] * q_refs[i][at, :]
    here = (here - shift * q_here) * inverse
    if step > 2:
        here = here - length * q_refs[step - 2][at, :]
    here = without_first(here, chunk)
    if even:
        send_all(send_ref, 0, [times_cols(a_ref, here)])
        send_all(send_ref, 1, halves(here))
    else:
        send_all(send_ref, 0, halves(times_rows(a_ref, here)))
        send_all(send_ref, 2, [here])
    if step == 2:
        send_all(send_ref, 3, [piece_ref[...]])
    if step == 2:
        new_piece_ref[...] = recv_ref[0, 3]
    if step == 3:
        edge_ref[...] = jnp.concatenate([recv_ref[c, 3][0:2] for c in range(16)], axis=0)


def last_send_kernel(recv_ref, piece_ref, send_ref):
    send_all(send_ref, 0, [along_rows(recv_ref), piece_ref[...]])


def sign(k):
    return -1.0 if k % 2 else 1.0


def product(x, y):
    return lax.dot_general(
        x,
        y,
        (((0,), (0,)), ((), ())),
        precision=lax.Precision.HIGHEST,
        preferred_element_type=F32,
    )


def rows_at(refs, row):
    blank = jnp.zeros((1, LANES), F32)
    return jnp.concatenate(
        [sign(k) * refs[k][pl.ds(row, 1), :] if k in refs else blank for k in range(1, 9)], axis=0
    )


def d_tile(q_refs, row):
    lanes, ks = iota((8, LANES), 1), iota((8, LANES), 0)
    unit = jnp.where((lanes == ks + 1) & (row == 0), 1.0, 0.0)
    return unit - rows_at(q_refs, row)


def three(x):
    high = x.astype(jnp.bfloat16).astype(F32)
    middle = (x - high).astype(jnp.bfloat16).astype(F32)
    low = (x - high - middle).astype(jnp.bfloat16).astype(F32)
    return high, middle, low


def panel_kernel(*refs):
    row_index, col_index = places()
    refs = list(refs)
    refs.insert(0, None)
    recv_ref, packed_ref, edge_r_ref = refs[1:4]
    scal_refs = {i: refs[3 + i] for i in range(1, 8)}
    q_refs = {i: refs[10 + i] for i in range(1, 8)}
    aq_rows = {i: refs[17 + i] for i in range(1, 7)}
    q_out, flag_ref, reflect_ref, side_ref, left_ref, right_ref, rows_out = refs[24:31]
    q, length, _, _, cs, scal = settle(
        9, whole_from_cols(recv_ref, 1), scal_refs[7][...], {i: r[...] for i, r in q_refs.items()}
    )
    q_out[...] = q
    rows_out[...] = product_rows(9, recv_ref, scal_refs[7][...], q_refs)
    aq_rows[7] = rows_out
    rest = jnp.zeros((16, LANES), F32)
    for i in range(1, 8):
        rest = rest + cs[i] * aq_rows[i][...]
    side_ref[96:104, :] = scal[8:16]
    side_ref[104:120, :] = rest
    side_ref[120:128, :] = jnp.zeros((8, LANES), F32) + cs[7] * length
    q_refs[8] = q_out
    lanes, ks = iota((8, LANES), 1), iota((8, LANES), 0)
    top = d_tile(q_refs, 0)
    work = jnp.where(lanes < 8, pltpu.roll(top, LANES - 1, 1), 0.0)
    work = work + jnp.where(lanes == ks + 8, 1.0, 0.0)
    to_reflect = jnp.zeros((8, LANES), F32)
    pivot = jnp.ones((1, 1), F32)
    for k in range(8):
        row = work[k : k + 1]
        pivot = jnp.minimum(pivot, row[:, k : k + 1])
        beta = (scal if k == 7 else scal_refs[k + 1])[0:1, :]
        to_reflect = jnp.where(ks == k, row * beta, to_reflect)
        row = row / row[:, k : k + 1]
        column = jnp.where(ks == k, 0.0, work)[:, k : k + 1]
        work = jnp.where(ks == k, row, work - column * row)
    sound = (scal[11:12, 0:1] <= GROWTH) & (pivot >= PIVOT)
    flag_ref[...] = jnp.zeros((8, LANES), F32) + jnp.where(sound, 1.0, 0.0)
    factor = pltpu.roll(work, LANES - 8, 1)[:, 0:8]
    flipped = jnp.concatenate(
        [jnp.where(lanes < 8, pltpu.roll(work, LANES - 8, 1), 0.0), jnp.zeros((LANES - 8, LANES), F32)],
        axis=0,
    ).T[0:8, 0:8]
    to_reflect = jnp.where(lanes < 8, pltpu.roll(to_reflect, LANES - 8, 1), 0.0)
    inner = jnp.zeros((8, LANES), F32)
    packed = packed_ref[2:3]
    for k in range(8):
        entry = pltpu.roll(packed, LANES - 16 * k, 1) if k else packed
        inner = jnp.where(ks == k, entry, inner)
    used = (lanes >= 1) & (lanes <= 8)
    inner = jnp.where(used, inner, 0.0)
    cross = jnp.where(used, rows_at(aq_rows, 12), 0.0)
    inner = pltpu.roll(inner - cross, LANES - 1, 1)
    cross = pltpu.roll(cross, LANES - 1, 1)
    square = jnp.concatenate([cross, jnp.zeros((LANES - 8, LANES), F32)], axis=0)
    inner = inner - square.T[0:8]
    for k in range(1, 8):
        source = scal if k == 7 else scal_refs[k + 1]
        near = ((ks == k - 1) & (lanes == k)) | ((ks == k) & (lanes == k - 1))
        inner = inner - jnp.where(near, source[0:1, :], 0.0)
        alpha = source[10:11, :]
        inner = inner + jnp.where((ks == k - 1) & (lanes == k - 1), alpha, 0.0)
    inner = inner[:, 0:8]
    core = product(factor, product(inner, factor))

    def tiles(base, count, edge_ref, first, kept):
        ds, ys = [], []
        for t in range(count):
            row = base + t
            d = d_tile(q_refs, row)
            ad = -rows_at(aq_rows, kept + t)
            if edge_ref is not None:
                ad = ad + jnp.concatenate(
                    [edge_ref[count * k + t : count * k + t + 1, :] for k in range(8)], axis=0
                )
            ds.append(d)
            ys.append(product(factor, ad) - 0.5 * product(core, d))
            side_ref[first + 8 * t : first + 8 * t + 8, :] = product(flipped, d)
        return ds, ys

    ds, ys = tiles(4 * row_index, 4, edge_r_ref, 0, 0)
    for t in range(4):
        high, middle, low = three(jnp.concatenate([ds[t], ys[t]], axis=0))
        stack = [high, high, middle, middle, high, low, jnp.zeros((32, LANES), F32)]
        at = slice(t * LANES, (t + 1) * LANES)
        left_ref[at, 0:LANES] = jnp.concatenate(stack, axis=0).T.astype(jnp.bfloat16)
        high, middle, low = three(side_ref[8 * t : 8 * t + 8, :])
        stack = [high, high, middle, middle, high, low, jnp.zeros((80, LANES), F32)]
        left_ref[at, LANES:] = jnp.concatenate(stack, axis=0).T.astype(jnp.bfloat16)
        out = jnp.zeros((8, LANES), F32)
        for k in range(8):
            out = out + to_reflect[:, k : k + 1] * ds[t][k : k + 1, :]
        out = jnp.where((4 * row_index + t == 0) & (lanes <= ks), 0.0, out)
        reflect_ref[:, t * LANES : (t + 1) * LANES] = out
    ds, ys = tiles(8 * col_index, 8, None, 32, 4)
    for t in range(8):
        high, middle, low = three(jnp.concatenate([ys[t], ds[t]], axis=0))
        stack = [high, middle, high, middle, low, high]
        at = slice(t * LANES, (t + 1) * LANES)
        right_ref[:, at] = jnp.concatenate(stack, axis=0).astype(jnp.bfloat16)


def trailing_kernel(
    a_ref, recv_ref, q_ref, side_ref, left_ref, right_ref, out_ref, block_ref, edge_ref, sems
):
    for t in range(8):
        members = [divmod(8 * k + t, 2) for k in range(8)]
        high, middle, low = three(
            jnp.concatenate([recv_ref[r, 1][i : i + 1] for r, i in members], axis=0)
        )
        stack = jnp.concatenate([high, middle, high, middle, low, high], axis=0)
        edge_ref[:, t * LANES : (t + 1) * LANES] = stack.astype(jnp.bfloat16)
    inverse = coefficient(side_ref, 96)
    aq = (given_rows(recv_ref, True) - side_ref[104:120, :]) * inverse
    alpha = total(q_ref[...] * whole_from_rows(recv_ref, 0)) - coefficient(side_ref, 120)
    alpha = alpha * inverse
    lanes = iota((1, LANES), 1)
    shifted = pltpu.roll(aq[12:13, :], LANES - 1, 1)
    added = jnp.where(lanes == 7, 0.5 * alpha, 0.0) - jnp.where(lanes < 8, shifted, 0.0)
    added = jnp.concatenate([added, jnp.zeros((7, LANES), F32)], axis=0).T[0:8, 0:1]

    def last(count, first, kept):
        return [
            -aq[kept + t : kept + t + 1, :]
            - jnp.sum(added * side_ref[first + 8 * t : first + 8 * t + 8, :], axis=0, keepdims=True)
            for t in range(count)
        ]

    ws_r = last(4, 0, 0)
    ws_c = last(8, 32, 4)
    blank = jnp.zeros((6, LANES), F32)
    copies = []
    for q in range(4):
        upright = jnp.concatenate([side_ref[8 * q + 7 : 8 * q + 8, :], ws_r[q], blank], axis=0).T
        for half in range(2):
            at = slice(q * LANES + half * 64, q * LANES + half * 64 + 64)
            piece = upright[half * 64 : half * 64 + 64]
            change = jnp.dot(left_ref[at, 0:96], right_ref[...], preferred_element_type=F32)
            edge = left_ref[at, LANES : LANES + 48]
            change = change + jnp.dot(edge, edge_ref[...], preferred_element_type=F32)
            for t in range(8):
                to = slice(t * LANES, (t + 1) * LANES)
                block_ref[at, to] = (
                    a_ref[at, to]
                    - change[:, to]
                    - piece[:, 0:1] * ws_c[t]
                    - piece[:, 1:2] * side_ref[39 + 8 * t : 40 + 8 * t, :]
                )
            copy = pltpu.make_async_copy(
                block_ref.at[at, :], out_ref.at[at, :], sems.at[2 * q + half]
            )
            copy.start()
            copies.append(copy)
    for copy in copies:
        copy.wait()


def call(kernel, outs, *args, scratch=(), pinned=True, flops=1000):
    def shape(x):
        if not isinstance(x, tuple):
            return x
        return VMEM(x, F32) if pinned else jax.ShapeDtypeStruct(x, F32)

    return pl.pallas_call(
        kernel,
        out_shape=[shape(x) for x in outs],
        in_specs=[pl.BlockSpec(memory_space=VMEM)] * len(args),
        out_specs=[pl.BlockSpec(memory_space=VMEM)] * len(outs),
        scratch_shapes=[VMEM(s, F32) for s in scratch],
        compiler_params=pltpu.CompilerParams(vmem_limit_bytes=LIMIT),
        cost_estimate=pl.CostEstimate(flops=flops, bytes_accessed=1000, transcendentals=0),
    )(*args)


def exchange(x, axis):
    return lax.all_to_all(x, axis, 0, 0, tiled=True)


def local(matrix):
    whole = (N // LANES, LANES)
    send, held = pl.pallas_call(
        start_kernel,
        out_shape=[VMEM((16, 2, 4, LANES), F32), VMEM(matrix.shape, F32)],
        in_specs=[pl.BlockSpec(memory_space=pltpu.HBM)],
        out_specs=[pl.BlockSpec(memory_space=VMEM)] * 2,
        scratch_shapes=[VMEM((matrix.shape[0], LANES), F32), pltpu.SemaphoreType.DMA((2,))],
        compiler_params=pltpu.CompilerParams(vmem_limit_bytes=LIMIT),
    )(pltpu.with_memory_space_constraint(matrix, pltpu.HBM))
    recv = exchange(send, "col")
    send, piece = call(first_kernel, [(32, 4, 4, LANES), (4, LANES)], held, recv)
    recv = exchange(send, "row")
    qs, aq_rows, scals = {}, {}, {}
    for step in range(2, 9):
        args = [held, recv]
        if step == 2:
            args.append(piece)
        if step > 2:
            args.append(scals[step - 2])
        args += [qs[i] for i in range(1, step - 1)] + [aq_rows[i] for i in range(1, step - 2)]
        groups = 4 if step == 2 else 3
        outs = [(16 if step % 2 == 0 else 32, groups, 4, LANES), whole]
        if step > 2:
            outs.append((16, LANES))
        outs.append((16, LANES))
        if step == 3:
            outs.append((32, LANES))
        if step == 2:
            outs.append((4, LANES))
        result = list(call(functools.partial(step_kernel, step), outs, *args))
        send = result.pop(0)
        qs[step - 1] = result.pop(0)
        if step > 2:
            aq_rows[step - 2] = result.pop(0)
        scals[step - 1] = result.pop(0)
        if step == 3:
            edge_r = result.pop(0)
        if step == 2:
            piece = packed = result.pop(0)
        recv = exchange(send, "col" if step % 2 == 0 else "row")
    (send,) = call(last_send_kernel, [(32, 2, 4, LANES)], recv, packed)
    last = exchange(send, "row")
    rows, cols = matrix.shape
    q, flag, reflect, side, left, right = call(
        panel_kernel,
        [whole, jax.ShapeDtypeStruct((8, LANES), F32), pltpu.HBM((8, rows), F32), (128, LANES)]
        + [VMEM((rows, 2 * LANES), jnp.bfloat16), VMEM((96, cols), jnp.bfloat16)],
        recv,
        packed,
        edge_r,
        *[scals[i] for i in range(1, 8)],
        *[qs[i] for i in range(1, 8)],
        *[aq_rows[i] for i in range(1, 7)],
        scratch=[(16, LANES)],
        flops=40000000,
    )
    trailing = pl.pallas_call(
        trailing_kernel,
        out_shape=jax.ShapeDtypeStruct(matrix.shape, F32),
        in_specs=[pl.BlockSpec(memory_space=VMEM)] * 6,
        out_specs=pl.BlockSpec(memory_space=pltpu.HBM),
        scratch_shapes=[
            VMEM(matrix.shape, F32),
            VMEM((48, cols), jnp.bfloat16),
            pltpu.SemaphoreType.DMA((8,)),
        ],
        compiler_params=pltpu.CompilerParams(vmem_limit_bytes=LIMIT),
    )(held, last, q, side, left, right)
    if not GUARD:
        return trailing, reflect.T
    _, trailing, reflect = lax.while_loop(
        lambda state: state[0],
        lambda state: (jnp.bool_(False), *column_by_column(matrix)),
        (flag[0, 0] < 0.5, trailing, reflect),
    )
    return trailing, reflect.T


def as_it_is(x_ref, out_ref):
    out_ref[...] = x_ref[...]


def of_everyone(shard, axis):
    size = lax.axis_size(axis)
    return exchange(jnp.broadcast_to(shard[None], (size, *shard.shape)), axis)


def column_by_column(matrix):
    rows, cols = matrix.shape
    row_at, col_at = lax.axis_index("row") * rows, lax.axis_index("col") * cols
    panel = of_everyone(matrix[:, :COLS].T, "col")[0]
    panel = of_everyone(panel, "row").transpose(1, 0, 2).reshape(COLS, N)
    positions = jnp.arange(N, dtype=jnp.int32)

    def one(column, state):
        reflect, companion = state

        def row(x):
            return lax.dynamic_index_in_dim(x, column, 0, keepdims=False)

        def entries(x):
            return lax.dynamic_index_in_dim(x, column, 1, keepdims=True)

        current = row(panel) - jnp.sum(
            reflect * entries(companion) + companion * entries(reflect), axis=0
        )
        below = jnp.where(positions > column, current, 0.0)
        leading = jnp.sum(jnp.where(positions == column + 1, current, 0.0))
        length = jnp.sqrt(jnp.sum(below * below))
        vector = below + jnp.where(positions == column + 1, length, 0.0)
        scaling = 1.0 / (length * (length + leading))
        along_rows_here = lax.dynamic_slice_in_dim(vector, row_at, rows, 0)
        image = jnp.sum(matrix * along_rows_here[:, None], axis=0)
        image = of_everyone(image, "row").sum(axis=0)
        image = of_everyone(image, "col").reshape(N)
        to_reflect = jnp.sum(companion * vector, axis=1, keepdims=True)
        to_companion = jnp.sum(reflect * vector, axis=1, keepdims=True)
        pushed = scaling * (
            image - jnp.sum(reflect * to_reflect + companion * to_companion, axis=0)
        )
        update = pushed - 0.5 * scaling * jnp.sum(pushed * vector) * vector
        reflect = lax.dynamic_update_index_in_dim(reflect, vector, column, 0)
        return reflect, lax.dynamic_update_index_in_dim(companion, update, column, 0)

    zero = jnp.zeros((COLS, N), F32)
    reflect, companion = lax.fori_loop(0, COLS, one, (zero, zero))
    reflect_rows = lax.dynamic_slice_in_dim(reflect, row_at, rows, 1)
    companion_rows = lax.dynamic_slice_in_dim(companion, row_at, rows, 1)
    reflect_cols = lax.dynamic_slice_in_dim(reflect, col_at, cols, 1)
    companion_cols = lax.dynamic_slice_in_dim(companion, col_at, cols, 1)

    def subtract(k, trailing):
        def row(x):
            return lax.dynamic_index_in_dim(x, k, 0, keepdims=False)

        return (
            trailing
            - row(reflect_rows)[:, None] * row(companion_cols)[None, :]
            - row(companion_rows)[:, None] * row(reflect_cols)[None, :]
        )

    (reflect_rows,) = call(as_it_is, [(COLS, rows)], reflect_rows, pinned=False)
    return lax.fori_loop(0, COLS, subtract, matrix), reflect_rows


def solution(mesh):
    placed = (P("row", "col"),)
    return jax.shard_map(
        local,
        mesh=mesh,
        in_specs=placed,
        out_specs=(P("row", "col"), P("row", None)),
        check_vma=False,
    )
```

```python
import functools

import jax
import jax.numpy as jnp
from jax import lax
from jax.experimental import pallas as pl
from jax.experimental.pallas import tpu as pltpu
from jax.sharding import PartitionSpec as P


N = 16384
COLS = 8
LANES = 128
F32 = jnp.float32
VMEM = pltpu.VMEM
LIMIT = 16 << 20
GUARD = True
GROWTH = 16.0
PIVOT = 0.05


def places():
    return lax.axis_index("row"), lax.axis_index("col")


def total(x):
    return jnp.sum(jnp.sum(x, axis=0, keepdims=True), axis=1, keepdims=True)


def iota(shape, dim):
    return lax.broadcasted_iota(jnp.int32, shape, dim)


def without_first(x, owner):
    hit = (iota(x.shape, 0) == 0) & (iota(x.shape, 1) == 0)
    if owner is not None:
        hit = hit & (owner == 0)
    return jnp.where(hit, 0.0, x)


def times_rows(a_ref, x):
    upright = jnp.concatenate([x, jnp.zeros_like(x)], axis=0).T
    out = []
    for t in range(8):
        acc = jnp.zeros((8, LANES), F32)
        for q in range(4):
            block = a_ref[q * LANES : (q + 1) * LANES, t * LANES : (t + 1) * LANES]
            acc = acc + jnp.sum((block * upright[:, q : q + 1]).reshape(16, 8, LANES), axis=0)
        out.append(jnp.sum(acc, axis=0, keepdims=True))
    return jnp.concatenate(out, axis=0)


def times_cols(a_ref, x):
    out = []
    for q in range(4):
        acc = jnp.zeros((LANES, LANES), F32)
        for t in range(8):
            block = a_ref[q * LANES : (q + 1) * LANES, t * LANES : (t + 1) * LANES]
            acc = acc + block * x[t : t + 1, :]
        out.append(jnp.sum(acc.T, axis=0, keepdims=True))
    return jnp.concatenate(out, axis=0)


def send_all(send_ref, first, x):
    height = send_ref.shape[2]
    for member in range(send_ref.shape[0]):
        for k in range(x.shape[0] // height):
            send_ref[member, first // height + k] = x[k * height : (k + 1) * height]


def taken(recv_ref, member, first, count):
    height = recv_ref.shape[2]
    return [recv_ref[member, first // height + k] for k in range(count // height)]


def summed(recv_ref, count):
    height = recv_ref.shape[2]
    blocks = [jnp.sum(recv_ref[:, k], axis=0) for k in range(count // height)]
    return jnp.concatenate(blocks, axis=0)


def gathered(recv_ref, first, count):
    members = range(recv_ref.shape[0])
    return jnp.concatenate(
        [block for m in members for block in taken(recv_ref, m, first, count)], axis=0
    )


def start_kernel(a_ref, send_ref, held_ref, slab_ref, sems):
    copy = pltpu.make_async_copy(a_ref.at[:, pl.ds(0, LANES)], slab_ref, sems.at[0])
    copy.start()
    hold = pltpu.make_async_copy(a_ref, held_ref, sems.at[1])
    hold.start()
    copy.wait()
    left = [slab_ref[q * LANES : (q + 1) * LANES, :].T for q in range(4)]
    column = jnp.concatenate([x[0:1] for x in left], axis=0)
    corner = slab_ref[0:16, :]
    packed = jnp.zeros((1, LANES), F32)
    for j in range(COLS):
        lanes = iota((1, LANES), 1)
        entry = jnp.where(lanes < 16, corner[j + 1 : j + 2], 0.0)
        packed = packed + (pltpu.roll(entry, 16 * j, 1) if j else entry)
    blank = jnp.zeros((1, LANES), F32)
    for member in range(16):
        j, half = member // 2, member % 2
        rows = [left[2 * half + k][j + 1 : j + 2] for k in range(2)]
        send_ref[member, 0] = column
        send_ref[member, 1] = jnp.concatenate([*rows, packed, blank], axis=0)
    hold.wait()


def first_kernel(a_ref, recv_ref, send_ref, piece_ref):
    ids_ref = places()
    column = recv_ref[0, 0]
    piece_ref[...] = recv_ref[0, 1]
    packed = recv_ref[0, 1][2:3]
    send_all(send_ref, 0, times_rows(a_ref, without_first(column, ids_ref[0])))
    send_all(send_ref, 8, column)
    blank = jnp.zeros((1, LANES), F32)
    for member in range(32):
        j, quarter = member // 4, member % 4
        rows = [
            a_ref[j + 1 : j + 2, (2 * quarter + k) * LANES : (2 * quarter + k + 1) * LANES]
            for k in range(2)
        ]
        send_ref[member, 3] = jnp.concatenate([*rows, packed, blank], axis=0)


def coefficient(scal, k):
    return scal[k : k + 1, 0:1]


def settle(step, given, scal, qs):
    u = without_first(given, None) if step == 2 else given
    zero = jnp.zeros((1, LANES), F32)
    w, cs, growth = u, {}, 0.0
    known = range(1, step - 1)
    rows = [jnp.sum(u * qs[i], axis=0, keepdims=True) for i in known]
    rows = rows + [zero] * (7 - len(rows)) + [jnp.sum(u * u, axis=0, keepdims=True)]
    sums = jnp.sum(jnp.concatenate(rows, axis=0), axis=1, keepdims=True)
    squared = sums[7:8, 0:1]
    if step == 2:
        alpha = shift = given[0:1, 0:1]
    else:
        for i in known:
            cs[i] = sums[i - 1 : i, 0:1]
            w = w - cs[i] * qs[i]
        growth = jnp.sum(jnp.where(iota((8, 1), 0) < 7, sums * sums, 0.0), axis=0, keepdims=True)
        squared = squared - growth
        alpha, before = cs[step - 2] + coefficient(scal, 9), coefficient(scal, 10)
        smaller = jnp.where(jnp.abs(alpha) < jnp.abs(before), alpha, before)
        shift = jnp.where(alpha * before > 0.0, smaller, 0.0)
    length = jnp.sqrt(squared)
    inverse = 1.0 / length
    growth = 1.0 + growth * inverse * inverse
    if step > 2:
        growth = growth * coefficient(scal, 11)
    out = [zero + length] + [zero + cs[i] if i in cs else zero for i in range(1, 8)]
    out = out + [zero + x for x in (inverse, shift, alpha, growth)] + [zero] * 4
    return w * inverse, length, inverse, shift, cs, jnp.concatenate(out, axis=0)


def given_rows(recv_ref, by_rows):
    row_index, col_index = places()
    height = recv_ref.shape[2]
    if by_rows:
        start = 8 if recv_ref.shape[1] * height > 8 else 0
        here = taken(recv_ref, row_index, start, 4)
        there = taken(recv_ref, 2 * col_index, start, 4) + taken(recv_ref, 2 * col_index + 1, start, 4)
    else:
        start, half = 4, row_index % 2 * (4 // height)
        here = [recv_ref[row_index // 2, half + (start // height + k)] for k in range(4 // height)]
        there = taken(recv_ref, col_index, start, 8)
    first = recv_ref[0, start // height][0:1]
    return jnp.concatenate([*here, *there, first, jnp.zeros((3, LANES), F32)], axis=0)


def kept_rows(ref):
    row_index, col_index = places()
    here, there = ref[pl.ds(4 * row_index, 4), :], ref[pl.ds(8 * col_index, 8), :]
    return jnp.concatenate([here, there, ref[0:1, :], jnp.zeros((3, LANES), F32)], axis=0)


def product_rows(step, recv_ref, scal, q_refs):
    out = given_rows(recv_ref, step % 2 == 0)
    out = out + coefficient(scal, 9) * kept_rows(q_refs[step - 2])
    if step > 3:
        return out + coefficient(scal, 0) * kept_rows(q_refs[step - 3])
    row_index, col_index = places()
    rows, lanes = iota(out.shape, 0), iota(out.shape, 1)
    start = ((rows == 0) & (row_index == 0)) | ((rows == 4) & (col_index == 0)) | (rows == 12)
    return out + jnp.where(start & (lanes == 0), coefficient(scal, 0), 0.0)


def step_kernel(step, *refs):
    refs = list(refs)
    a_ref, recv_ref = refs[:2]
    del refs[:2]
    row_index, col_index = places()
    piece_ref = refs.pop(0) if step == 2 else None
    scal = refs.pop(0)[...] if step > 2 else None
    q_refs = {i: refs.pop(0) for i in range(1, step - 1)}
    rows_refs = {i: refs.pop(0) for i in range(1, step - 2)}
    send_ref = refs.pop(0)
    q_ref = refs.pop(0)
    if step > 2:
        rows_refs[step - 2] = refs.pop(0)
    scal_ref = refs.pop(0)
    edge_ref = refs.pop(0) if step == 3 else None
    new_piece_ref = refs.pop(0) if step == 2 else None

    even = step % 2 == 0
    if even:
        y_here, given = summed(recv_ref, 8), gathered(recv_ref, 8, 4)
        chunk, count, part = col_index, 8, slice(4, 12)
    else:
        y_here, given = summed(recv_ref, 4), gathered(recv_ref, 4, 8)
        chunk, count, part = row_index, 4, slice(0, 4)
    if step > 2:
        rows_refs[step - 2][...] = product_rows(step, recv_ref, scal, q_refs)
    q, length, inverse, shift, cs, scal_out = settle(
        step, given, scal, {i: r[...] for i, r in q_refs.items()}
    )
    q_ref[...] = q
    scal_ref[...] = scal_out
    at = pl.ds(chunk * count, count)
    here = y_here
    for i in cs:
        here = here - cs[i] * rows_refs[i][part, :]
    q_here = without_first(given_rows(recv_ref, even)[part], chunk)
    for i in cs:
        q_here = q_here - cs[i] * q_refs[i][at, :]
    here = (here - shift * q_here) * inverse
    if step > 2:
        here = here - length * q_refs[step - 2][at, :]
    here = without_first(here, chunk)
    if even:
        send_all(send_ref, 0, times_cols(a_ref, here))
        send_all(send_ref, 4, here)
    else:
        send_all(send_ref, 0, times_rows(a_ref, here))
        send_all(send_ref, 8, here)
    if step == 2:
        send_all(send_ref, 12, piece_ref[0:2, :])
        new_piece_ref[...] = recv_ref[0, 3]
    if step == 3:
        edge_ref[...] = gathered(recv_ref, 12, 2)


def last_send_kernel(recv_ref, piece_ref, send_ref):
    send_all(send_ref, 0, summed(recv_ref, 4))
    send_all(send_ref, 4, piece_ref[0:2, :])


def sign(k):
    return -1.0 if k % 2 else 1.0


def product(x, y):
    return lax.dot_general(
        x,
        y,
        (((0,), (0,)), ((), ())),
        precision=lax.Precision.HIGHEST,
        preferred_element_type=F32,
    )


def rows_at(refs, row):
    blank = jnp.zeros((1, LANES), F32)
    return jnp.concatenate(
        [sign(k) * refs[k][pl.ds(row, 1), :] if k in refs else blank for k in range(1, 9)], axis=0
    )


def d_tile(q_refs, row):
    lanes, ks = iota((8, LANES), 1), iota((8, LANES), 0)
    unit = jnp.where((lanes == ks + 1) & (row == 0), 1.0, 0.0)
    return unit - rows_at(q_refs, row)


def three(x):
    high = x.astype(jnp.bfloat16).astype(F32)
    middle = (x - high).astype(jnp.bfloat16).astype(F32)
    low = (x - high - middle).astype(jnp.bfloat16).astype(F32)
    return high, middle, low


def panel_kernel(*refs):
    row_index, col_index = places()
    refs = list(refs)
    refs.insert(0, None)
    recv_ref, packed_ref, edge_r_ref = refs[1:4]
    scal_refs = {i: refs[3 + i] for i in range(1, 8)}
    q_refs = {i: refs[10 + i] for i in range(1, 8)}
    aq_rows = {i: refs[17 + i] for i in range(1, 7)}
    q_out, flag_ref, reflect_ref, side_ref, left_ref, right_ref, rows_out = refs[24:31]
    q, length, _, _, cs, scal = settle(
        9, gathered(recv_ref, 4, 8), scal_refs[7][...], {i: r[...] for i, r in q_refs.items()}
    )
    q_out[...] = q
    rows_out[...] = product_rows(9, recv_ref, scal_refs[7][...], q_refs)
    aq_rows[7] = rows_out
    rest = jnp.zeros((16, LANES), F32)
    for i in range(1, 8):
        rest = rest + cs[i] * aq_rows[i][...]
    side_ref[96:104, :] = scal[8:16]
    side_ref[104:120, :] = rest
    side_ref[120:128, :] = jnp.zeros((8, LANES), F32) + cs[7] * length
    q_refs[8] = q_out
    lanes, ks = iota((8, LANES), 1), iota((8, LANES), 0)
    top = d_tile(q_refs, 0)
    work = jnp.where(lanes < 8, pltpu.roll(top, LANES - 1, 1), 0.0)
    work = work + jnp.where(lanes == ks + 8, 1.0, 0.0)
    to_reflect = jnp.zeros((8, LANES), F32)
    pivot = jnp.ones((1, 1), F32)
    for k in range(8):
        row = work[k : k + 1]
        pivot = jnp.minimum(pivot, row[:, k : k + 1])
        beta = (scal if k == 7 else scal_refs[k + 1])[0:1, :]
        to_reflect = jnp.where(ks == k, row * beta, to_reflect)
        row = row / row[:, k : k + 1]
        column = jnp.where(ks == k, 0.0, work)[:, k : k + 1]
        work = jnp.where(ks == k, row, work - column * row)
    sound = (scal[11:12, 0:1] <= GROWTH) & (pivot >= PIVOT)
    flag_ref[...] = jnp.zeros((8, LANES), F32) + jnp.where(sound, 1.0, 0.0)
    factor = pltpu.roll(work, LANES - 8, 1)[:, 0:8]
    flipped = jnp.concatenate(
        [jnp.where(lanes < 8, pltpu.roll(work, LANES - 8, 1), 0.0), jnp.zeros((LANES - 8, LANES), F32)],
        axis=0,
    ).T[0:8, 0:8]
    to_reflect = jnp.where(lanes < 8, pltpu.roll(to_reflect, LANES - 8, 1), 0.0)
    inner = jnp.zeros((8, LANES), F32)
    packed = packed_ref[2:3]
    for k in range(8):
        entry = pltpu.roll(packed, LANES - 16 * k, 1) if k else packed
        inner = jnp.where(ks == k, entry, inner)
    used = (lanes >= 1) & (lanes <= 8)
    inner = jnp.where(used, inner, 0.0)
    cross = jnp.where(used, rows_at(aq_rows, 12), 0.0)
    inner = pltpu.roll(inner - cross, LANES - 1, 1)
    cross = pltpu.roll(cross, LANES - 1, 1)
    square = jnp.concatenate([cross, jnp.zeros((LANES - 8, LANES), F32)], axis=0)
    inner = inner - square.T[0:8]
    for k in range(1, 8):
        source = scal if k == 7 else scal_refs[k + 1]
        near = ((ks == k - 1) & (lanes == k)) | ((ks == k) & (lanes == k - 1))
        inner = inner - jnp.where(near, source[0:1, :], 0.0)
        alpha = source[10:11, :]
        inner = inner + jnp.where((ks == k - 1) & (lanes == k - 1), alpha, 0.0)
    inner = inner[:, 0:8]
    core = product(factor, product(inner, factor))

    def tiles(base, count, edge_ref, first, kept):
        ds, ys = [], []
        for t in range(count):
            row = base + t
            d = d_tile(q_refs, row)
            ad = -rows_at(aq_rows, kept + t)
            if edge_ref is not None:
                ad = ad + jnp.concatenate(
                    [edge_ref[count * k + t : count * k + t + 1, :] for k in range(8)], axis=0
                )
            ds.append(d)
            ys.append(product(factor, ad) - 0.5 * product(core, d))
            side_ref[first + 8 * t : first + 8 * t + 8, :] = product(flipped, d)
        return ds, ys

    ds, ys = tiles(4 * row_index, 4, edge_r_ref, 0, 0)
    for t in range(4):
        high, middle, low = three(jnp.concatenate([ds[t], ys[t]], axis=0))
        stack = [high, high, middle, middle, high, low, jnp.zeros((32, LANES), F32)]
        at = slice(t * LANES, (t + 1) * LANES)
        left_ref[at, 0:LANES] = jnp.concatenate(stack, axis=0).T.astype(jnp.bfloat16)
        high, middle, low = three(side_ref[8 * t : 8 * t + 8, :])
        stack = [high, high, middle, middle, high, low, jnp.zeros((80, LANES), F32)]
        left_ref[at, LANES:] = jnp.concatenate(stack, axis=0).T.astype(jnp.bfloat16)
        out = jnp.zeros((8, LANES), F32)
        for k in range(8):
            out = out + to_reflect[:, k : k + 1] * ds[t][k : k + 1, :]
        out = jnp.where((4 * row_index + t == 0) & (lanes <= ks), 0.0, out)
        reflect_ref[:, t * LANES : (t + 1) * LANES] = out
    ds, ys = tiles(8 * col_index, 8, None, 32, 4)
    for t in range(8):
        high, middle, low = three(jnp.concatenate([ys[t], ds[t]], axis=0))
        stack = [high, middle, high, middle, low, high]
        at = slice(t * LANES, (t + 1) * LANES)
        right_ref[:, at] = jnp.concatenate(stack, axis=0).astype(jnp.bfloat16)


def trailing_kernel(
    a_ref, recv_ref, q_ref, side_ref, left_ref, right_ref, out_ref, block_ref, edge_ref, sems
):
    for t in range(8):
        members = [divmod(8 * k + t, 2) for k in range(8)]
        high, middle, low = three(
            jnp.concatenate([recv_ref[r, 2][i : i + 1] for r, i in members], axis=0)
        )
        stack = jnp.concatenate([high, middle, high, middle, low, high], axis=0)
        edge_ref[:, t * LANES : (t + 1) * LANES] = stack.astype(jnp.bfloat16)
    inverse = coefficient(side_ref, 96)
    aq = (given_rows(recv_ref, True) - side_ref[104:120, :]) * inverse
    alpha = total(q_ref[...] * gathered(recv_ref, 0, 4)) - coefficient(side_ref, 120)
    alpha = alpha * inverse
    lanes = iota((1, LANES), 1)
    shifted = pltpu.roll(aq[12:13, :], LANES - 1, 1)
    added = -jnp.where(lanes < 8, shifted, 0.0)
    added = jnp.concatenate([added, jnp.zeros((7, LANES), F32)], axis=0).T[0:8, 0:1]

    def last(count, first, kept):
        return [
            -aq[kept + t : kept + t + 1, :]
            - jnp.sum(added * side_ref[first + 8 * t : first + 8 * t + 8, :], axis=0, keepdims=True)
            for t in range(count)
        ]

    ws_r = last(4, 0, 0)
    ws_c = last(8, 32, 4)
    blank = jnp.zeros((6, LANES), F32)
    copies = []
    for q in range(4):
        slope = side_ref[8 * q + 7 : 8 * q + 8, :]
        upright = jnp.concatenate([slope, ws_r[q] - alpha * slope, blank], axis=0).T
        for half in range(2):
            at = slice(q * LANES + half * 64, q * LANES + half * 64 + 64)
            piece = upright[half * 64 : half * 64 + 64]
            change = jnp.dot(left_ref[at, 0:96], right_ref[...], preferred_element_type=F32)
            edge = left_ref[at, LANES : LANES + 48]
            change = change + jnp.dot(edge, edge_ref[...], preferred_element_type=F32)
            for t in range(8):
                to = slice(t * LANES, (t + 1) * LANES)
                block_ref[at, to] = (
                    a_ref[at, to]
                    - change[:, to]
                    - piece[:, 0:1] * ws_c[t]
                    - piece[:, 1:2] * side_ref[39 + 8 * t : 40 + 8 * t, :]
                )
            copy = pltpu.make_async_copy(
                block_ref.at[at, :], out_ref.at[at, :], sems.at[2 * q + half]
            )
            copy.start()
            copies.append(copy)
    for copy in copies:
        copy.wait()


def call(kernel, outs, *args, scratch=(), pinned=True, flops=1000):
    def shape(x):
        if not isinstance(x, tuple):
            return x
        return VMEM(x, F32) if pinned else jax.ShapeDtypeStruct(x, F32)

    return pl.pallas_call(
        kernel,
        out_shape=[shape(x) for x in outs],
        in_specs=[pl.BlockSpec(memory_space=VMEM)] * len(args),
        out_specs=[pl.BlockSpec(memory_space=VMEM)] * len(outs),
        scratch_shapes=[VMEM(s, F32) for s in scratch],
        compiler_params=pltpu.CompilerParams(vmem_limit_bytes=LIMIT),
        cost_estimate=pl.CostEstimate(flops=flops, bytes_accessed=1000, transcendentals=0),
    )(*args)


def exchange(x, axis):
    return lax.all_to_all(x, axis, 0, 0, tiled=True)


def local(matrix):
    whole = (N // LANES, LANES)
    send, held = pl.pallas_call(
        start_kernel,
        out_shape=[VMEM((16, 2, 4, LANES), F32), VMEM(matrix.shape, F32)],
        in_specs=[pl.BlockSpec(memory_space=pltpu.HBM)],
        out_specs=[pl.BlockSpec(memory_space=VMEM)] * 2,
        scratch_shapes=[VMEM((matrix.shape[0], LANES), F32), pltpu.SemaphoreType.DMA((2,))],
        compiler_params=pltpu.CompilerParams(vmem_limit_bytes=LIMIT),
    )(pltpu.with_memory_space_constraint(matrix, pltpu.HBM))
    recv = exchange(send, "col")
    send, piece = call(first_kernel, [(32, 4, 4, LANES), (4, LANES)], held, recv)
    recv = exchange(send, "row")
    qs, aq_rows, scals = {}, {}, {}
    for step in range(2, 9):
        args = [held, recv]
        if step == 2:
            args.append(piece)
        if step > 2:
            args.append(scals[step - 2])
        args += [qs[i] for i in range(1, step - 1)] + [aq_rows[i] for i in range(1, step - 2)]
        message = (7, 2, LANES) if step == 2 else (3, 4, LANES)
        outs = [(16 if step % 2 == 0 else 32, *message), whole]
        if step > 2:
            outs.append((16, LANES))
        outs.append((16, LANES))
        if step == 3:
            outs.append((32, LANES))
        if step == 2:
            outs.append((4, LANES))
        result = list(call(functools.partial(step_kernel, step), outs, *args))
        send = result.pop(0)
        qs[step - 1] = result.pop(0)
        if step > 2:
            aq_rows[step - 2] = result.pop(0)
        scals[step - 1] = result.pop(0)
        if step == 3:
            edge_r = result.pop(0)
        if step == 2:
            piece = packed = result.pop(0)
        recv = exchange(send, "col" if step % 2 == 0 else "row")
    (send,) = call(last_send_kernel, [(32, 3, 2, LANES)], recv, packed)
    last = exchange(send, "row")
    rows, cols = matrix.shape
    q, flag, reflect, side, left, right = call(
        panel_kernel,
        [whole, jax.ShapeDtypeStruct((8, LANES), F32), pltpu.HBM((8, rows), F32), (128, LANES)]
        + [VMEM((rows, 2 * LANES), jnp.bfloat16), VMEM((96, cols), jnp.bfloat16)],
        recv,
        packed,
        edge_r,
        *[scals[i] for i in range(1, 8)],
        *[qs[i] for i in range(1, 8)],
        *[aq_rows[i] for i in range(1, 7)],
        scratch=[(16, LANES)],
        flops=40000000,
    )
    trailing = pl.pallas_call(
        trailing_kernel,
        out_shape=jax.ShapeDtypeStruct(matrix.shape, F32),
        in_specs=[pl.BlockSpec(memory_space=VMEM)] * 6,
        out_specs=pl.BlockSpec(memory_space=pltpu.HBM),
        scratch_shapes=[
            VMEM(matrix.shape, F32),
            VMEM((48, cols), jnp.bfloat16),
            pltpu.SemaphoreType.DMA((8,)),
        ],
        compiler_params=pltpu.CompilerParams(vmem_limit_bytes=LIMIT),
    )(held, last, q, side, left, right)
    if not GUARD:
        return trailing, reflect.T
    _, trailing, reflect = lax.while_loop(
        lambda state: state[0],
        lambda state: (jnp.bool_(False), *column_by_column(matrix)),
        (flag[0, 0] < 0.5, trailing, reflect),
    )
    return trailing, reflect.T


def as_it_is(x_ref, out_ref):
    out_ref[...] = x_ref[...]


def of_everyone(shard, axis):
    size = lax.axis_size(axis)
    return exchange(jnp.broadcast_to(shard[None], (size, *shard.shape)), axis)


def column_by_column(matrix):
    rows, cols = matrix.shape
    row_at, col_at = lax.axis_index("row") * rows, lax.axis_index("col") * cols
    panel = of_everyone(matrix[:, :COLS].T, "col")[0]
    panel = of_everyone(panel, "row").transpose(1, 0, 2).reshape(COLS, N)
    positions = jnp.arange(N, dtype=jnp.int32)

    def one(column, state):
        reflect, companion = state

        def row(x):
            return lax.dynamic_index_in_dim(x, column, 0, keepdims=False)

        def entries(x):
            return lax.dynamic_index_in_dim(x, column, 1, keepdims=True)

        current = row(panel) - jnp.sum(
            reflect * entries(companion) + companion * entries(reflect), axis=0
        )
        below = jnp.where(positions > column, current, 0.0)
        leading = jnp.sum(jnp.where(positions == column + 1, current, 0.0))
        length = jnp.sqrt(jnp.sum(below * below))
        vector = below + jnp.where(positions == column + 1, length, 0.0)
        scaling = 1.0 / (length * (length + leading))
        along_rows_here = lax.dynamic_slice_in_dim(vector, row_at, rows, 0)
        image = jnp.sum(matrix * along_rows_here[:, None], axis=0)
        image = of_everyone(image, "row").sum(axis=0)
        image = of_everyone(image, "col").reshape(N)
        to_reflect = jnp.sum(companion * vector, axis=1, keepdims=True)
        to_companion = jnp.sum(reflect * vector, axis=1, keepdims=True)
        pushed = scaling * (
            image - jnp.sum(reflect * to_reflect + companion * to_companion, axis=0)
        )
        update = pushed - 0.5 * scaling * jnp.sum(pushed * vector) * vector
        reflect = lax.dynamic_update_index_in_dim(reflect, vector, column, 0)
        return reflect, lax.dynamic_update_index_in_dim(companion, update, column, 0)

    zero = jnp.zeros((COLS, N), F32)
    reflect, companion = lax.fori_loop(0, COLS, one, (zero, zero))
    reflect_rows = lax.dynamic_slice_in_dim(reflect, row_at, rows, 1)
    companion_rows = lax.dynamic_slice_in_dim(companion, row_at, rows, 1)
    reflect_cols = lax.dynamic_slice_in_dim(reflect, col_at, cols, 1)
    companion_cols = lax.dynamic_slice_in_dim(companion, col_at, cols, 1)

    def subtract(k, trailing):
        def row(x):
            return lax.dynamic_index_in_dim(x, k, 0, keepdims=False)

        return (
            trailing
            - row(reflect_rows)[:, None] * row(companion_cols)[None, :]
            - row(companion_rows)[:, None] * row(reflect_cols)[None, :]
        )

    (reflect_rows,) = call(as_it_is, [(COLS, rows)], reflect_rows, pinned=False)
    return lax.fori_loop(0, COLS, subtract, matrix), reflect_rows


def solution(mesh):
    placed = (P("row", "col"),)
    return jax.shard_map(
        local,
        mesh=mesh,
        in_specs=placed,
        out_specs=(P("row", "col"), P("row", None)),
        check_vma=False,
    )
```

```python
import functools

import jax
import jax.numpy as jnp
from jax import lax
from jax.experimental import pallas as pl
from jax.experimental.pallas import tpu as pltpu
from jax.sharding import PartitionSpec as P


N = 16384
COLS = 8
LANES = 128
F32 = jnp.float32
VMEM = pltpu.VMEM
LIMIT = 16 << 20
GUARD = True
GROWTH = 16.0
PIVOT = 0.05


def places():
    return lax.axis_index("row"), lax.axis_index("col")


def total(x):
    return jnp.sum(jnp.sum(x, axis=0, keepdims=True), axis=1, keepdims=True)


def iota(shape, dim):
    return lax.broadcasted_iota(jnp.int32, shape, dim)


def without_first(x, owner):
    hit = (iota(x.shape, 0) == 0) & (iota(x.shape, 1) == 0)
    if owner is not None:
        hit = hit & (owner == 0)
    return jnp.where(hit, 0.0, x)


def times_rows(a_ref, x):
    upright = jnp.concatenate([x, jnp.zeros_like(x)], axis=0).T
    out = []
    for t in range(8):
        acc = jnp.zeros((8, LANES), F32)
        for q in range(4):
            block = a_ref[q * LANES : (q + 1) * LANES, t * LANES : (t + 1) * LANES]
            acc = acc + jnp.sum((block * upright[:, q : q + 1]).reshape(16, 8, LANES), axis=0)
        out.append(jnp.sum(acc, axis=0, keepdims=True))
    return jnp.concatenate(out, axis=0)


def times_cols(a_ref, x):
    out = []
    for q in range(4):
        acc = jnp.zeros((LANES, LANES), F32)
        for t in range(8):
            block = a_ref[q * LANES : (q + 1) * LANES, t * LANES : (t + 1) * LANES]
            acc = acc + block * x[t : t + 1, :]
        out.append(jnp.sum(acc.T, axis=0, keepdims=True))
    return jnp.concatenate(out, axis=0)


def send_all(send_ref, first, x):
    height = send_ref.shape[2]
    for member in range(send_ref.shape[0]):
        for k in range(x.shape[0] // height):
            send_ref[member, first // height + k] = x[k * height : (k + 1) * height]


def taken(recv_ref, member, first, count):
    height = recv_ref.shape[2]
    return [recv_ref[member, first // height + k] for k in range(count // height)]


def summed(recv_ref, count):
    height = recv_ref.shape[2]
    blocks = [jnp.sum(recv_ref[:, k], axis=0) for k in range(count // height)]
    return jnp.concatenate(blocks, axis=0)


def gathered(recv_ref, first, count):
    members = range(recv_ref.shape[0])
    return jnp.concatenate(
        [block for m in members for block in taken(recv_ref, m, first, count)], axis=0
    )


def start_kernel(a_ref, send_ref, held_ref, slab_ref, sems):
    copy = pltpu.make_async_copy(a_ref.at[:, pl.ds(0, LANES)], slab_ref, sems.at[0])
    copy.start()
    holds = []
    for q in range(4):
        at = pl.ds(q * LANES, LANES)
        hold = pltpu.make_async_copy(a_ref.at[at, :], held_ref.at[at, :], sems.at[1 + q])
        hold.start()
        holds.append(hold)
    copy.wait()
    left = [slab_ref[q * LANES : (q + 1) * LANES, :].T for q in range(4)]
    column = jnp.concatenate([x[0:1] for x in left], axis=0)
    corner = slab_ref[0:16, :]
    packed = jnp.zeros((1, LANES), F32)
    for j in range(COLS):
        lanes = iota((1, LANES), 1)
        entry = jnp.where(lanes < 16, corner[j + 1 : j + 2], 0.0)
        packed = packed + (pltpu.roll(entry, 16 * j, 1) if j else entry)
    blank = jnp.zeros((1, LANES), F32)
    for member in range(16):
        j, half = member // 2, member % 2
        rows = [left[2 * half + k][j + 1 : j + 2] for k in range(2)]
        send_ref[member, 0] = column
        send_ref[member, 1] = jnp.concatenate([*rows, packed, blank], axis=0)
    for hold in holds:
        hold.wait()


def first_kernel(a_ref, recv_ref, send_ref, piece_ref):
    ids_ref = places()
    column = recv_ref[0, 0]
    piece_ref[...] = recv_ref[0, 1]
    packed = recv_ref[0, 1][2:3]
    send_all(send_ref, 0, times_rows(a_ref, without_first(column, ids_ref[0])))
    send_all(send_ref, 8, column)
    blank = jnp.zeros((1, LANES), F32)
    for member in range(32):
        j, quarter = member // 4, member % 4
        rows = [
            a_ref[j + 1 : j + 2, (2 * quarter + k) * LANES : (2 * quarter + k + 1) * LANES]
            for k in range(2)
        ]
        send_ref[member, 3] = jnp.concatenate([*rows, packed, blank], axis=0)


def coefficient(scal, k):
    return scal[k : k + 1, 0:1]


def settle(step, given, scal, qs):
    u = without_first(given, None) if step == 2 else given
    zero = jnp.zeros((1, LANES), F32)
    w, cs, growth = u, {}, 0.0
    known = range(1, step - 1)
    rows = [jnp.sum(u * qs[i], axis=0, keepdims=True) for i in known]
    rows = rows + [zero] * (7 - len(rows)) + [jnp.sum(u * u, axis=0, keepdims=True)]
    sums = jnp.sum(jnp.concatenate(rows, axis=0), axis=1, keepdims=True)
    squared = sums[7:8, 0:1]
    if step == 2:
        alpha = shift = given[0:1, 0:1]
    else:
        for i in known:
            cs[i] = sums[i - 1 : i, 0:1]
            w = w - cs[i] * qs[i]
        growth = jnp.sum(jnp.where(iota((8, 1), 0) < 7, sums * sums, 0.0), axis=0, keepdims=True)
        squared = squared - growth
        alpha, before = cs[step - 2] + coefficient(scal, 9), coefficient(scal, 10)
        smaller = jnp.where(jnp.abs(alpha) < jnp.abs(before), alpha, before)
        shift = jnp.where(alpha * before > 0.0, smaller, 0.0)
    length = jnp.sqrt(squared)
    inverse = 1.0 / length
    growth = 1.0 + growth * inverse * inverse
    if step > 2:
        growth = growth * coefficient(scal, 11)
    out = [zero + length] + [zero + cs[i] if i in cs else zero for i in range(1, 8)]
    out = out + [zero + x for x in (inverse, shift, alpha, growth)] + [zero] * 4
    return w * inverse, length, inverse, shift, cs, jnp.concatenate(out, axis=0)


def given_rows(recv_ref, by_rows):
    row_index, col_index = places()
    height = recv_ref.shape[2]
    if by_rows:
        start = 8 if recv_ref.shape[1] * height > 8 else 0
        here = taken(recv_ref, row_index, start, 4)
        there = taken(recv_ref, 2 * col_index, start, 4) + taken(recv_ref, 2 * col_index + 1, start, 4)
    else:
        start, half = 4, row_index % 2 * (4 // height)
        here = [recv_ref[row_index // 2, half + (start // height + k)] for k in range(4 // height)]
        there = taken(recv_ref, col_index, start, 8)
    first = recv_ref[0, start // height][0:1]
    return jnp.concatenate([*here, *there, first, jnp.zeros((3, LANES), F32)], axis=0)


def kept_rows(ref):
    row_index, col_index = places()
    here, there = ref[pl.ds(4 * row_index, 4), :], ref[pl.ds(8 * col_index, 8), :]
    return jnp.concatenate([here, there, ref[0:1, :], jnp.zeros((3, LANES), F32)], axis=0)


def product_rows(step, recv_ref, scal, q_refs):
    out = given_rows(recv_ref, step % 2 == 0)
    out = out + coefficient(scal, 9) * kept_rows(q_refs[step - 2])
    if step > 3:
        return out + coefficient(scal, 0) * kept_rows(q_refs[step - 3])
    row_index, col_index = places()
    rows, lanes = iota(out.shape, 0), iota(out.shape, 1)
    start = ((rows == 0) & (row_index == 0)) | ((rows == 4) & (col_index == 0)) | (rows == 12)
    return out + jnp.where(start & (lanes == 0), coefficient(scal, 0), 0.0)


def step_kernel(step, *refs):
    refs = list(refs)
    a_ref, recv_ref = refs[:2]
    del refs[:2]
    row_index, col_index = places()
    piece_ref = refs.pop(0) if step == 2 else None
    scal = refs.pop(0)[...] if step > 2 else None
    q_refs = {i: refs.pop(0) for i in range(1, step - 1)}
    rows_refs = {i: refs.pop(0) for i in range(1, step - 2)}
    send_ref = refs.pop(0)
    q_ref = refs.pop(0)
    if step > 2:
        rows_refs[step - 2] = refs.pop(0)
    scal_ref = refs.pop(0)
    edge_ref = refs.pop(0) if step == 3 else None
    new_piece_ref = refs.pop(0) if step == 2 else None

    even = step % 2 == 0
    if even:
        y_here, given = summed(recv_ref, 8), gathered(recv_ref, 8, 4)
        chunk, count, part = col_index, 8, slice(4, 12)
    else:
        y_here, given = summed(recv_ref, 4), gathered(recv_ref, 4, 8)
        chunk, count, part = row_index, 4, slice(0, 4)
    if step > 2:
        rows_refs[step - 2][...] = product_rows(step, recv_ref, scal, q_refs)
    q, length, inverse, shift, cs, scal_out = settle(
        step, given, scal, {i: r[...] for i, r in q_refs.items()}
    )
    q_ref[...] = q
    scal_ref[...] = scal_out
    at = pl.ds(chunk * count, count)
    here = y_here
    for i in cs:
        here = here - cs[i] * rows_refs[i][part, :]
    q_here = without_first(given_rows(recv_ref, even)[part], chunk)
    for i in cs:
        q_here = q_here - cs[i] * q_refs[i][at, :]
    here = (here - shift * q_here) * inverse
    if step > 2:
        here = here - length * q_refs[step - 2][at, :]
    here = without_first(here, chunk)
    if even:
        send_all(send_ref, 0, times_cols(a_ref, here))
        send_all(send_ref, 4, here)
    else:
        send_all(send_ref, 0, times_rows(a_ref, here))
        send_all(send_ref, 8, here)
    if step == 2:
        send_all(send_ref, 12, piece_ref[0:2, :])
        new_piece_ref[...] = recv_ref[0, 3]
    if step == 3:
        edge_ref[...] = gathered(recv_ref, 12, 2)


def last_send_kernel(recv_ref, piece_ref, send_ref):
    send_all(send_ref, 0, summed(recv_ref, 4))
    send_all(send_ref, 4, piece_ref[0:2, :])


def sign(k):
    return -1.0 if k % 2 else 1.0


def product(x, y):
    return lax.dot_general(
        x,
        y,
        (((0,), (0,)), ((), ())),
        precision=lax.Precision.HIGHEST,
        preferred_element_type=F32,
    )


def rows_at(refs, row):
    blank = jnp.zeros((1, LANES), F32)
    return jnp.concatenate(
        [sign(k) * refs[k][pl.ds(row, 1), :] if k in refs else blank for k in range(1, 9)], axis=0
    )


def d_tile(q_refs, row):
    lanes, ks = iota((8, LANES), 1), iota((8, LANES), 0)
    unit = jnp.where((lanes == ks + 1) & (row == 0), 1.0, 0.0)
    return unit - rows_at(q_refs, row)


def three(x):
    high = x.astype(jnp.bfloat16).astype(F32)
    middle = (x - high).astype(jnp.bfloat16).astype(F32)
    low = (x - high - middle).astype(jnp.bfloat16).astype(F32)
    return high, middle, low


def panel_kernel(*refs):
    row_index, col_index = places()
    refs = list(refs)
    refs.insert(0, None)
    recv_ref, packed_ref, edge_r_ref = refs[1:4]
    scal_refs = {i: refs[3 + i] for i in range(1, 8)}
    q_refs = {i: refs[10 + i] for i in range(1, 8)}
    aq_rows = {i: refs[17 + i] for i in range(1, 7)}
    q_out, flag_ref, reflect_ref, side_ref, left_ref, right_ref, rows_out = refs[24:31]
    q, length, _, _, cs, scal = settle(
        9, gathered(recv_ref, 4, 8), scal_refs[7][...], {i: r[...] for i, r in q_refs.items()}
    )
    q_out[...] = q
    rows_out[...] = product_rows(9, recv_ref, scal_refs[7][...], q_refs)
    aq_rows[7] = rows_out
    rest = jnp.zeros((16, LANES), F32)
    for i in range(1, 8):
        rest = rest + cs[i] * aq_rows[i][...]
    side_ref[96:104, :] = scal[8:16]
    side_ref[104:120, :] = rest
    side_ref[120:128, :] = jnp.zeros((8, LANES), F32) + cs[7] * length
    q_refs[8] = q_out
    lanes, ks = iota((8, LANES), 1), iota((8, LANES), 0)
    top = d_tile(q_refs, 0)
    work = jnp.where(lanes < 8, pltpu.roll(top, LANES - 1, 1), 0.0)
    work = work + jnp.where(lanes == ks + 8, 1.0, 0.0)
    to_reflect = jnp.zeros((8, LANES), F32)
    pivot = jnp.ones((1, 1), F32)
    for k in range(8):
        row = work[k : k + 1]
        pivot = jnp.minimum(pivot, row[:, k : k + 1])
        beta = (scal if k == 7 else scal_refs[k + 1])[0:1, :]
        to_reflect = jnp.where(ks == k, row * beta, to_reflect)
        row = row / row[:, k : k + 1]
        column = jnp.where(ks == k, 0.0, work)[:, k : k + 1]
        work = jnp.where(ks == k, row, work - column * row)
    sound = (scal[11:12, 0:1] <= GROWTH) & (pivot >= PIVOT)
    flag_ref[...] = jnp.zeros((8, LANES), F32) + jnp.where(sound, 1.0, 0.0)
    factor = pltpu.roll(work, LANES - 8, 1)[:, 0:8]
    flipped = jnp.concatenate(
        [jnp.where(lanes < 8, pltpu.roll(work, LANES - 8, 1), 0.0), jnp.zeros((LANES - 8, LANES), F32)],
        axis=0,
    ).T[0:8, 0:8]
    to_reflect = jnp.where(lanes < 8, pltpu.roll(to_reflect, LANES - 8, 1), 0.0)
    inner = jnp.zeros((8, LANES), F32)
    packed = packed_ref[2:3]
    for k in range(8):
        entry = pltpu.roll(packed, LANES - 16 * k, 1) if k else packed
        inner = jnp.where(ks == k, entry, inner)
    used = (lanes >= 1) & (lanes <= 8)
    inner = jnp.where(used, inner, 0.0)
    cross = jnp.where(used, rows_at(aq_rows, 12), 0.0)
    inner = pltpu.roll(inner - cross, LANES - 1, 1)
    cross = pltpu.roll(cross, LANES - 1, 1)
    square = jnp.concatenate([cross, jnp.zeros((LANES - 8, LANES), F32)], axis=0)
    inner = inner - square.T[0:8]
    for k in range(1, 8):
        source = scal if k == 7 else scal_refs[k + 1]
        near = ((ks == k - 1) & (lanes == k)) | ((ks == k) & (lanes == k - 1))
        inner = inner - jnp.where(near, source[0:1, :], 0.0)
        alpha = source[10:11, :]
        inner = inner + jnp.where((ks == k - 1) & (lanes == k - 1), alpha, 0.0)
    inner = inner[:, 0:8]
    core = product(factor, product(inner, factor))

    def tiles(base, count, edge_ref, first, kept):
        ds, ys = [], []
        for t in range(count):
            row = base + t
            d = d_tile(q_refs, row)
            ad = -rows_at(aq_rows, kept + t)
            if edge_ref is not None:
                ad = ad + jnp.concatenate(
                    [edge_ref[count * k + t : count * k + t + 1, :] for k in range(8)], axis=0
                )
            ds.append(d)
            ys.append(product(factor, ad) - 0.5 * product(core, d))
            side_ref[first + 8 * t : first + 8 * t + 8, :] = product(flipped, d)
        return ds, ys

    ds, ys = tiles(4 * row_index, 4, edge_r_ref, 0, 0)
    for t in range(4):
        high, middle, low = three(jnp.concatenate([ds[t], ys[t]], axis=0))
        stack = [high, high, middle, middle, high, low, jnp.zeros((32, LANES), F32)]
        at = slice(t * LANES, (t + 1) * LANES)
        left_ref[at, 0:LANES] = jnp.concatenate(stack, axis=0).T.astype(jnp.bfloat16)
        high, middle, low = three(side_ref[8 * t : 8 * t + 8, :])
        stack = [high, high, middle, middle, high, low, jnp.zeros((80, LANES), F32)]
        left_ref[at, LANES:] = jnp.concatenate(stack, axis=0).T.astype(jnp.bfloat16)
        out = jnp.zeros((8, LANES), F32)
        for k in range(8):
            out = out + to_reflect[:, k : k + 1] * ds[t][k : k + 1, :]
        out = jnp.where((4 * row_index + t == 0) & (lanes <= ks), 0.0, out)
        reflect_ref[:, t * LANES : (t + 1) * LANES] = out
    ds, ys = tiles(8 * col_index, 8, None, 32, 4)
    for t in range(8):
        high, middle, low = three(jnp.concatenate([ys[t], ds[t]], axis=0))
        stack = [high, middle, high, middle, low, high]
        at = slice(t * LANES, (t + 1) * LANES)
        right_ref[:, at] = jnp.concatenate(stack, axis=0).astype(jnp.bfloat16)


def trailing_kernel(
    a_ref, recv_ref, q_ref, side_ref, left_ref, right_ref, out_ref, block_ref, edge_ref, sems
):
    for t in range(8):
        members = [divmod(8 * k + t, 2) for k in range(8)]
        high, middle, low = three(
            jnp.concatenate([recv_ref[r, 2][i : i + 1] for r, i in members], axis=0)
        )
        stack = jnp.concatenate([high, middle, high, middle, low, high], axis=0)
        edge_ref[:, t * LANES : (t + 1) * LANES] = stack.astype(jnp.bfloat16)
    inverse = coefficient(side_ref, 96)
    aq = (given_rows(recv_ref, True) - side_ref[104:120, :]) * inverse
    alpha = total(q_ref[...] * gathered(recv_ref, 0, 4)) - coefficient(side_ref, 120)
    alpha = alpha * inverse
    lanes = iota((1, LANES), 1)
    shifted = pltpu.roll(aq[12:13, :], LANES - 1, 1)
    added = -jnp.where(lanes < 8, shifted, 0.0)
    added = jnp.concatenate([added, jnp.zeros((7, LANES), F32)], axis=0).T[0:8, 0:1]

    def last(count, first, kept):
        return [
            -aq[kept + t : kept + t + 1, :]
            - jnp.sum(added * side_ref[first + 8 * t : first + 8 * t + 8, :], axis=0, keepdims=True)
            for t in range(count)
        ]

    ws_r = last(4, 0, 0)
    ws_c = last(8, 32, 4)
    blank = jnp.zeros((6, LANES), F32)
    copies = []
    for q in range(4):
        slope = side_ref[8 * q + 7 : 8 * q + 8, :]
        upright = jnp.concatenate([slope, ws_r[q] - alpha * slope, blank], axis=0).T
        for half in range(2):
            at = slice(q * LANES + half * 64, q * LANES + half * 64 + 64)
            piece = upright[half * 64 : half * 64 + 64]
            change = jnp.dot(left_ref[at, 0:96], right_ref[...], preferred_element_type=F32)
            edge = left_ref[at, LANES : LANES + 48]
            change = change + jnp.dot(edge, edge_ref[...], preferred_element_type=F32)
            for t in range(8):
                to = slice(t * LANES, (t + 1) * LANES)
                block_ref[at, to] = (
                    a_ref[at, to]
                    - change[:, to]
                    - piece[:, 0:1] * ws_c[t]
                    - piece[:, 1:2] * side_ref[39 + 8 * t : 40 + 8 * t, :]
                )
            copy = pltpu.make_async_copy(
                block_ref.at[at, :], out_ref.at[at, :], sems.at[2 * q + half]
            )
            copy.start()
            copies.append(copy)
    for copy in copies:
        copy.wait()


def call(kernel, outs, *args, scratch=(), pinned=True, flops=1000):
    def shape(x):
        if not isinstance(x, tuple):
            return x
        return VMEM(x, F32) if pinned else jax.ShapeDtypeStruct(x, F32)

    return pl.pallas_call(
        kernel,
        out_shape=[shape(x) for x in outs],
        in_specs=[pl.BlockSpec(memory_space=VMEM)] * len(args),
        out_specs=[pl.BlockSpec(memory_space=VMEM)] * len(outs),
        scratch_shapes=[VMEM(s, F32) for s in scratch],
        compiler_params=pltpu.CompilerParams(vmem_limit_bytes=LIMIT),
        cost_estimate=pl.CostEstimate(flops=flops, bytes_accessed=1000, transcendentals=0),
    )(*args)


def exchange(x, axis):
    return lax.all_to_all(x, axis, 0, 0, tiled=True)


def local(matrix):
    whole = (N // LANES, LANES)
    send, held = pl.pallas_call(
        start_kernel,
        out_shape=[VMEM((16, 2, 4, LANES), F32), VMEM(matrix.shape, F32)],
        in_specs=[pl.BlockSpec(memory_space=pltpu.HBM)],
        out_specs=[pl.BlockSpec(memory_space=VMEM)] * 2,
        scratch_shapes=[VMEM((matrix.shape[0], LANES), F32), pltpu.SemaphoreType.DMA((5,))],
        compiler_params=pltpu.CompilerParams(vmem_limit_bytes=LIMIT),
    )(pltpu.with_memory_space_constraint(matrix, pltpu.HBM))
    recv = exchange(send, "col")
    send, piece = call(first_kernel, [(32, 4, 4, LANES), (4, LANES)], held, recv)
    recv = exchange(send, "row")
    qs, aq_rows, scals = {}, {}, {}
    for step in range(2, 9):
        args = [held, recv]
        if step == 2:
            args.append(piece)
        if step > 2:
            args.append(scals[step - 2])
        args += [qs[i] for i in range(1, step - 1)] + [aq_rows[i] for i in range(1, step - 2)]
        message = (7, 2, LANES) if step == 2 else (3, 4, LANES)
        outs = [(16 if step % 2 == 0 else 32, *message), whole]
        if step > 2:
            outs.append((16, LANES))
        outs.append((16, LANES))
        if step == 3:
            outs.append((32, LANES))
        if step == 2:
            outs.append((4, LANES))
        result = list(call(functools.partial(step_kernel, step), outs, *args))
        send = result.pop(0)
        qs[step - 1] = result.pop(0)
        if step > 2:
            aq_rows[step - 2] = result.pop(0)
        scals[step - 1] = result.pop(0)
        if step == 3:
            edge_r = result.pop(0)
        if step == 2:
            piece = packed = result.pop(0)
        recv = exchange(send, "col" if step % 2 == 0 else "row")
    (send,) = call(last_send_kernel, [(32, 3, 2, LANES)], recv, packed)
    last = exchange(send, "row")
    rows, cols = matrix.shape
    q, flag, reflect, side, left, right = call(
        panel_kernel,
        [whole, jax.ShapeDtypeStruct((8, LANES), F32), pltpu.HBM((8, rows), F32), (128, LANES)]
        + [VMEM((rows, 2 * LANES), jnp.bfloat16), VMEM((96, cols), jnp.bfloat16)],
        recv,
        packed,
        edge_r,
        *[scals[i] for i in range(1, 8)],
        *[qs[i] for i in range(1, 8)],
        *[aq_rows[i] for i in range(1, 7)],
        scratch=[(16, LANES)],
        flops=40000000,
    )
    trailing = pl.pallas_call(
        trailing_kernel,
        out_shape=jax.ShapeDtypeStruct(matrix.shape, F32),
        in_specs=[pl.BlockSpec(memory_space=VMEM)] * 6,
        out_specs=pl.BlockSpec(memory_space=pltpu.HBM),
        scratch_shapes=[
            VMEM(matrix.shape, F32),
            VMEM((48, cols), jnp.bfloat16),
            pltpu.SemaphoreType.DMA((8,)),
        ],
        compiler_params=pltpu.CompilerParams(
            vmem_limit_bytes=LIMIT
        ),
    )(held, last, q, side, left, right)
    if not GUARD:
        return trailing, reflect.T
    _, trailing, reflect = lax.while_loop(
        lambda state: state[0],
        lambda state: (jnp.bool_(False), *column_by_column(matrix)),
        (flag[0, 0] < 0.5, trailing, reflect),
    )
    return trailing, reflect.T


def as_it_is(x_ref, out_ref):
    out_ref[...] = x_ref[...]


def of_everyone(shard, axis):
    size = lax.axis_size(axis)
    return exchange(jnp.broadcast_to(shard[None], (size, *shard.shape)), axis)


def column_by_column(matrix):
    rows, cols = matrix.shape
    row_at, col_at = lax.axis_index("row") * rows, lax.axis_index("col") * cols
    panel = of_everyone(matrix[:, :COLS].T, "col")[0]
    panel = of_everyone(panel, "row").transpose(1, 0, 2).reshape(COLS, N)
    positions = jnp.arange(N, dtype=jnp.int32)

    def one(column, state):
        reflect, companion = state

        def row(x):
            return lax.dynamic_index_in_dim(x, column, 0, keepdims=False)

        def entries(x):
            return lax.dynamic_index_in_dim(x, column, 1, keepdims=True)

        current = row(panel) - jnp.sum(
            reflect * entries(companion) + companion * entries(reflect), axis=0
        )
        below = jnp.where(positions > column, current, 0.0)
        leading = jnp.sum(jnp.where(positions == column + 1, current, 0.0))
        length = jnp.sqrt(jnp.sum(below * below))
        vector = below + jnp.where(positions == column + 1, length, 0.0)
        scaling = 1.0 / (length * (length + leading))
        along_rows_here = lax.dynamic_slice_in_dim(vector, row_at, rows, 0)
        image = jnp.sum(matrix * along_rows_here[:, None], axis=0)
        image = of_everyone(image, "row").sum(axis=0)
        image = of_everyone(image, "col").reshape(N)
        to_reflect = jnp.sum(companion * vector, axis=1, keepdims=True)
        to_companion = jnp.sum(reflect * vector, axis=1, keepdims=True)
        pushed = scaling * (
            image - jnp.sum(reflect * to_reflect + companion * to_companion, axis=0)
        )
        update = pushed - 0.5 * scaling * jnp.sum(pushed * vector) * vector
        reflect = lax.dynamic_update_index_in_dim(reflect, vector, column, 0)
        return reflect, lax.dynamic_update_index_in_dim(companion, update, column, 0)

    zero = jnp.zeros((COLS, N), F32)
    reflect, companion = lax.fori_loop(0, COLS, one, (zero, zero))
    reflect_rows = lax.dynamic_slice_in_dim(reflect, row_at, rows, 1)
    companion_rows = lax.dynamic_slice_in_dim(companion, row_at, rows, 1)
    reflect_cols = lax.dynamic_slice_in_dim(reflect, col_at, cols, 1)
    companion_cols = lax.dynamic_slice_in_dim(companion, col_at, cols, 1)

    def subtract(k, trailing):
        def row(x):
            return lax.dynamic_index_in_dim(x, k, 0, keepdims=False)

        return (
            trailing
            - row(reflect_rows)[:, None] * row(companion_cols)[None, :]
            - row(companion_rows)[:, None] * row(reflect_cols)[None, :]
        )

    (reflect_rows,) = call(as_it_is, [(COLS, rows)], reflect_rows, pinned=False)
    return lax.fori_loop(0, COLS, subtract, matrix), reflect_rows


def solution(mesh):
    placed = (P("row", "col"),)
    return jax.shard_map(
        local,
        mesh=mesh,
        in_specs=placed,
        out_specs=(P("row", "col"), P("row", None)),
        check_vma=False,
    )
```
